32 devices in a mesh: dp: 16 (over z, y, x), tensor: 2 (over core).
Axes of the slice: x: 2, y: 2, z: 4, core: 2. Of those that a mesh axis runs over, the one named last changes fastest.
Arguments:
- inputs: bfloat16 [6144, 2560], P('dp'), may hold values from -6 to 6
- segment_ids: int32 [6144], P('dp'), may hold values from 0 to 11, never falling along the last dimension, each value on 1 to 1024 neighbouring positions
- cotangent: bfloat16 [6144, 2560], P('dp'), may hold values from -6 to 6
- branch_weight: bfloat16 [2, 2560, 2560], P(None, 'dp', 'tensor'), may hold values from -0.125 to 0.125
- out_weight: bfloat16 [2560, 2560], P('tensor', 'dp'), may hold values from -0.15625 to 0.15625
- ffw_in: bfloat16 [2, 2560, 7680], P(None, 'dp', 'tensor'), may hold values from -0.125 to 0.125
- ffw_out: bfloat16 [7680, 2560], P('tensor', 'dp'), may hold values from -0.09375 to 0.09375
- norm_scales: float32 [2, 2560], replicated, may hold values from -0.5 to 0.5
- branch_bias: float32 [2, 2560], P(None, 'tensor'), may hold values from -3 to 3
- conv_weight: float32 [4, 2560], P(None, 'tensor'), may hold values from -3 to 3
- conv_bias: float32 [2560], P('tensor'), may hold values from -3 to 3
- gate_weights: bfloat16 [2, 10, 256, 256], P(None, 'tensor'), may hold values from -0.375 to 0.375
- gate_bias: float32 [2, 2560], P(None, 'tensor'), may hold values from -3 to 3
- decay_param: float32 [2560], P('tensor'), may hold values from -10.5 to -5
- out_bias: float32 [2, 2560], replicated, may hold values from -3 to 3
- ffw_bias: float32 [2, 7680], P(None, 'tensor'), may hold values from -3 to 3
Outputs:
- output: float32 [6144, 2560], P('dp')
- input_grad: float32 [6144, 2560], P('dp')
- branch_weight_grad: float32 [2, 2560, 2560], P(None, 'dp', 'tensor')
- out_weight_grad: float32 [2560, 2560], P('tensor', 'dp')
- ffw_in_grad: float32 [2, 2560, 7680], P(None, 'dp', 'tensor')
- ffw_out_grad: float32 [7680, 2560], P('tensor', 'dp')
- norm_scales_grad: float32 [2, 2560], replicated
- branch_bias_grad: float32 [2, 2560], P(None, 'tensor')
- conv_weight_grad: float32 [4, 2560], P(None, 'tensor')
- conv_bias_grad: float32 [2560], P('tensor')
- gate_weights_grad: float32 [2, 10, 256, 256], P(None, 'tensor', 'dp')
- gate_bias_grad: float32 [2, 2560], P(None, 'tensor')
- decay_param_grad: float32 [2560], P('tensor')
- out_bias_grad: float32 [2, 2560], replicated
- ffw_bias_grad: float32 [2, 7680], P(None, 'tensor')
The draws below stay inside these ranges and needn't reach their ends.
Inputs may be any that keep to these rules, and one draw needn't show every extreme that they name: `segment_ids`: segment numbers never fall along the tokens; each sequence holds 1 to 1024 tokens and one holds exactly 1024.
All inputs are finite; a program needn't handle non-finite values.
Results may differ from the reference program's by a relative error of at most 0.0095.
Values may be sent and summed in bfloat16 or wider, within the bound.
A program may use at most 448 MiB of HBM per device.

```python
import math
import jax
import jax.numpy as jnp
import numpy as np
from jax import lax

D = 2560
HEADS = 10
BLOCK = 256
FF = 7680
CONV = 4
SEQ = 1024
R = 2560
TOKENS = 6144
SEGS = 12


def spiked(entries, rng, source, target, shards_of, factor):
    def block_of(axis_at):
        return (jnp.arange(entries.shape[axis_at]) // (entries.shape[axis_at] // shards_of)).reshape((-1,) + (1,) * (entries.ndim - 1 - axis_at))

    one_side = jax.random.permutation(rng, shards_of)[block_of(target)]
    other_side = (block_of(target) + shards_of // 2) % shards_of
    return jnp.where((block_of(source) == one_side) | (block_of(source) == other_side), factor * entries, entries)


def steps_of(rng, dims, cuts, smallest, top_value):
    level, own = 1.0, jax.random.fold_in(rng, 6)
    for axis_at, parts in cuts:
        steps = jnp.exp(jax.random.uniform(jax.random.fold_in(own, axis_at), (parts,), jnp.float32, smallest / len(cuts), top_value / len(cuts)))
        level = level * jnp.repeat(steps, dims[axis_at] // parts).reshape([-1 if axis == axis_at else 1 for axis in range(len(dims))])
    return level


def profile(number_of, total, limit, skew):
    weights = [(1 << 20) // math.isqrt(rank ** skew) + 1 for rank in range(2, number_of + 1)]
    rest, given = total - limit - (number_of - 1), [1] * (number_of - 1)
    while rest > 0:
        movable = [i for i in range(number_of - 1) if given[i] < limit]
        whole, remaining = sum([weights[i] for i in movable]), rest
        for i in movable:
            extra = min(limit - given[i], max(1, remaining * weights[i] // whole), rest)
            given[i] = given[i] + extra
            rest = rest - extra
    return np.array([limit] + given)


def uneven(rng, amount, total, most, slope):
    if amount == 2:
        one = jax.random.randint(rng, (), max(1, total - most), min(most, total - 1) + 1)
        return jnp.stack([one, total - one])
    lengths = jnp.asarray(profile(amount, total, most, slope), jnp.int32)
    twos = (amount - 1) // 2
    giver, receiver = lengths[1:1 + 2 * twos:2], lengths[2:2 + 2 * twos:2]
    slack = jnp.minimum(giver - 1, most - receiver)
    shifted = jax.random.randint(jax.random.fold_in(rng, 1), (twos,), 0, 1 << 20) % (slack + 1)
    lengths = lengths.at[1:1 + 2 * twos:2].set(giver - shifted).at[2:2 + 2 * twos:2].set(receiver + shifted)
    return lengths[jax.random.permutation(jax.random.fold_in(rng, 2), amount)]


def bell_draw(own_key, dims, spread, most, shards=(), kind=jnp.bfloat16):
    entries = jax.random.normal(own_key, dims, jnp.float32) * spread
    if len(shards) > 0:
        entries = steps_of(own_key, dims, shards, -0.22, 0.18) * entries
    return jnp.clip(entries, min=-most, max=most).astype(kind)


def bell_draw_with(key, dims, scale, bound, split, heavy, kind=jnp.bfloat16):
    values = scale * jax.random.normal(key, dims, jnp.float32)
    if split:
        values = values * steps_of(key, dims, split, -0.22, 0.18)
    return jnp.clip(spiked(values, jax.random.fold_in(key, 3), *heavy), -bound, bound).astype(kind)


def setup_inputs(seed: int = 0) -> dict:
    keys = jax.random.split(jax.random.key(seed), 17)
    return {
        "inputs": bell_draw_with(keys[0], (TOKENS, D), 1.0, 6.0, ((0, 16),), (0, 1, 16, 2.0)),
        "segment_ids": jnp.searchsorted(jnp.cumsum(uneven(keys[1], SEGS, TOKENS, SEQ, 1)), jnp.arange(TOKENS), side="right").astype(jnp.int32),
        "cotangent": bell_draw_with(keys[2], (TOKENS, D), 1.0, 6.0, ((0, 16),), (0, 1, 16, 2.0)),
        "branch_weight": bell_draw(keys[3], (2, D, R), D ** -0.5, 0.125, ((1, 16), (2, 2))),
        "out_weight": bell_draw(keys[4], (R, D), (R // 2) ** -0.5, 0.15625, ((0, 2), (1, 16))),
        "ffw_in": bell_draw(keys[5], (2, D, FF), D ** -0.5, 0.125, ((1, 16), (2, 2))),
        "ffw_out": bell_draw(keys[6], (FF, D), (FF // 2) ** -0.5, 0.09375, ((0, 2), (1, 16))),
        "norm_scales": jnp.clip(jax.random.uniform(keys[7], (2, D), jnp.float32, -0.5, 0.5), -0.5, 0.5),
        "branch_bias": bell_draw(keys[8], (2, R), 0.5, 3.0, ((1, 2),), jnp.float32),
        "conv_weight": bell_draw(keys[9], (CONV, R), 0.5, 3.0, ((1, 2),), jnp.float32),
        "conv_bias": bell_draw(keys[10], (R,), 0.5, 3.0, ((0, 2),), jnp.float32),
        "gate_weights": bell_draw(keys[11], (2, HEADS, BLOCK, BLOCK), BLOCK ** -0.5, 0.375, ((1, 2),)),
        "gate_bias": bell_draw(keys[12], (2, R), 0.5, 3.0, ((1, 2),), jnp.float32),
        "decay_param": jnp.clip(-10.5 + 5.5 * jax.random.uniform(keys[13], (R,), jnp.float32) ** steps_of(keys[13], (R,), ((0, 2),), -0.2, 0.2), -10.5, -5.0),
        "out_bias": bell_draw(keys[14], (2, D), 0.5, 3.0, (), jnp.float32),
        "ffw_bias": bell_draw(keys[15], (2, FF), 0.5, 3.0, ((1, 2),), jnp.float32),
    }


@jax.custom_vjp
def low(v):
    return lax.optimization_barrier(v.astype(jnp.bfloat16)).astype(jnp.float32)

@jax.custom_vjp
def low_back(v):
    return v

def low_keep(v):
    return (low(v), None)

def low_pass(kept, grad):
    return (grad,)

def back_keep(v):
    return (v, None)

def back_low(kept, grad):
    return (low(grad),)
low.defvjp(low_keep, low_pass)
low_back.defvjp(back_keep, back_low)
HIGHEST = lax.Precision.HIGHEST

def rms_norm(values, scaling):
    inverse = lax.rsqrt(lax.optimization_barrier(jnp.mean(values * values, axis=-1, keepdims=True)) + 1e-06)
    return values * inverse * (1.0 + scaling)

def gelu_tanh(values):
    return jax.nn.gelu(values, approximate=True)

def lru_inputs(gate_decay, gate_input, conv_in, decay_in, resets):
    log_decay = -8.0 * jax.nn.sigmoid(gate_decay) * jax.nn.softplus(decay_in)
    decay = jnp.exp(log_decay)
    multiplier = jnp.sqrt(jnp.maximum(-jnp.expm1(2.0 * log_decay), 0.001))
    multiplier = jnp.where(resets, 1.0, multiplier)
    keep_rate = jnp.where(resets, 0.0, decay)
    return (keep_rate, conv_in * jax.nn.sigmoid(gate_input) * multiplier)

def recurrence(keep_rate, drive_in):

    def advance(carried, element):
        carried = element[0] * carried + element[1]
        return (carried, carried)
    _, states = lax.scan(advance, jnp.zeros((keep_rate.shape[1],), jnp.float32), (keep_rate, drive_in))
    return states

def shift_rows(values, offset):
    return jnp.concatenate([jnp.zeros((offset, values.shape[1]), jnp.float32), values[:values.shape[0] - offset]], axis=0)

def reference(inputs, segment_ids, cotangent, branch_weight, out_weight, ffw_in, ffw_out, norm_scales, branch_bias, conv_weight, conv_bias, gate_weights, gate_bias, decay_param, out_bias, ffw_bias):
    row_count = inputs.shape[0]
    seg_ids = segment_ids.astype(jnp.int32)

    def lagged_ids(offset):
        return jnp.concatenate([jnp.full((offset,), -1, jnp.int32), seg_ids[:row_count - offset]])
    resets = (seg_ids != lagged_ids(1))[:, None]
    matches = [(lagged_ids(offset) == seg_ids).astype(jnp.float32)[:, None] for offset in range(CONV)]

    def forward(source, branch_mat, out_mat, ffw_in_mat, ffw_out_mat, scales, branch_shift, conv_taps, conv_shift, gate_mats, gate_shift, decay_raw, out_shift, ffw_shift):
        normed = low(rms_norm(source, scales[0]))
        branches = low_back(jnp.einsum('nd,kdr->knr', normed, branch_mat, precision=HIGHEST) + branch_shift[:, None, :])
        conv_sum = jnp.zeros_like(branches[0]) + conv_shift
        for offset in range(CONV):
            conv_sum = conv_sum + conv_taps[offset] * matches[offset] * shift_rows(branches[0], offset)
        conv = low(conv_sum)
        blocks = conv.reshape(row_count, HEADS, BLOCK)
        gate_pre = jnp.einsum('nhb,ghbc->gnhc', blocks, gate_mats, precision=HIGHEST).reshape(2, row_count, R) + gate_shift[:, None, :]
        gate_pre = low_back(gate_pre)
        keep_rate, drive_in = lru_inputs(gate_pre[0], gate_pre[1], conv, decay_raw, resets)
        states = recurrence(keep_rate, drive_in)
        mixed_in = low(states * gelu_tanh(branches[1]))
        residual = source + low_back(jnp.dot(mixed_in, out_mat, precision=HIGHEST) + out_shift[0])
        normed_two = low(rms_norm(residual, scales[1]))
        gate_up = low_back(jnp.einsum('nd,kdf->knf', normed_two, ffw_in_mat, precision=HIGHEST) + ffw_shift[:, None, :])
        hidden = low(gelu_tanh(gate_up[0]) * gate_up[1])
        return residual + jnp.dot(hidden, ffw_out_mat, precision=HIGHEST) + out_shift[1]
    floats = [value.astype(jnp.float32) for value in (inputs, branch_weight, out_weight, ffw_in, ffw_out, norm_scales, branch_bias, conv_weight, conv_bias, gate_weights, gate_bias, decay_param, out_bias, ffw_bias)]
    output, pullback = jax.vjp(forward, *floats)
    gradients = pullback(cotangent.astype(jnp.float32))
    return (output, gradients[0], gradients[1], gradients[2], gradients[3], gradients[4], gradients[5], gradients[6], gradients[7], gradients[8], gradients[9], gradients[10], gradients[11], gradients[12], gradients[13])
```

```python
import functools

import jax
import jax.numpy as jnp
from jax import lax
from jax.experimental import pallas as pl
from jax.experimental.pallas import tpu as pltpu
from jax.sharding import Mesh
from jax.sharding import PartitionSpec as P

INNER = 4
DP = ("o", "i")
EPS = 1e-06
F32 = jnp.float32
BF16 = jnp.bfloat16


def swap(value):
    return lax.ppermute(value, "tensor", [(0, 1), (1, 0)])


def ring(value):
    count = lax.axis_size("o")
    return lax.ppermute(value, "o", [(k, (k + 1) % count) for k in range(count)])


def from_behind(value, steps):
    count = lax.axis_size(DP)
    first, last = max(0, -steps), min(count, count - steps)
    return lax.ppermute(value, DP, [(k, k + steps) for k in range(first, last)])


def sum_over_all(value):
    count, bit = lax.axis_size(DP), 1
    while bit < count:
        value = value + lax.ppermute(value, DP, [(k, k ^ bit) for k in range(count)])
        bit *= 2
    return value


def half_of(value, which):
    rows = value.shape[0] // 2
    return lax.dynamic_slice_in_dim(value, which * rows, rows, 0)


def join_halves(own, other, core):
    first = jnp.where(core == 0, own, other)
    second = jnp.where(core == 0, other, own)
    return jnp.concatenate([first, second], axis=0)


def scan_kernel(reverse, keep_ref, drive_ref, cum_ref, state_ref):
    rows, width = keep_ref.shape
    groups = rows // 8
    place = lax.broadcasted_iota(jnp.int32, (8, width), 0)

    def step(k, carried):
        before_a, before_b = carried
        group = groups - 1 - k if reverse else k
        at = pl.ds(pl.multiple_of(group * 8, 8), 8)
        a, b = keep_ref[at, :], drive_ref[at, :]
        for d in (1, 2, 4):
            far_a = pltpu.roll(a, 8 - d if reverse else d, 0)
            far_b = pltpu.roll(b, 8 - d if reverse else d, 0)
            inside = place < 8 - d if reverse else place >= d
            b = jnp.where(inside, a * far_b + b, b)
            a = jnp.where(inside, a * far_a, a)
        b = a * before_b + b
        a = a * before_a
        cum_ref[at, :] = a
        state_ref[at, :] = b
        edge = slice(0, 1) if reverse else slice(7, 8)
        return (a[edge], b[edge])

    lax.fori_loop(
        0, groups, step, (jnp.ones((1, width), F32), jnp.zeros((1, width), F32))
    )


def local_scan(keep, drive, reverse):
    rows, width = keep.shape
    block = 256
    spec = pl.BlockSpec((rows, block), lambda j: (0, j))
    shape = jax.ShapeDtypeStruct((rows, width), F32)
    return pl.pallas_call(
        functools.partial(scan_kernel, reverse),
        grid=(width // block,),
        in_specs=[spec, spec],
        out_specs=[spec, spec],
        out_shape=[shape, shape],
        cost_estimate=pl.CostEstimate(
            flops=20 * rows * width, bytes_accessed=16 * rows * width, transcendentals=0
        ),
    )(keep, drive)


def entering(decay, state, reverse):
    count, index = lax.axis_size(DP), lax.axis_index(DP)
    every = lax.all_gather(jnp.stack([decay, state]), DP)
    carried = jnp.zeros_like(state)
    for k in range(count):
        at = count - 1 - k if reverse else k
        reached = at > index if reverse else at < index
        carried = jnp.where(reached, every[at, 0] * carried + every[at, 1], carried)
    return carried


def gelu_tanh(values):
    return jax.nn.gelu(values, approximate=True)


def geglu(gate_vals, up_vals):
    return gelu_tanh(gate_vals) * up_vals


def lru_inputs(gate_decay, gate_input, conv_in, decay_in, resets):
    log_decay = -8.0 * jax.nn.sigmoid(gate_decay) * jax.nn.softplus(decay_in)
    decay = jnp.exp(log_decay)
    multiplier = jnp.sqrt(jnp.maximum(-jnp.expm1(2.0 * log_decay), 0.001))
    multiplier = jnp.where(resets, 1.0, multiplier)
    keep_rate = jnp.where(resets, 0.0, decay)
    return (keep_rate, conv_in * jax.nn.sigmoid(gate_input) * multiplier)


def norm_back(values, scaling, delta):
    inverse = lax.rsqrt(jnp.mean(values * values, axis=-1, keepdims=True) + EPS)
    unit = values * inverse
    scaled = delta * (1.0 + scaling)
    moved = inverse * (scaled - unit * jnp.mean(scaled * unit, axis=-1, keepdims=True))
    return moved, jnp.sum(delta * unit, axis=0)


def rms_norm(values, scaling):
    inverse = lax.rsqrt(jnp.mean(values * values, axis=-1, keepdims=True) + EPS)
    return values * inverse * (1.0 + scaling)


def dot(a, b, contract):
    return lax.dot_general(a, b, ((contract[0], contract[1]), ((), ())), preferred_element_type=F32)


def mm(a, b):
    return dot(a, b, ((1,), (0,)))


def mm_nt(a, b):
    return dot(a, b, ((1,), (1,)))


def mm_tn(a, b):
    return dot(a, b, ((0,), (0,)))


def gather_slots(half):
    slots = []
    for k in range(lax.axis_size("o")):
        half = ring(half) if k else half
        slots.append(jnp.concatenate([half, swap(half)], axis=0))
    return slots


def reduce_slots(parts):
    count = len(parts)
    rows = parts[0].shape[0] // 2

    def both(part):
        return part[:rows] + swap(part[rows:].astype(BF16)).astype(F32)

    if count == 1:
        return both(parts[0])
    total = both(parts[1])
    for k in range(1, count):
        total = both(parts[(k + 1) % count]) + ring(total.astype(BF16)).astype(F32)
    return total


def spread(value, axis):
    return lax.all_to_all(value, "o", axis, axis, tiled=True)


def per_device(
    inputs,
    segment_ids,
    cotangent,
    branch_weight,
    out_weight,
    ffw_in,
    ffw_out,
    norm_scales,
    branch_bias,
    conv_weight,
    conv_bias,
    gate_weights,
    gate_bias,
    decay_param,
    out_bias,
    ffw_bias,
):
    outer, inner = lax.axis_size("o"), lax.axis_size("i")
    count = outer * inner
    core, along = lax.axis_index("tensor"), lax.axis_index("o")
    tok_rows, width = inputs.shape
    part_width = width // count
    hidden_half = ffw_out.shape[0]
    hidden_part = hidden_half // outer
    taps_count = conv_weight.shape[0]
    rim_rows = taps_count - 1
    heads_half, block_size = gate_weights.shape[1], gate_weights.shape[2]
    width_half = heads_half * block_size

    branch_x_full = lax.all_gather(branch_weight[0], DP, axis=0, tiled=True)
    branch_y_full = lax.all_gather(branch_weight[1], DP, axis=0, tiled=True)
    out_full_t = lax.all_gather(out_weight.T, DP, axis=0, tiled=True)
    in_parts = (
        ffw_in.reshape(2, part_width, outer, hidden_part)
        .transpose(2, 1, 0, 3)
        .reshape(outer, part_width, 2 * hidden_part)
    )
    out_parts = ffw_out.reshape(outer, hidden_part, part_width).transpose(0, 2, 1)
    ffw_in_full = lax.all_gather(spread(in_parts, 0), "i", axis=1, tiled=True).reshape(
        width, 2 * hidden_part
    )
    ffw_out_full_t = lax.all_gather(spread(out_parts, 0), "i", axis=1, tiled=True).reshape(
        width, hidden_part
    )
    cot_slots = gather_slots(half_of(cotangent, core))

    seg_marks = (segment_ids + 1).astype(F32)
    source_half = half_of(inputs, core).astype(F32)
    normed_low = rms_norm(inputs.astype(F32), norm_scales[0]).astype(BF16)
    branch_x = mm(normed_low, branch_x_full) + branch_bias[0]
    branch_y = mm(normed_low, branch_y_full) + branch_bias[1]
    rim_values, rim_marks = from_behind(
        (branch_x[tok_rows - rim_rows :], seg_marks[tok_rows - rim_rows :]), 1
    )
    padded_branch = jnp.concatenate([rim_values, branch_x], axis=0)
    padded_marks = jnp.concatenate([rim_marks, seg_marks], axis=0)
    resets = (seg_marks != padded_marks[rim_rows - 1 : rim_rows - 1 + tok_rows])[:, None]
    conv_out = jnp.zeros_like(branch_x) + conv_bias
    shifted_rows = []
    for offset in range(taps_count):
        matches = (
            padded_marks[rim_rows - offset : rim_rows - offset + tok_rows] == seg_marks
        ).astype(F32)[:, None]
        shifted = padded_branch[rim_rows - offset : rim_rows - offset + tok_rows] * matches
        shifted_rows.append(shifted)
        conv_out = conv_out + conv_weight[offset] * shifted
    conv_low = conv_out.astype(BF16)
    conv_float = conv_low.astype(F32)
    conv_blocks = conv_low.reshape(tok_rows, heads_half, block_size)
    gate_pre = (
        jnp.einsum(
            "thb,ghbc->gthc", conv_blocks, gate_weights, preferred_element_type=F32
        ).reshape(2, tok_rows, width_half)
        + gate_bias[:, None, :]
    )

    def lru_local(gate_decay, gate_input, conv_in, decay_in):
        return lru_inputs(gate_decay, gate_input, conv_in, decay_in, resets)

    (keep_rate, drive_in), lru_back = jax.vjp(
        lru_local, gate_pre[0], gate_pre[1], conv_float, decay_param
    )
    cumulative, local_state = local_scan(keep_rate, drive_in, False)
    carry_in = entering(cumulative[tok_rows - 1], local_state[tok_rows - 1], False)
    states = local_state + cumulative * carry_in
    branch_act, gelu_back = jax.vjp(gelu_tanh, branch_y)
    mixed_in = (states * branch_act).astype(BF16)
    mixed_part = mm_nt(mixed_in, out_full_t)
    residual = (
        source_half
        + half_of(mixed_part, core)
        + swap(half_of(mixed_part, 1 - core))
        + out_bias[0]
    )

    normed_slots = gather_slots(rms_norm(residual, norm_scales[1]).astype(BF16))
    bias_part = lax.dynamic_slice_in_dim(ffw_bias, along * hidden_part, hidden_part, 1)
    bias_row = bias_part.reshape(2 * hidden_part)
    hidden_slots, delta_slots, result_parts, delta_parts = [], [], [], []
    for normed_two, cot in zip(normed_slots, cot_slots):
        gate_up = mm(normed_two, ffw_in_full) + bias_row
        hidden, hidden_back = jax.vjp(geglu, gate_up[:, :hidden_part], gate_up[:, hidden_part:])
        hidden_low = hidden.astype(BF16)
        delta_gate_up = jnp.concatenate(hidden_back(mm(cot, ffw_out_full_t)), axis=1).astype(BF16)
        hidden_slots.append(hidden_low)
        delta_slots.append(delta_gate_up)
        delta_parts.append(mm_nt(delta_gate_up, ffw_in_full))
    delta_normed_two = reduce_slots(delta_parts)
    for hidden_low in hidden_slots:
        result_parts.append(mm_nt(hidden_low, ffw_out_full_t))
    normed_all, cot_all = jnp.concatenate(normed_slots), jnp.concatenate(cot_slots)
    hidden_all, delta_all = jnp.concatenate(hidden_slots), jnp.concatenate(delta_slots)

    def sum_inner(grad):
        rows = grad.reshape(outer, inner, part_width, -1).transpose(1, 0, 2, 3)
        own = lax.psum_scatter(
            rows.reshape(width, -1).astype(BF16), "i", scatter_dimension=0, tiled=True
        )
        return spread(own.reshape(outer, part_width, -1), 0)

    grad_ffw_out_t = sum_inner(mm_tn(cot_all, hidden_all))
    ffw_out_grad = (
        grad_ffw_out_t.transpose(0, 2, 1).reshape(hidden_half, part_width).astype(F32)
    )
    grad_ffw_in = sum_inner(mm_tn(normed_all, delta_all)).reshape(
        outer, part_width, 2, hidden_part
    )
    ffw_in_grad = (
        grad_ffw_in.transpose(2, 1, 0, 3).reshape(2, part_width, hidden_half).astype(F32)
    )
    bias_sum = jnp.sum(delta_all, axis=0, dtype=F32).reshape(2, hidden_part)
    grad_ffw_bias = lax.dynamic_update_slice_in_dim(
        jnp.zeros((2, hidden_half), F32), bias_sum, along * hidden_part, 1
    )
    result_half = residual + reduce_slots(result_parts) + out_bias[1]
    result = join_halves(result_half, swap(result_half), core)

    cot_half = half_of(cotangent, core).astype(F32)
    delta_res_norm, grad_scale_two = norm_back(residual, norm_scales[1], delta_normed_two)
    delta_residual = cot_half + delta_res_norm
    delta_half = delta_residual.astype(BF16)
    delta_mixed = join_halves(delta_half, swap(delta_half), core)
    delta_mixed_in = mm(delta_mixed, out_full_t)
    grad_out_t = lax.psum_scatter(
        mm_tn(delta_mixed, mixed_in).astype(BF16), DP, scatter_dimension=0, tiled=True
    )
    delta_states = delta_mixed_in * branch_act
    (delta_branch_y,) = gelu_back(delta_mixed_in * states)
    delta_y_low = delta_branch_y.astype(BF16)
    grad_branch_y = lax.psum_scatter(
        mm_tn(normed_low, delta_y_low).astype(BF16), DP, scatter_dimension=0, tiled=True
    )
    alpha_next = jnp.concatenate([keep_rate[1:], jnp.ones((1, width_half), F32)], axis=0)
    suffix, local_adjoint = local_scan(alpha_next, delta_states, True)
    leaving = entering(keep_rate[0] * suffix[0], keep_rate[0] * local_adjoint[0], True)
    adjoint = local_adjoint + suffix * leaving
    states_before = jnp.concatenate([carry_in[None, :], states[: tok_rows - 1]], axis=0)
    delta_gate_decay, delta_gate_input, delta_conv_direct, grad_decay = lru_back(
        (adjoint * states_before, adjoint)
    )
    delta_gates = jnp.stack([delta_gate_decay, delta_gate_input]).astype(BF16)
    delta_blocks = delta_gates.reshape(2, tok_rows, heads_half, block_size)
    grad_gate_weights = jnp.einsum(
        "thb,gthc->ghbc", conv_blocks, delta_blocks, preferred_element_type=F32
    )
    gate_rows = (
        grad_gate_weights.reshape(2, heads_half, count, block_size // count, block_size)
        .transpose(2, 0, 1, 3, 4)
        .reshape(2 * heads_half * block_size, block_size)
        .astype(BF16)
    )
    gate_grad = lax.psum_scatter(gate_rows, DP, scatter_dimension=0, tiled=True)
    gate_grad = gate_grad.reshape(2, heads_half, block_size // count, block_size).astype(F32)
    grad_gate_bias = jnp.sum(delta_gates, axis=1, dtype=F32)
    delta_conv = delta_conv_direct + jnp.einsum(
        "gthc,ghbc->thb", delta_blocks, gate_weights, preferred_element_type=F32
    ).reshape(tok_rows, width_half)
    rim_delta, rim_next_marks = from_behind((delta_conv[:rim_rows], seg_marks[:rim_rows]), -1)
    padded_delta = jnp.concatenate([delta_conv, rim_delta], axis=0)
    next_marks = jnp.concatenate([seg_marks, rim_next_marks], axis=0)
    delta_branch_x = jnp.zeros_like(delta_conv)
    conv_weight_rows = []
    for offset in range(taps_count):
        matches = (next_marks[offset : offset + tok_rows] == seg_marks).astype(F32)[:, None]
        delta_branch_x = (
            delta_branch_x
            + conv_weight[offset] * padded_delta[offset : offset + tok_rows] * matches
        )
        conv_weight_rows.append(jnp.sum(delta_conv * shifted_rows[offset], axis=0))
    grad_conv_bias = jnp.sum(delta_conv, axis=0)
    delta_x_low = delta_branch_x.astype(BF16)
    grad_branch_x = lax.psum_scatter(
        mm_tn(normed_low, delta_x_low).astype(BF16), DP, scatter_dimension=0, tiled=True
    )
    delta_part = mm_nt(delta_x_low, branch_x_full) + mm_nt(delta_y_low, branch_y_full)
    delta_normed = half_of(delta_part, core) + swap(
        half_of(delta_part, 1 - core).astype(BF16)
    ).astype(F32)
    delta_source_norm, grad_scale_one = norm_back(source_half, norm_scales[0], delta_normed)
    grad_half = delta_residual + delta_source_norm
    input_grad = join_halves(grad_half, swap(grad_half), core)

    halves = jnp.stack(
        [
            grad_scale_one,
            grad_scale_two,
            jnp.sum(delta_half, axis=0, dtype=F32),
            jnp.sum(cot_half, axis=0),
        ]
    )
    halves = halves + swap(halves)
    flat = [
        halves.reshape(-1),
        jnp.sum(delta_x_low, axis=0, dtype=F32),
        jnp.sum(delta_y_low, axis=0, dtype=F32),
        *conv_weight_rows,
        grad_conv_bias,
        grad_gate_bias.reshape(-1),
        grad_decay,
        grad_ffw_bias.reshape(-1),
    ]
    small = sum_over_all(jnp.concatenate(flat).reshape(-1, 128)).reshape(-1)
    at = 0
    taken = []
    for shape in (
        (2, width),
        (2, width),
        (2, width_half),
        (taps_count, width_half),
        (width_half,),
        (2, width_half),
        (width_half,),
        (2, hidden_half),
    ):
        size = 1
        for n in shape:
            size *= n
        taken.append(small[at : at + size].reshape(shape))
        at += size
    scales, out_bias_grad, branch_bias_grad, taps_grad, conv_bias_grad, gate_bias_grad, decay_grad, ffw_bias_grad = taken
    return (
        result,
        input_grad,
        jnp.stack([grad_branch_x, grad_branch_y]).astype(F32),
        grad_out_t.T.astype(F32),
        ffw_in_grad,
        ffw_out_grad,
        scales,
        branch_bias_grad,
        taps_grad,
        conv_bias_grad,
        gate_grad,
        gate_bias_grad,
        decay_grad,
        out_bias_grad,
        ffw_bias_grad,
    )


def solution(mesh):
    count = mesh.shape["dp"]
    grid = Mesh(
        mesh.devices.reshape(count // INNER, INNER, mesh.shape["tensor"]), ("o", "i", "tensor")
    )
    in_specs = (
        P(DP, None),
        P(DP),
        P(DP, None),
        P(None, DP, "tensor"),
        P("tensor", DP),
        P(None, DP, "tensor"),
        P("tensor", DP),
        P(),
        P(None, "tensor"),
        P(None, "tensor"),
        P("tensor"),
        P(None, "tensor", None, None),
        P(None, "tensor"),
        P("tensor"),
        P(),
        P(None, "tensor"),
    )
    out_specs = (
        P(DP, None),
        P(DP, None),
        P(None, DP, "tensor"),
        P("tensor", DP),
        P(None, DP, "tensor"),
        P("tensor", DP),
        P(),
        P(None, "tensor"),
        P(None, "tensor"),
        P("tensor"),
        P(None, "tensor", DP, None),
        P(None, "tensor"),
        P("tensor"),
        P(),
        P(None, "tensor"),
    )
    return jax.shard_map(
        per_device, mesh=grid, in_specs=in_specs, out_specs=out_specs, check_vma=False
    )
```

```python
import functools

import jax
import jax.numpy as jnp
from jax import lax
from jax.experimental import pallas as pl
from jax.experimental.pallas import tpu as pltpu
from jax.sharding import Mesh
from jax.sharding import PartitionSpec as P


INNER = 4
DP = ("o", "i")
EPS = 1e-06
F32 = jnp.float32
BF16 = jnp.bfloat16


def swap(value):
    return lax.ppermute(value, "tensor", [(0, 1), (1, 0)])


def ring(value):
    count = lax.axis_size("o")
    return lax.ppermute(value, "o", [(k, (k + 1) % count) for k in range(count)])


def from_behind(value, steps):
    count = lax.axis_size(DP)
    first, last = max(0, -steps), min(count, count - steps)
    return lax.ppermute(value, DP, [(k, k + steps) for k in range(first, last)])


def sum_over_all(value):
    count, bit = lax.axis_size(DP), 1
    while bit < count:
        value = value + lax.ppermute(value, DP, [(k, k ^ bit) for k in range(count)])
        bit *= 2
    return value


def half_of(value, which):
    rows = value.shape[0] // 2
    return lax.dynamic_slice_in_dim(value, which * rows, rows, 0)


def join_halves(own, other, core):
    first = jnp.where(core == 0, own, other)
    second = jnp.where(core == 0, other, own)
    return jnp.concatenate([first, second], axis=0)


def scan_kernel(reverse, keep_ref, drive_ref, cum_ref, state_ref):
    rows, width = keep_ref.shape
    groups = rows // 8
    place = lax.broadcasted_iota(jnp.int32, (8, width), 0)

    def step(k, carried):
        before_a, before_b = carried
        group = groups - 1 - k if reverse else k
        at = pl.ds(pl.multiple_of(group * 8, 8), 8)
        a, b = keep_ref[at, :], drive_ref[at, :]
        for d in (1, 2, 4):
            far_a = pltpu.roll(a, 8 - d if reverse else d, 0)
            far_b = pltpu.roll(b, 8 - d if reverse else d, 0)
            inside = place < 8 - d if reverse else place >= d
            b = jnp.where(inside, a * far_b + b, b)
            a = jnp.where(inside, a * far_a, a)
        b = a * before_b + b
        a = a * before_a
        cum_ref[at, :] = a
        state_ref[at, :] = b
        edge = slice(0, 1) if reverse else slice(7, 8)
        return (a[edge], b[edge])

    lax.fori_loop(
        0, groups, step, (jnp.ones((1, width), F32), jnp.zeros((1, width), F32))
    )


def local_scan(keep, drive, reverse):
    rows, width = keep.shape
    block = 256
    spec = pl.BlockSpec((rows, block), lambda j: (0, j))
    shape = jax.ShapeDtypeStruct((rows, width), F32)
    return pl.pallas_call(
        functools.partial(scan_kernel, reverse),
        grid=(width // block,),
        in_specs=[spec, spec],
        out_specs=[spec, spec],
        out_shape=[shape, shape],
        cost_estimate=pl.CostEstimate(
            flops=20 * rows * width, bytes_accessed=16 * rows * width, transcendentals=0
        ),
    )(keep, drive)


MESH_ID = pl.DeviceIdType.MESH
VMEM = pl.BlockSpec(memory_space=pltpu.VMEM)
ANY = pl.BlockSpec(memory_space=pl.ANY)


def enter_kernel(outer, inner, reverse, ends_ref, carry_ref, every, send_sem, recv_sem):
    count = outer * inner
    core = lax.axis_index("tensor")
    me = lax.axis_index("o") * inner + lax.axis_index("i")
    barrier = pltpu.get_barrier_semaphore()
    for k in range(1, count):
        peer = lax.rem(me + k, count)
        to = (peer // inner, lax.rem(peer, inner), core)
        pl.semaphore_signal(barrier, inc=1, device_id=to, device_id_type=MESH_ID)
    pl.semaphore_wait(barrier, count - 1)

    def copy(k, mine):
        peer = lax.rem(me + k, count)
        return pltpu.make_async_remote_copy(
            src_ref=ends_ref,
            dst_ref=every.at[me if mine else peer],
            send_sem=send_sem.at[k],
            recv_sem=recv_sem.at[me if mine else peer],
            device_id=(peer // inner, lax.rem(peer, inner), core),
            device_id_type=MESH_ID,
        )

    for k in range(1, count):
        copy(k, True).start()
    for k in range(1, count):
        copy(k, False).wait_recv()
    carried = jnp.zeros((1, ends_ref.shape[1]), F32)
    for k in range(count):
        at = count - 1 - k if reverse else k
        reached = at > me if reverse else at < me
        block = every[at]
        carried = jnp.where(reached, block[0:1] * carried + block[1:2], carried)
    carry_ref[...] = carried
    for k in range(1, count):
        copy(k, True).wait_send()


def entering(decay, state, reverse):
    outer, inner = lax.axis_size("o"), lax.axis_size("i")
    count, width = outer * inner, state.shape[0]
    carried = pl.pallas_call(
        functools.partial(enter_kernel, outer, inner, reverse),
        in_specs=[VMEM],
        out_specs=VMEM,
        out_shape=jax.ShapeDtypeStruct((1, width), F32),
        scratch_shapes=[
            pltpu.VMEM((count, 2, width), F32),
            pltpu.SemaphoreType.DMA((count,)),
            pltpu.SemaphoreType.DMA((count,)),
        ],
        compiler_params=pltpu.CompilerParams(
            collective_id=2 if reverse else 1, has_side_effects=True
        ),
    )(jnp.stack([decay, state]))
    return carried[0]


def gather_kernel(outer, groups, parts, *refs):
    own, send = refs[:groups], refs[groups : groups + parts]
    refs = refs[groups + parts :]
    full, got = refs[:groups], refs[groups : groups + parts]
    line_send, line_recv, side_send, side_recv, half_send, half_recv, part_send, part_recv, local = refs[
        groups + parts :
    ]
    o, i, core = lax.axis_index("o"), lax.axis_index("i"), lax.axis_index("tensor")
    sides = (i + 1 - 2 * lax.rem(i, 2), lax.rem(i + 2, 4))
    far = lax.rem(sides[0] + 2, 4)
    lanes = own[0].shape[1] // 2

    barrier = pltpu.get_barrier_semaphore()
    for k in range(1, outer):
        pl.semaphore_signal(
            barrier, inc=1, device_id=(lax.rem(o + k, outer), i, core), device_id_type=MESH_ID
        )
    for side in sides:
        pl.semaphore_signal(barrier, inc=1, device_id=(o, side, core), device_id_type=MESH_ID)
    pl.semaphore_wait(barrier, outer + 1)

    def remote(src, dst, send_sem, recv_sem, to):
        return pltpu.make_async_remote_copy(
            src_ref=src,
            dst_ref=dst,
            send_sem=send_sem,
            recv_sem=recv_sem,
            device_id=to,
            device_id_type=MESH_ID,
        )

    def block(g, k, j):
        return full[g].at[k, j]

    def along_line(g, k, mine, step):
        return remote(
            own[g] if mine else block(g, k, i),
            block(g, k, i),
            line_send.at[g, k, step],
            line_recv.at[g, k],
            (o + 2 * step - 1, i, core),
        )

    def to_side(g, k, mine, side):
        return remote(
            own[g] if mine else block(g, k, i),
            block(g, k, i),
            side_send.at[g, k, side],
            side_recv.at[g, k, side],
            (o, sides[side], core),
        )

    def from_side(g, k, side):
        return remote(
            block(g, k, sides[side]),
            block(g, k, sides[side]),
            side_send.at[g, k, side],
            side_recv.at[g, k, side],
            (o, sides[side], core),
        )

    def half(g, k, side, to):
        part = full[g].at[k, side, :, pl.ds(lanes * to, lanes)]
        return remote(
            part, part, half_send.at[g, k, to], half_recv.at[g, k, to], (o, sides[to], core)
        )

    def visit(first, then):
        first(o)
        for d in range(1, outer):
            pl.when(o - d >= 0)(functools.partial(then, o - d, True))
            pl.when(o + d < outer)(functools.partial(then, o + d, False))

    for g in range(groups):
        pltpu.make_async_copy(own[g], block(g, o, i), local.at[g]).start()
        pl.when(o + 1 < outer)(lambda g=g: along_line(g, o, True, 1).start())
        pl.when(o > 0)(lambda g=g: along_line(g, o, True, 0).start())
        for side in range(2):
            to_side(g, o, True, side).start()

    def pass_on(k, from_left):
        for g in range(groups):
            along_line(g, k, False, 0).wait_recv()
            if from_left:
                pl.when(o + 1 < outer)(lambda g=g: along_line(g, k, False, 1).start())
            else:
                pl.when(o > 0)(lambda g=g: along_line(g, k, False, 0).start())
            for side in range(2):
                to_side(g, k, False, side).start()

    visit(lambda k: None, pass_on)

    def part(p, k, mine):
        peer = lax.rem(o + k, outer)
        return remote(
            send[p].at[peer],
            got[p].at[o if mine else peer],
            part_send.at[p, k],
            part_recv.at[p, o if mine else peer],
            (peer, i, core),
        )

    for p in range(parts):
        pltpu.make_async_copy(send[p].at[o], got[p].at[o], local.at[groups + p]).start()
        for k in range(1, outer):
            part(p, k, True).start()

    def turn(k, _=None):
        for g in range(groups):
            for side in range(2):
                from_side(g, k, side).wait_recv()
                half(g, k, sides[side], 1 - side).start()

    visit(turn, turn)

    def finish(k, _=None):
        for g in range(groups):
            for side in range(2):
                half(g, k, far, side).wait_recv()

    visit(finish, finish)
    for p in range(parts):
        for k in range(1, outer):
            part(p, k, False).wait_recv()

    def sent(k, from_left):
        for g in range(groups):
            if from_left is None or from_left:
                pl.when(o + 1 < outer)(lambda g=g: along_line(g, k, False, 1).wait_send())
            if not from_left:
                pl.when(o > 0)(lambda g=g: along_line(g, k, False, 0).wait_send())
            for side in range(2):
                to_side(g, k, False, side).wait_send()
                half(g, k, sides[side], 1 - side).wait_send()

    visit(functools.partial(sent, from_left=None), sent)
    for p in range(parts):
        for k in range(1, outer):
            part(p, k, True).wait_send()
    for g in range(groups):
        pltpu.make_async_copy(own[g], block(g, o, i), local.at[g]).wait()
    for p in range(parts):
        pltpu.make_async_copy(send[p].at[o], got[p].at[o], local.at[groups + p]).wait()


def gather_weights(own, send):
    outer, inner = lax.axis_size("o"), lax.axis_size("i")
    groups, parts = len(own), len(send)
    dma = pltpu.SemaphoreType.DMA
    out_shape = [jax.ShapeDtypeStruct((outer, inner, *w.shape), w.dtype) for w in own] + [
        jax.ShapeDtypeStruct(w.shape, w.dtype) for w in send
    ]
    result = pl.pallas_call(
        functools.partial(gather_kernel, outer, groups, parts),
        in_specs=[VMEM] * (groups + parts),
        out_specs=[ANY] * (groups + parts),
        out_shape=out_shape,
        scratch_shapes=[
            dma((groups, outer, 2)),
            dma((groups, outer)),
            dma((groups, outer, 2)),
            dma((groups, outer, 2)),
            dma((groups, outer, 2)),
            dma((groups, outer, 2)),
            dma((parts, outer)),
            dma((parts, outer)),
            dma((groups + parts,)),
        ],
        compiler_params=pltpu.CompilerParams(collective_id=0, has_side_effects=True),
    )(*own, *send)
    full = [w.reshape(-1, w.shape[-1]) for w in result[:groups]]
    return full, result[groups:]


def grads_kernel(plan, added, *refs):
    out_ref = refs[-1]
    inner, _, rows, _ = out_ref.shape
    take = rows - added
    if added:
        out_ref[:, 0, take:, :] = refs[-2][0]
    refs = iter(refs)
    at = 0
    for terms in plan:
        total = None
        for pieces in terms:
            a = [next(refs)[...] for _ in range(pieces)]
            term = mm_tn(jnp.concatenate(a) if pieces > 1 else a[0], next(refs)[...])
            total = term if total is None else total + term
        size = total.shape[1]
        out_ref[:, 0, :take, at : at + size] = total.astype(BF16).reshape(inner, take, size)
        at += size


def grads_rows(columns, extra=None):
    outer, inner = lax.axis_size("o"), lax.axis_size("i")
    width = columns[0][0][0][0].shape[1]
    block = width // outer
    rows = block // inner
    size = sum(terms[0][1].shape[1] for terms in columns)
    tokens = sum(b.shape[0] for _, b in columns[0])
    added = 0 if extra is None else extra.shape[2]
    if block % 128:
        whole = [
            sum(mm_tn(jnp.concatenate(a), b) for a, b in terms).astype(BF16) for terms in columns
        ]
        whole = jnp.concatenate(whole, axis=1).reshape(outer, inner, rows, size)
        if added:
            whole = jnp.concatenate([whole, extra], axis=2)
        return whole.transpose(1, 0, 2, 3).reshape(inner, -1, size)
    specs, given = [], []
    for terms in columns:
        for a, b in terms:
            for piece in a:
                specs.append(pl.BlockSpec((piece.shape[0], block), lambda k: (0, k)))
                given.append(piece)
            specs.append(pl.BlockSpec(b.shape, lambda k: (0, 0)))
            given.append(b)
    if added:
        specs.append(pl.BlockSpec((1, inner, added, size), lambda k: (k, 0, 0, 0)))
        given.append(extra)
    plan = tuple(tuple(len(a) for a, _ in terms) for terms in columns)
    result = pl.pallas_call(
        functools.partial(grads_kernel, plan, added),
        grid=(outer,),
        in_specs=specs,
        out_specs=pl.BlockSpec((inner, 1, rows + added, size), lambda k: (0, k, 0, 0)),
        out_shape=jax.ShapeDtypeStruct((inner, outer, rows + added, size), BF16),
        cost_estimate=pl.CostEstimate(
            flops=2 * tokens * width * size,
            bytes_accessed=2 * (tokens * (width + size) + width * size),
            transcendentals=0,
        ),
    )(*given)
    return result.reshape(inner, -1, size)


def gelu_tanh(values):
    return jax.nn.gelu(values, approximate=True)


def geglu(gate_vals, up_vals):
    return gelu_tanh(gate_vals) * up_vals


def lru_inputs(gate_decay, gate_input, conv_in, decay_in, resets):
    log_decay = -8.0 * jax.nn.sigmoid(gate_decay) * jax.nn.softplus(decay_in)
    decay = jnp.exp(log_decay)
    multiplier = jnp.sqrt(jnp.maximum(-jnp.expm1(2.0 * log_decay), 0.001))
    multiplier = jnp.where(resets, 1.0, multiplier)
    keep_rate = jnp.where(resets, 0.0, decay)
    return (keep_rate, conv_in * jax.nn.sigmoid(gate_input) * multiplier)


def norm_back(values, scaling, delta):
    inverse = lax.rsqrt(jnp.mean(values * values, axis=-1, keepdims=True) + EPS)
    unit = values * inverse
    scaled = delta * (1.0 + scaling)
    moved = inverse * (scaled - unit * jnp.mean(scaled * unit, axis=-1, keepdims=True))
    return moved, jnp.sum(delta * unit, axis=0)


def rms_norm(values, scaling):
    inverse = lax.rsqrt(jnp.mean(values * values, axis=-1, keepdims=True) + EPS)
    return values * inverse * (1.0 + scaling)


def dot(a, b, contract):
    return lax.dot_general(a, b, ((contract[0], contract[1]), ((), ())), preferred_element_type=F32)


def mm(a, b):
    return dot(a, b, ((1,), (0,)))


def mm_nt(a, b):
    return dot(a, b, ((1,), (1,)))


def mm_tn(a, b):
    return dot(a, b, ((0,), (0,)))


def gather_slots(half):
    slots = []
    for k in range(lax.axis_size("o")):
        if k:
            half = ring(half)
        slots.append([half, swap(half)])
    return slots


def shift_outer(value, k):
    count = lax.axis_size("o")
    return lax.ppermute(value, "o", [(j, (j + k) % count) for j in range(count)])


def both_cores(part):
    rows = part.shape[0] // 2
    return part[:rows] + swap(part[rows:].astype(BF16)).astype(F32)


def reduce_slots(sums):
    total = sums[0]
    for part in sums[1:]:
        low = total.astype(BF16)
        moved = ring(low)
        total = part + moved.astype(F32)
    return total


def reduce_direct(halves):
    count = len(halves)
    total = halves[0].astype(F32)
    for k in range(1, count):
        moved = lax.ppermute(halves[k], "o", [(j, (j - k) % count) for j in range(count)])
        total = total + moved.astype(F32)
    return total


def spread(value):
    return lax.all_to_all(value, "o", 0, 0, tiled=True)


def gather_inner(whole):
    return lax.all_gather(whole, "i", axis=1, tiled=True).reshape(-1, whole.shape[-1])


def sum_inner(rows):
    own = lax.psum_scatter(
        rows.reshape(-1, rows.shape[-1]), "i", scatter_dimension=0, tiled=True
    )
    return own.reshape(lax.axis_size("o"), -1, rows.shape[-1])


def sum_outer(parts):
    count, at = lax.axis_size("o"), lax.axis_index("o")
    total = lax.dynamic_index_in_dim(parts, at, 0, False).astype(F32)
    for k in range(1, count):
        part = lax.dynamic_index_in_dim(parts, lax.rem(at + k, count), 0, False)
        moved = lax.ppermute(part, "o", [(j, (j + k) % count) for j in range(count)])
        total = total + moved.astype(F32)
    return total


def cuts_of(size):
    first = size // 2 // 128 * 128 + 128 if size > 512 else size
    return ((0, first), (first, size - first)) if size > first else ((0, size),)


def per_device(
    inputs,
    segment_ids,
    cotangent,
    branch_weight,
    out_weight,
    ffw_in,
    ffw_out,
    norm_scales,
    branch_bias,
    conv_weight,
    conv_bias,
    gate_weights,
    gate_bias,
    decay_param,
    out_bias,
    ffw_bias,
):
    outer, inner = lax.axis_size("o"), lax.axis_size("i")
    count = outer * inner
    core, along = lax.axis_index("tensor"), lax.axis_index("o")
    tok_rows, width = inputs.shape
    part_width = width // count
    hidden_half = ffw_out.shape[0]
    hidden_part = hidden_half // outer
    taps_count = conv_weight.shape[0]
    rim_rows = taps_count - 1
    heads_half, block_size = gate_weights.shape[1], gate_weights.shape[2]
    width_half = heads_half * block_size

    cuts = cuts_of(hidden_part)
    ffw_out_t = ffw_out.T
    packed = [
        jnp.stack(
            [
                jnp.concatenate(
                    [
                        w[:, k * hidden_part + start : k * hidden_part + start + size]
                        for w in (ffw_in[0], ffw_in[1], ffw_out_t)
                    ],
                    axis=1,
                )
                for k in range(outer)
            ]
        )
        for start, size in cuts
    ]
    (branch_x_full, branch_y_full, out_full_t), parts = gather_weights(
        [branch_weight[0], branch_weight[1], out_weight.T], packed
    )
    ffw_parts = []
    for k, (_, size) in enumerate(cuts):
        whole = gather_inner(parts[k])
        ffw_parts.append((whole[:, : 2 * size], whole[:, 2 * size :]))
    cot_own, branch_x_full = lax.optimization_barrier((half_of(cotangent, core), branch_x_full))
    near = [k for k in range(1, outer) if k in (1, outer - 1)]
    far = [k for k in range(1, outer) if k not in near]
    cot_near = [shift_outer(cot_own, k) for k in near]

    seg_marks = (segment_ids + 1).astype(F32)
    source_half = half_of(inputs, core).astype(F32)
    normed_low = rms_norm(inputs.astype(F32), norm_scales[0]).astype(BF16)
    branch_x = mm(normed_low, branch_x_full) + branch_bias[0]
    branch_y = mm(normed_low, branch_y_full) + branch_bias[1]
    rim_values, rim_marks = from_behind(
        (branch_x[tok_rows - rim_rows :], seg_marks[tok_rows - rim_rows :]), 1
    )
    padded_branch = jnp.concatenate([rim_values, branch_x], axis=0)
    padded_marks = jnp.concatenate([rim_marks, seg_marks], axis=0)
    resets = (seg_marks != padded_marks[rim_rows - 1 : rim_rows - 1 + tok_rows])[:, None]
    conv_out = jnp.zeros_like(branch_x) + conv_bias
    shifted_rows = []
    for offset in range(taps_count):
        matches = (
            padded_marks[rim_rows - offset : rim_rows - offset + tok_rows] == seg_marks
        ).astype(F32)[:, None]
        shifted = padded_branch[rim_rows - offset : rim_rows - offset + tok_rows] * matches
        shifted_rows.append(shifted)
        conv_out = conv_out + conv_weight[offset] * shifted
    conv_low = conv_out.astype(BF16)
    conv_float = conv_low.astype(F32)
    conv_blocks = conv_low.reshape(tok_rows, heads_half, block_size)
    gate_pre = (
        jnp.einsum(
            "thb,ghbc->gthc", conv_blocks, gate_weights, preferred_element_type=F32
        ).reshape(2, tok_rows, width_half)
        + gate_bias[:, None, :]
    )

    def lru_local(gate_decay, gate_input, conv_in, decay_in):
        return lru_inputs(gate_decay, gate_input, conv_in, decay_in, resets)

    (keep_rate, drive_in), lru_back = jax.vjp(
        lru_local, gate_pre[0], gate_pre[1], conv_float, decay_param
    )
    cumulative, local_state = local_scan(keep_rate, drive_in, False)
    ends = (cumulative[tok_rows - 1], local_state[tok_rows - 1])
    ends, cot_near = lax.optimization_barrier((ends, cot_near))
    carry_in = entering(*ends, False)
    carry_in, cot_own = lax.optimization_barrier((carry_in, cot_own))
    cot_far = [shift_outer(cot_own, k) for k in far]
    states = local_state + cumulative * carry_in
    branch_act, gelu_back = jax.vjp(gelu_tanh, branch_y)
    mixed_in = (states * branch_act).astype(BF16)
    mixed_part = mm_nt(mixed_in, out_full_t)
    residual = (
        source_half
        + half_of(mixed_part, core)
        + swap(half_of(mixed_part, 1 - core))
        + out_bias[0]
    )

    residual, cot_far = lax.optimization_barrier((residual, cot_far))
    cot_halves = dict(zip([0, *near, *far], [cot_own, *cot_near, *cot_far]))
    cot_slots = [[cot_halves[k], swap(cot_halves[k])] for k in range(outer)]
    normed_slots = gather_slots(rms_norm(residual, norm_scales[1]).astype(BF16))
    normed_joined = [jnp.concatenate(slot) for slot in normed_slots]
    cot_joined = [jnp.concatenate(slot) for slot in cot_slots]
    bias_part = lax.dynamic_slice_in_dim(ffw_bias, along * hidden_part, hidden_part, 1)
    slots = range(outer)
    hidden_of, delta_of, inner_sums, bias_sums, rows = [], [], [], [], None
    for p, (start, size) in enumerate(cuts):
        if rows is not None:
            rows, normed_joined, cot_joined = lax.optimization_barrier(
                (rows, normed_joined, cot_joined)
            )
            inner_sums.append(sum_inner(rows))
        in_full, out_full = ffw_parts[p]
        bias_row = bias_part[:, start : start + size].reshape(2 * size)
        hiddens, deltas = [], []
        for k in slots:
            gate_up = mm(normed_joined[k], in_full) + bias_row
            hidden, hidden_back = jax.vjp(geglu, gate_up[:, :size], gate_up[:, size:])
            hiddens.append(hidden.astype(BF16))
            deltas.append(
                jnp.concatenate(hidden_back(mm(cot_joined[k], out_full)), axis=1).astype(BF16)
            )
        if p == len(cuts) - 1:
            delta_parts = [
                sum(mm_nt(d[k], w[0]) for d, w in zip(delta_of + [deltas], ffw_parts))
                for k in slots
            ]
            sums = [both_cores(part) for part in delta_parts[1:] + delta_parts[:1]]
            _, hiddens, deltas = lax.optimization_barrier((sums[0], hiddens, deltas))
        hidden_of.append(hiddens)
        delta_of.append(deltas)
        bias_sums.append(
            sum(jnp.sum(d, axis=0, dtype=F32) for d in deltas).reshape(2, size)
        )
        rows = grads_rows([list(zip(normed_slots, deltas)), list(zip(cot_slots, hiddens))])
    inner_sums.append(sum_inner(rows))
    delta_normed_two = reduce_slots(sums)
    result_parts = [
        sum(mm_nt(hidden_of[p][k], ffw_parts[p][1]) for p in range(len(cuts))) for k in slots
    ]
    result_parts = [both_cores(part) for part in result_parts]
    result_parts = [result_parts[0]] + [part.astype(BF16) for part in result_parts[1:]]
    delta_normed_two, result_parts, inner_sums[0] = lax.optimization_barrier(
        (delta_normed_two, result_parts, inner_sums[0])
    )
    grads = [spread(inner_sums[0])]
    grad_ffw_bias = lax.dynamic_update_slice_in_dim(
        jnp.zeros((2, hidden_half), F32),
        jnp.concatenate(bias_sums, axis=1),
        along * hidden_part,
        1,
    )

    cot_half = half_of(cotangent, core).astype(F32)
    delta_res_norm, grad_scale_two = norm_back(residual, norm_scales[1], delta_normed_two)
    delta_residual = cot_half + delta_res_norm
    delta_half = delta_residual.astype(BF16)
    delta_mixed = join_halves(delta_half, swap(delta_half), core)
    delta_mixed_in = mm(delta_mixed, out_full_t)
    delta_states = delta_mixed_in * branch_act
    (delta_branch_y,) = gelu_back(delta_mixed_in * states)
    delta_y_low = delta_branch_y.astype(BF16)
    oy_rows = grads_rows([[([delta_mixed], mixed_in)], [([normed_low], delta_y_low)]])
    grad_oy_inner = sum_inner(oy_rows)
    alpha_next = jnp.concatenate([keep_rate[1:], jnp.ones((1, width_half), F32)], axis=0)
    suffix, local_adjoint = local_scan(alpha_next, delta_states, True)
    leaving = entering(keep_rate[0] * suffix[0], keep_rate[0] * local_adjoint[0], True)
    adjoint = local_adjoint + suffix * leaving
    states_before = jnp.concatenate([carry_in[None, :], states[: tok_rows - 1]], axis=0)
    delta_gate_decay, delta_gate_input, delta_conv_direct, grad_decay = lru_back(
        (adjoint * states_before, adjoint)
    )
    delta_gates = jnp.stack([delta_gate_decay, delta_gate_input]).astype(BF16)
    delta_blocks = delta_gates.reshape(2, tok_rows, heads_half, block_size)
    grad_gate_weights = jnp.einsum(
        "thb,gthc->ghbc", conv_blocks, delta_blocks, preferred_element_type=F32
    )
    gate_rows = (
        grad_gate_weights.reshape(2, heads_half, count, block_size // count, block_size)
        .transpose(2, 0, 1, 3, 4)
        .reshape(outer, inner, -1, width_half)
        .astype(BF16)
    )
    grad_gate_bias = jnp.sum(delta_gates, axis=1, dtype=F32)
    delta_conv = delta_conv_direct + jnp.einsum(
        "gthc,ghbc->thb", delta_blocks, gate_weights, preferred_element_type=F32
    ).reshape(tok_rows, width_half)
    rim_delta, rim_next_marks = from_behind((delta_conv[:rim_rows], seg_marks[:rim_rows]), -1)
    rim_delta, inner_sums, result_parts = lax.optimization_barrier(
        (rim_delta, inner_sums[1:], result_parts)
    )
    for k in range(1, len(cuts)):
        grads.append(spread(inner_sums[k - 1]))
    result_half = residual + reduce_direct(result_parts) + out_bias[1]
    result = join_halves(result_half, swap(result_half), core)
    ffw_in_grad = jnp.concatenate(
        [
            grad[:, :, : 2 * size].reshape(outer, part_width, 2, size)
            for grad, (_, size) in zip(grads, cuts)
        ],
        axis=3,
    )
    ffw_in_grad = (
        ffw_in_grad.transpose(2, 1, 0, 3).reshape(2, part_width, hidden_half).astype(F32)
    )
    ffw_out_grad = jnp.concatenate(
        [grad[:, :, 2 * size :] for grad, (_, size) in zip(grads, cuts)], axis=2
    )
    ffw_out_grad = ffw_out_grad.transpose(0, 2, 1).reshape(hidden_half, part_width).astype(F32)
    padded_delta = jnp.concatenate([delta_conv, rim_delta], axis=0)
    next_marks = jnp.concatenate([seg_marks, rim_next_marks], axis=0)
    delta_branch_x = jnp.zeros_like(delta_conv)
    conv_weight_rows = []
    for offset in range(taps_count):
        matches = (next_marks[offset : offset + tok_rows] == seg_marks).astype(F32)[:, None]
        delta_branch_x = (
            delta_branch_x
            + conv_weight[offset] * padded_delta[offset : offset + tok_rows] * matches
        )
        conv_weight_rows.append(jnp.sum(delta_conv * shifted_rows[offset], axis=0))
    grad_conv_bias = jnp.sum(delta_conv, axis=0)
    delta_x_low = delta_branch_x.astype(BF16)
    x_rows = grads_rows([[([normed_low], delta_x_low)]], gate_rows)
    grad_x_inner = sum_inner(x_rows)
    grad_oy = sum_outer(grad_oy_inner)
    delta_part = mm_nt(delta_x_low, branch_x_full) + mm_nt(delta_y_low, branch_y_full)
    delta_normed = half_of(delta_part, core) + swap(
        half_of(delta_part, 1 - core).astype(BF16)
    ).astype(F32)
    delta_source_norm, grad_scale_one = norm_back(source_half, norm_scales[0], delta_normed)
    grad_half = delta_residual + delta_source_norm
    input_grad = join_halves(grad_half, swap(grad_half), core)

    halves = jnp.stack(
        [
            grad_scale_one,
            grad_scale_two,
            jnp.sum(delta_half, axis=0, dtype=F32),
            jnp.sum(cot_half, axis=0),
        ]
    )
    halves = halves + swap(halves)
    flat = [
        halves.reshape(-1),
        jnp.sum(delta_x_low, axis=0, dtype=F32),
        jnp.sum(delta_y_low, axis=0, dtype=F32),
        *conv_weight_rows,
        grad_conv_bias,
        grad_gate_bias.reshape(-1),
        grad_decay,
        grad_ffw_bias.reshape(-1),
    ]
    flat = jnp.concatenate(flat).reshape(-1, 128)
    grad_x_inner, flat, input_grad, result, ffw_in_grad, ffw_out_grad, grad_oy = (
        lax.optimization_barrier(
            (grad_x_inner, flat, input_grad, result, ffw_in_grad, ffw_out_grad, grad_oy)
        )
    )
    grad_x_gate = sum_outer(grad_x_inner)
    grad_branch_x = grad_x_gate[:part_width]
    gate_grad = grad_x_gate[part_width:].reshape(2, heads_half, block_size // count, block_size)
    small = sum_over_all(flat).reshape(-1)
    at = 0
    taken = []
    for shape in (
        (2, width),
        (2, width),
        (2, width_half),
        (taps_count, width_half),
        (width_half,),
        (2, width_half),
        (width_half,),
        (2, hidden_half),
    ):
        size = 1
        for n in shape:
            size *= n
        taken.append(small[at : at + size].reshape(shape))
        at += size
    scales, out_bias_grad, branch_bias_grad, taps_grad, conv_bias_grad, gate_bias_grad, decay_grad, ffw_bias_grad = taken
    return (
        result,
        input_grad,
        jnp.stack([grad_branch_x, grad_oy[:, width_half:]]),
        grad_oy[:, :width_half].T,
        ffw_in_grad,
        ffw_out_grad,
        scales,
        branch_bias_grad,
        taps_grad,
        conv_bias_grad,
        gate_grad,
        gate_bias_grad,
        decay_grad,
        out_bias_grad,
        ffw_bias_grad,
    )


def solution(mesh):
    count = mesh.shape["dp"]
    grid = Mesh(
        mesh.devices.reshape(count // INNER, INNER, mesh.shape["tensor"]), ("o", "i", "tensor")
    )
    in_specs = (
        P(DP, None),
        P(DP),
        P(DP, None),
        P(None, DP, "tensor"),
        P("tensor", DP),
        P(None, DP, "tensor"),
        P("tensor", DP),
        P(),
        P(None, "tensor"),
        P(None, "tensor"),
        P("tensor"),
        P(None, "tensor", None, None),
        P(None, "tensor"),
        P("tensor"),
        P(),
        P(None, "tensor"),
    )
    out_specs = (
        P(DP, None),
        P(DP, None),
        P(None, DP, "tensor"),
        P("tensor", DP),
        P(None, DP, "tensor"),
        P("tensor", DP),
        P(),
        P(None, "tensor"),
        P(None, "tensor"),
        P("tensor"),
        P(None, "tensor", DP, None),
        P(None, "tensor"),
        P("tensor"),
        P(),
        P(None, "tensor"),
    )

    return jax.shard_map(
        per_device, mesh=grid, in_specs=in_specs, out_specs=out_specs, check_vma=False
    )
```

```python
import functools

import jax
import jax.numpy as jnp
from jax import lax
from jax.experimental import pallas as pl
from jax.experimental.pallas import tpu as pltpu
from jax.sharding import Mesh
from jax.sharding import PartitionSpec as P


INNER = 4
DP = ("o", "i")
EPS = 1e-06
F32 = jnp.float32
BF16 = jnp.bfloat16


def swap(value):
    return lax.ppermute(value, "tensor", [(0, 1), (1, 0)])


def ring(value):
    count = lax.axis_size("o")
    return lax.ppermute(value, "o", [(k, (k + 1) % count) for k in range(count)])


def from_behind(value, steps):
    count = lax.axis_size(DP)
    first, last = max(0, -steps), min(count, count - steps)
    return lax.ppermute(value, DP, [(k, k + steps) for k in range(first, last)])


def sum_over_all(value):
    count, bit = lax.axis_size(DP), 1
    while bit < count:
        value = value + lax.ppermute(value, DP, [(k, k ^ bit) for k in range(count)])
        bit *= 2
    return value


def half_of(value, which):
    rows = value.shape[0] // 2
    return lax.dynamic_slice_in_dim(value, which * rows, rows, 0)


def join_halves(own, other, core):
    first = jnp.where(core == 0, own, other)
    second = jnp.where(core == 0, other, own)
    return jnp.concatenate([first, second], axis=0)


def scan_kernel(reverse, keep_ref, drive_ref, cum_ref, state_ref):
    rows, width = keep_ref.shape
    groups = rows // 8
    place = lax.broadcasted_iota(jnp.int32, (8, width), 0)

    def step(k, carried):
        before_a, before_b = carried
        group = groups - 1 - k if reverse else k
        at = pl.ds(pl.multiple_of(group * 8, 8), 8)
        a, b = keep_ref[at, :], drive_ref[at, :]
        for d in (1, 2, 4):
            far_a = pltpu.roll(a, 8 - d if reverse else d, 0)
            far_b = pltpu.roll(b, 8 - d if reverse else d, 0)
            inside = place < 8 - d if reverse else place >= d
            b = jnp.where(inside, a * far_b + b, b)
            a = jnp.where(inside, a * far_a, a)
        b = a * before_b + b
        a = a * before_a
        cum_ref[at, :] = a
        state_ref[at, :] = b
        edge = slice(0, 1) if reverse else slice(7, 8)
        return (a[edge], b[edge])

    lax.fori_loop(
        0, groups, step, (jnp.ones((1, width), F32), jnp.zeros((1, width), F32))
    )


def local_scan(keep, drive, reverse):
    rows, width = keep.shape
    block = 256
    spec = pl.BlockSpec((rows, block), lambda j: (0, j))
    shape = jax.ShapeDtypeStruct((rows, width), F32)
    return pl.pallas_call(
        functools.partial(scan_kernel, reverse),
        grid=(width // block,),
        in_specs=[spec, spec],
        out_specs=[spec, spec],
        out_shape=[shape, shape],
        cost_estimate=pl.CostEstimate(
            flops=20 * rows * width, bytes_accessed=16 * rows * width, transcendentals=0
        ),
    )(keep, drive)


MESH_ID = pl.DeviceIdType.MESH
VMEM = pl.BlockSpec(memory_space=pltpu.VMEM)
ANY = pl.BlockSpec(memory_space=pl.ANY)


def enter_kernel(outer, inner, reverse, ends_ref, carry_ref, every, send_sem, recv_sem):
    count = outer * inner
    core = lax.axis_index("tensor")
    me = lax.axis_index("o") * inner + lax.axis_index("i")
    barrier = pltpu.get_barrier_semaphore()
    for k in range(1, count):
        peer = lax.rem(me + k, count)
        to = (peer // inner, lax.rem(peer, inner), core)
        pl.semaphore_signal(barrier, inc=1, device_id=to, device_id_type=MESH_ID)
    pl.semaphore_wait(barrier, count - 1)

    def copy(k, mine):
        peer = lax.rem(me + k, count)
        return pltpu.make_async_remote_copy(
            src_ref=ends_ref,
            dst_ref=every.at[me if mine else peer],
            send_sem=send_sem.at[k],
            recv_sem=recv_sem.at[me if mine else peer],
            device_id=(peer // inner, lax.rem(peer, inner), core),
            device_id_type=MESH_ID,
        )

    for k in range(1, count):
        copy(k, True).start()
    for k in range(1, count):
        copy(k, False).wait_recv()
    carried = jnp.zeros((1, ends_ref.shape[1]), F32)
    for k in range(count):
        at = count - 1 - k if reverse else k
        reached = at > me if reverse else at < me
        block = every[at]
        carried = jnp.where(reached, block[0:1] * carried + block[1:2], carried)
    carry_ref[...] = carried
    for k in range(1, count):
        copy(k, True).wait_send()


def entering(decay, state, reverse):
    outer, inner = lax.axis_size("o"), lax.axis_size("i")
    count, width = outer * inner, state.shape[0]
    carried = pl.pallas_call(
        functools.partial(enter_kernel, outer, inner, reverse),
        in_specs=[VMEM],
        out_specs=VMEM,
        out_shape=jax.ShapeDtypeStruct((1, width), F32),
        scratch_shapes=[
            pltpu.VMEM((count, 2, width), F32),
            pltpu.SemaphoreType.DMA((count,)),
            pltpu.SemaphoreType.DMA((count,)),
        ],
        compiler_params=pltpu.CompilerParams(
            collective_id=2 if reverse else 1, has_side_effects=True
        ),
    )(jnp.stack([decay, state]))
    return carried[0]


def gather_kernel(outer, groups, parts, *refs):
    own, send = refs[:groups], refs[groups : groups + parts]
    refs = refs[groups + parts :]
    full, got = refs[:groups], refs[groups : groups + parts]
    line_send, line_recv, side_send, side_recv, half_send, half_recv, part_send, part_recv, local = refs[
        groups + parts :
    ]
    o, i, core = lax.axis_index("o"), lax.axis_index("i"), lax.axis_index("tensor")
    sides = (i + 1 - 2 * lax.rem(i, 2), lax.rem(i + 2, 4))
    far = lax.rem(sides[0] + 2, 4)
    lanes = own[0].shape[1] // 2

    barrier = pltpu.get_barrier_semaphore()
    for k in range(1, outer):
        pl.semaphore_signal(
            barrier, inc=1, device_id=(lax.rem(o + k, outer), i, core), device_id_type=MESH_ID
        )
    for side in sides:
        pl.semaphore_signal(barrier, inc=1, device_id=(o, side, core), device_id_type=MESH_ID)
    pl.semaphore_wait(barrier, outer + 1)

    def remote(src, dst, send_sem, recv_sem, to):
        return pltpu.make_async_remote_copy(
            src_ref=src,
            dst_ref=dst,
            send_sem=send_sem,
            recv_sem=recv_sem,
            device_id=to,
            device_id_type=MESH_ID,
        )

    def block(g, k, j):
        return full[g].at[k, j]

    def along_line(g, k, mine, step):
        return remote(
            own[g] if mine else block(g, k, i),
            block(g, k, i),
            line_send.at[g, k, step],
            line_recv.at[g, k],
            (o + 2 * step - 1, i, core),
        )

    def to_side(g, k, mine, side):
        return remote(
            own[g] if mine else block(g, k, i),
            block(g, k, i),
            side_send.at[g, k, side],
            side_recv.at[g, k, side],
            (o, sides[side], core),
        )

    def from_side(g, k, side):
        return remote(
            block(g, k, sides[side]),
            block(g, k, sides[side]),
            side_send.at[g, k, side],
            side_recv.at[g, k, side],
            (o, sides[side], core),
        )

    def half(g, k, side, to):
        part = full[g].at[k, side, :, pl.ds(lanes * to, lanes)]
        return remote(
            part, part, half_send.at[g, k, to], half_recv.at[g, k, to], (o, sides[to], core)
        )

    def visit(first, then):
        first(o)
        for d in range(1, outer):
            pl.when(o - d >= 0)(functools.partial(then, o - d, True))
            pl.when(o + d < outer)(functools.partial(then, o + d, False))

    for g in range(groups):
        pltpu.make_async_copy(own[g], block(g, o, i), local.at[g]).start()
        pl.when(o + 1 < outer)(lambda g=g: along_line(g, o, True, 1).start())
        pl.when(o > 0)(lambda g=g: along_line(g, o, True, 0).start())
        for side in range(2):
            to_side(g, o, True, side).start()

    def pass_on(k, from_left):
        for g in range(groups):
            along_line(g, k, False, 0).wait_recv()
            if from_left:
                pl.when(o + 1 < outer)(lambda g=g: along_line(g, k, False, 1).start())
            else:
                pl.when(o > 0)(lambda g=g: along_line(g, k, False, 0).start())
            for side in range(2):
                to_side(g, k, False, side).start()

    visit(lambda k: None, pass_on)

    def part(p, k, mine):
        peer = lax.rem(o + k, outer)
        return remote(
            send[p].at[peer],
            got[p].at[o if mine else peer],
            part_send.at[p, k],
            part_recv.at[p, o if mine else peer],
            (peer, i, core),
        )

    for p in range(parts):
        pltpu.make_async_copy(send[p].at[o], got[p].at[o], local.at[groups + p]).start()
        for k in range(1, outer):
            part(p, k, True).start()

    def turn(k, _=None):
        for g in range(groups):
            for side in range(2):
                from_side(g, k, side).wait_recv()
                half(g, k, sides[side], 1 - side).start()

    visit(turn, turn)

    def finish(k, _=None):
        for g in range(groups):
            for side in range(2):
                half(g, k, far, side).wait_recv()

    visit(finish, finish)
    for p in range(parts):
        for k in range(1, outer):
            part(p, k, False).wait_recv()

    def sent(k, from_left):
        for g in range(groups):
            if from_left is None or from_left:
                pl.when(o + 1 < outer)(lambda g=g: along_line(g, k, False, 1).wait_send())
            if not from_left:
                pl.when(o > 0)(lambda g=g: along_line(g, k, False, 0).wait_send())
            for side in range(2):
                to_side(g, k, False, side).wait_send()
                half(g, k, sides[side], 1 - side).wait_send()

    visit(functools.partial(sent, from_left=None), sent)
    for p in range(parts):
        for k in range(1, outer):
            part(p, k, True).wait_send()
    for g in range(groups):
        pltpu.make_async_copy(own[g], block(g, o, i), local.at[g]).wait()
    for p in range(parts):
        pltpu.make_async_copy(send[p].at[o], got[p].at[o], local.at[groups + p]).wait()


def gather_weights(own, send):
    outer, inner = lax.axis_size("o"), lax.axis_size("i")
    groups, parts = len(own), len(send)
    dma = pltpu.SemaphoreType.DMA
    out_shape = [jax.ShapeDtypeStruct((outer, inner, *w.shape), w.dtype) for w in own] + [
        jax.ShapeDtypeStruct(w.shape, w.dtype) for w in send
    ]
    result = pl.pallas_call(
        functools.partial(gather_kernel, outer, groups, parts),
        in_specs=[VMEM] * (groups + parts),
        out_specs=[ANY] * (groups + parts),
        out_shape=out_shape,
        scratch_shapes=[
            dma((groups, outer, 2)),
            dma((groups, outer)),
            dma((groups, outer, 2)),
            dma((groups, outer, 2)),
            dma((groups, outer, 2)),
            dma((groups, outer, 2)),
            dma((parts, outer)),
            dma((parts, outer)),
            dma((groups + parts,)),
        ],
        compiler_params=pltpu.CompilerParams(collective_id=0, has_side_effects=True),
    )(*own, *send)
    full = [w.reshape(-1, w.shape[-1]) for w in result[:groups]]
    return full, result[groups:]


def grads_kernel(plan, added, *refs):
    out_ref = refs[-1]
    inner, _, rows, _ = out_ref.shape
    take = rows - added
    if added:
        out_ref[:, 0, take:, :] = refs[-2][0]
    refs = iter(refs)
    at = 0
    for terms in plan:
        total = None
        for pieces in terms:
            a = [next(refs)[...] for _ in range(pieces)]
            term = mm_tn(jnp.concatenate(a) if pieces > 1 else a[0], next(refs)[...])
            total = term if total is None else total + term
        size = total.shape[1]
        out_ref[:, 0, :take, at : at + size] = total.astype(BF16).reshape(inner, take, size)
        at += size


def grads_rows(columns, extra=None):
    outer, inner = lax.axis_size("o"), lax.axis_size("i")
    width = columns[0][0][0][0].shape[1]
    block = width // outer
    rows = block // inner
    size = sum(terms[0][1].shape[1] for terms in columns)
    tokens = sum(b.shape[0] for _, b in columns[0])
    added = 0 if extra is None else extra.shape[2]
    if block % 128:
        whole = [
            sum(mm_tn(jnp.concatenate(a), b) for a, b in terms).astype(BF16) for terms in columns
        ]
        whole = jnp.concatenate(whole, axis=1).reshape(outer, inner, rows, size)
        if added:
            whole = jnp.concatenate([whole, extra], axis=2)
        return whole.transpose(1, 0, 2, 3).reshape(inner, -1, size)
    specs, given = [], []
    for terms in columns:
        for a, b in terms:
            for piece in a:
                specs.append(pl.BlockSpec((piece.shape[0], block), lambda k: (0, k)))
                given.append(piece)
            specs.append(pl.BlockSpec(b.shape, lambda k: (0, 0)))
            given.append(b)
    if added:
        specs.append(pl.BlockSpec((1, inner, added, size), lambda k: (k, 0, 0, 0)))
        given.append(extra)
    plan = tuple(tuple(len(a) for a, _ in terms) for terms in columns)
    result = pl.pallas_call(
        functools.partial(grads_kernel, plan, added),
        grid=(outer,),
        in_specs=specs,
        out_specs=pl.BlockSpec((inner, 1, rows + added, size), lambda k: (0, k, 0, 0)),
        out_shape=jax.ShapeDtypeStruct((inner, outer, rows + added, size), BF16),
        cost_estimate=pl.CostEstimate(
            flops=2 * tokens * width * size,
            bytes_accessed=2 * (tokens * (width + size) + width * size),
            transcendentals=0,
        ),
    )(*given)
    return result.reshape(inner, -1, size)


def gelu_tanh(values):
    return jax.nn.gelu(values, approximate=True)


def geglu(gate_vals, up_vals):
    return gelu_tanh(gate_vals) * up_vals


def lru_inputs(gate_decay, gate_input, conv_in, decay_in, resets):
    log_decay = -8.0 * jax.nn.sigmoid(gate_decay) * jax.nn.softplus(decay_in)
    decay = jnp.exp(log_decay)
    multiplier = jnp.sqrt(jnp.maximum(-jnp.expm1(2.0 * log_decay), 0.001))
    multiplier = jnp.where(resets, 1.0, multiplier)
    keep_rate = jnp.where(resets, 0.0, decay)
    return (keep_rate, conv_in * jax.nn.sigmoid(gate_input) * multiplier)


def norm_back(values, scaling, delta):
    inverse = lax.rsqrt(jnp.mean(values * values, axis=-1, keepdims=True) + EPS)
    unit = values * inverse
    scaled = delta * (1.0 + scaling)
    moved = inverse * (scaled - unit * jnp.mean(scaled * unit, axis=-1, keepdims=True))
    return moved, jnp.sum(delta * unit, axis=0)


def rms_norm(values, scaling):
    inverse = lax.rsqrt(jnp.mean(values * values, axis=-1, keepdims=True) + EPS)
    return values * inverse * (1.0 + scaling)


def dot(a, b, contract):
    return lax.dot_general(a, b, ((contract[0], contract[1]), ((), ())), preferred_element_type=F32)


def mm(a, b):
    return dot(a, b, ((1,), (0,)))


def mm_nt(a, b):
    return dot(a, b, ((1,), (1,)))


def mm_tn(a, b):
    return dot(a, b, ((0,), (0,)))


def gather_slots(half):
    slots = []
    for k in range(lax.axis_size("o")):
        if k:
            half = ring(half)
        slots.append([half, swap(half)])
    return slots


def both_cores(part):
    rows = part.shape[0] // 2
    return part[:rows] + swap(part[rows:].astype(BF16)).astype(F32)


def reduce_slots(sums):
    total = sums[0]
    for part in sums[1:]:
        low = total.astype(BF16)
        moved = ring(low)
        total = part + moved.astype(F32)
    return total


def send_direct(halves):
    count = len(halves)
    return [halves[0]] + [
        lax.ppermute(halves[k], "o", [(j, (j - k) % count) for j in range(count)])
        for k in range(1, count)
    ]


def spread(value):
    return lax.all_to_all(value, "o", 0, 0, tiled=True)


def gather_inner(whole):
    return lax.all_gather(whole, "i", axis=1, tiled=True).reshape(-1, whole.shape[-1])


def sum_inner(rows):
    own = lax.psum_scatter(
        rows.reshape(-1, rows.shape[-1]), "i", scatter_dimension=0, tiled=True
    )
    return own.reshape(lax.axis_size("o"), -1, rows.shape[-1])


def sum_outer(parts):
    count, at = lax.axis_size("o"), lax.axis_index("o")
    total = lax.dynamic_index_in_dim(parts, at, 0, False).astype(F32)
    for k in range(1, count):
        part = lax.dynamic_index_in_dim(parts, lax.rem(at + k, count), 0, False)
        moved = lax.ppermute(part, "o", [(j, (j + k) % count) for j in range(count)])
        total = total + moved.astype(F32)
    return total


def cuts_of(size):
    first = size // 2 // 128 * 128 + 128 if size > 512 else size
    return ((0, first), (first, size - first)) if size > first else ((0, size),)


def per_device(
    inputs,
    segment_ids,
    cotangent,
    branch_weight,
    out_weight,
    ffw_in,
    ffw_out,
    norm_scales,
    branch_bias,
    conv_weight,
    conv_bias,
    gate_weights,
    gate_bias,
    decay_param,
    out_bias,
    ffw_bias,
):
    outer, inner = lax.axis_size("o"), lax.axis_size("i")
    count = outer * inner
    core, along = lax.axis_index("tensor"), lax.axis_index("o")
    tok_rows, width = inputs.shape
    part_width = width // count
    hidden_half = ffw_out.shape[0]
    hidden_part = hidden_half // outer
    taps_count = conv_weight.shape[0]
    rim_rows = taps_count - 1
    heads_half, block_size = gate_weights.shape[1], gate_weights.shape[2]
    width_half = heads_half * block_size

    cuts = cuts_of(hidden_part)
    ffw_out_t = ffw_out.T
    packed = [
        jnp.stack(
            [
                jnp.concatenate(
                    [
                        w[:, k * hidden_part + start : k * hidden_part + start + size]
                        for w in (ffw_in[0], ffw_in[1], ffw_out_t)
                    ],
                    axis=1,
                )
                for k in range(outer)
            ]
        )
        for start, size in cuts
    ]
    (branch_x_full, branch_y_full, out_full_t), parts = gather_weights(
        [branch_weight[0], branch_weight[1], out_weight.T], packed
    )
    ffw_parts = []
    for k, (_, size) in enumerate(cuts):
        whole = gather_inner(parts[k])
        ffw_parts.append((whole[:, : 2 * size], whole[:, 2 * size :]))
    cot_own, branch_x_full = lax.optimization_barrier((half_of(cotangent, core), branch_x_full))
    cot_whole = lax.all_gather(cot_own, "o")

    seg_marks = (segment_ids + 1).astype(F32)
    source_half = half_of(inputs, core).astype(F32)
    normed_low = rms_norm(inputs.astype(F32), norm_scales[0]).astype(BF16)
    branch_x = mm(normed_low, branch_x_full) + branch_bias[0]
    branch_y = mm(normed_low, branch_y_full) + branch_bias[1]
    rim_values, rim_marks = from_behind(
        (branch_x[tok_rows - rim_rows :], seg_marks[tok_rows - rim_rows :]), 1
    )
    padded_branch = jnp.concatenate([rim_values, branch_x], axis=0)
    padded_marks = jnp.concatenate([rim_marks, seg_marks], axis=0)
    resets = (seg_marks != padded_marks[rim_rows - 1 : rim_rows - 1 + tok_rows])[:, None]
    conv_out = jnp.zeros_like(branch_x) + conv_bias
    shifted_rows = []
    for offset in range(taps_count):
        matches = (
            padded_marks[rim_rows - offset : rim_rows - offset + tok_rows] == seg_marks
        ).astype(F32)[:, None]
        shifted = padded_branch[rim_rows - offset : rim_rows - offset + tok_rows] * matches
        shifted_rows.append(shifted)
        conv_out = conv_out + conv_weight[offset] * shifted
    conv_low = conv_out.astype(BF16)
    conv_float = conv_low.astype(F32)
    conv_blocks = conv_low.reshape(tok_rows, heads_half, block_size)
    gate_pre = (
        jnp.einsum(
            "thb,ghbc->gthc", conv_blocks, gate_weights, preferred_element_type=F32
        ).reshape(2, tok_rows, width_half)
        + gate_bias[:, None, :]
    )

    def lru_local(gate_decay, gate_input, conv_in, decay_in):
        return lru_inputs(gate_decay, gate_input, conv_in, decay_in, resets)

    (keep_rate, drive_in), lru_back = jax.vjp(
        lru_local, gate_pre[0], gate_pre[1], conv_float, decay_param
    )
    cumulative, local_state = local_scan(keep_rate, drive_in, False)
    carry_in = entering(cumulative[tok_rows - 1], local_state[tok_rows - 1], False)
    states = local_state + cumulative * carry_in
    branch_act, gelu_back = jax.vjp(gelu_tanh, branch_y)
    mixed_in = (states * branch_act).astype(BF16)
    mixed_part = mm_nt(mixed_in, out_full_t)
    residual = (
        source_half
        + half_of(mixed_part, core)
        + swap(half_of(mixed_part, 1 - core))
        + out_bias[0]
    )

    normed_slots = gather_slots(rms_norm(residual, norm_scales[1]).astype(BF16))
    cot_other = swap(cot_whole)
    sources = [lax.rem(along - k + outer, outer) for k in range(outer)]
    cot_slots = [
        [lax.dynamic_index_in_dim(w, k, 0, False) for w in (cot_whole, cot_other)] for k in sources
    ]
    normed_joined = [jnp.concatenate(slot) for slot in normed_slots]
    cot_joined = [jnp.concatenate(slot) for slot in cot_slots]
    bias_part = lax.dynamic_slice_in_dim(ffw_bias, along * hidden_part, hidden_part, 1)
    slots = range(outer)
    hidden_of, delta_of, inner_sums, bias_sums, rows = [], [], [], [], None
    for p, (start, size) in enumerate(cuts):
        if rows is not None:
            rows, normed_joined, cot_joined = lax.optimization_barrier(
                (rows, normed_joined, cot_joined)
            )
            inner_sums.append(sum_inner(rows))
        in_full, out_full = ffw_parts[p]
        bias_row = bias_part[:, start : start + size].reshape(2 * size)
        hiddens, deltas = [], []
        for k in slots:
            gate_up = mm(normed_joined[k], in_full) + bias_row
            hidden, hidden_back = jax.vjp(geglu, gate_up[:, :size], gate_up[:, size:])
            hiddens.append(hidden.astype(BF16))
            deltas.append(
                jnp.concatenate(hidden_back(mm(cot_joined[k], out_full)), axis=1).astype(BF16)
            )
        if p == len(cuts) - 1:
            delta_parts = [
                sum(mm_nt(d[k], w[0]) for d, w in zip(delta_of + [deltas], ffw_parts))
                for k in slots
            ]
            sums = [both_cores(part) for part in delta_parts[1:] + delta_parts[:1]]
            _, hiddens, deltas = lax.optimization_barrier((sums[0], hiddens, deltas))
        hidden_of.append(hiddens)
        delta_of.append(deltas)
        bias_sums.append(
            sum(jnp.sum(d, axis=0, dtype=F32) for d in deltas).reshape(2, size)
        )
        rows = grads_rows([list(zip(normed_slots, deltas)), list(zip(cot_slots, hiddens))])
    inner_sums.append(sum_inner(rows))
    delta_normed_two = reduce_slots(sums)
    result_parts = [
        sum(mm_nt(hidden_of[p][k], ffw_parts[p][1]) for p in range(len(cuts))) for k in slots
    ]
    result_parts = [both_cores(part) for part in result_parts]
    result_parts = [result_parts[0]] + [part.astype(BF16) for part in result_parts[1:]]
    delta_normed_two, result_parts, inner_sums[0] = lax.optimization_barrier(
        (delta_normed_two, result_parts, inner_sums[0])
    )
    grads = [spread(inner_sums[0])]
    grad_ffw_bias = lax.dynamic_update_slice_in_dim(
        jnp.zeros((2, hidden_half), F32),
        jnp.concatenate(bias_sums, axis=1),
        along * hidden_part,
        1,
    )

    cot_half = half_of(cotangent, core).astype(F32)
    delta_res_norm, grad_scale_two = norm_back(residual, norm_scales[1], delta_normed_two)
    delta_residual = cot_half + delta_res_norm
    delta_half = delta_residual.astype(BF16)
    delta_mixed = join_halves(delta_half, swap(delta_half), core)
    delta_mixed_in = mm(delta_mixed, out_full_t)
    delta_states = delta_mixed_in * branch_act
    (delta_branch_y,) = gelu_back(delta_mixed_in * states)
    delta_y_low = delta_branch_y.astype(BF16)
    oy_rows = grads_rows([[([delta_mixed], mixed_in)], [([normed_low], delta_y_low)]])
    grad_oy_inner = sum_inner(oy_rows)
    alpha_next = jnp.concatenate([keep_rate[1:], jnp.ones((1, width_half), F32)], axis=0)
    suffix, local_adjoint = local_scan(alpha_next, delta_states, True)
    leaving = entering(keep_rate[0] * suffix[0], keep_rate[0] * local_adjoint[0], True)
    leaving, inner_sums[1:] = lax.optimization_barrier((leaving, inner_sums[1:]))
    for k in range(1, len(cuts)):
        grads.append(spread(inner_sums[k]))
    adjoint = local_adjoint + suffix * leaving
    states_before = jnp.concatenate([carry_in[None, :], states[: tok_rows - 1]], axis=0)
    delta_gate_decay, delta_gate_input, delta_conv_direct, grad_decay = lru_back(
        (adjoint * states_before, adjoint)
    )
    delta_gates = jnp.stack([delta_gate_decay, delta_gate_input]).astype(BF16)
    delta_blocks = delta_gates.reshape(2, tok_rows, heads_half, block_size)
    grad_gate_weights = jnp.einsum(
        "thb,gthc->ghbc", conv_blocks, delta_blocks, preferred_element_type=F32
    )
    gate_rows = (
        grad_gate_weights.reshape(2, heads_half, count, block_size // count, block_size)
        .transpose(2, 0, 1, 3, 4)
        .reshape(outer, inner, -1, width_half)
        .astype(BF16)
    )
    grad_gate_bias = jnp.sum(delta_gates, axis=1, dtype=F32)
    delta_conv = delta_conv_direct + jnp.einsum(
        "gthc,ghbc->thb", delta_blocks, gate_weights, preferred_element_type=F32
    ).reshape(tok_rows, width_half)
    rim_delta, rim_next_marks = from_behind((delta_conv[:rim_rows], seg_marks[:rim_rows]), -1)
    rim_delta, result_parts = lax.optimization_barrier((rim_delta, result_parts))
    result_moved = send_direct(result_parts)
    ffw_in_grad = jnp.concatenate(
        [
            grad[:, :, : 2 * size].reshape(outer, part_width, 2, size)
            for grad, (_, size) in zip(grads, cuts)
        ],
        axis=3,
    )
    ffw_in_grad = (
        ffw_in_grad.transpose(2, 1, 0, 3).reshape(2, part_width, hidden_half).astype(F32)
    )
    ffw_out_grad = jnp.concatenate(
        [grad[:, :, 2 * size :] for grad, (_, size) in zip(grads, cuts)], axis=2
    )
    ffw_out_grad = ffw_out_grad.transpose(0, 2, 1).reshape(hidden_half, part_width).astype(F32)
    padded_delta = jnp.concatenate([delta_conv, rim_delta], axis=0)
    next_marks = jnp.concatenate([seg_marks, rim_next_marks], axis=0)
    delta_branch_x = jnp.zeros_like(delta_conv)
    conv_weight_rows = []
    for offset in range(taps_count):
        matches = (next_marks[offset : offset + tok_rows] == seg_marks).astype(F32)[:, None]
        delta_branch_x = (
            delta_branch_x
            + conv_weight[offset] * padded_delta[offset : offset + tok_rows] * matches
        )
        conv_weight_rows.append(jnp.sum(delta_conv * shifted_rows[offset], axis=0))
    grad_conv_bias = jnp.sum(delta_conv, axis=0)
    delta_x_low = delta_branch_x.astype(BF16)
    x_rows = grads_rows([[([normed_low], delta_x_low)]], gate_rows)
    grad_x_inner = sum_inner(x_rows)
    delta_part = mm_nt(delta_x_low, branch_x_full) + mm_nt(delta_y_low, branch_y_full)
    delta_normed = half_of(delta_part, core) + swap(
        half_of(delta_part, 1 - core).astype(BF16)
    ).astype(F32)
    delta_source_norm, grad_scale_one = norm_back(source_half, norm_scales[0], delta_normed)
    grad_half = delta_residual + delta_source_norm
    input_grad = join_halves(grad_half, swap(grad_half), core)

    halves = jnp.stack(
        [
            grad_scale_one,
            grad_scale_two,
            jnp.sum(delta_half, axis=0, dtype=F32),
            jnp.sum(cot_half, axis=0),
        ]
    )
    halves = halves + swap(halves)
    flat = [
        halves.reshape(-1),
        jnp.sum(delta_x_low, axis=0, dtype=F32),
        jnp.sum(delta_y_low, axis=0, dtype=F32),
        *conv_weight_rows,
        grad_conv_bias,
        grad_gate_bias.reshape(-1),
        grad_decay,
        grad_ffw_bias.reshape(-1),
    ]
    small = sum_over_all(jnp.concatenate(flat).reshape(-1, 128))
    small, grad_oy_inner = lax.optimization_barrier((small, grad_oy_inner))
    grad_oy = sum_outer(grad_oy_inner)
    result_half = residual + sum(part.astype(F32) for part in result_moved) + out_bias[1]
    result = join_halves(result_half, swap(result_half), core)
    grad_x_inner, input_grad, result, ffw_in_grad, ffw_out_grad = lax.optimization_barrier(
        (grad_x_inner, input_grad, result, ffw_in_grad, ffw_out_grad)
    )
    grad_x_gate = sum_outer(grad_x_inner)
    grad_branch_x = grad_x_gate[:part_width]
    gate_grad = grad_x_gate[part_width:].reshape(2, heads_half, block_size // count, block_size)
    small = small.reshape(-1)
    at = 0
    taken = []
    for shape in (
        (2, width),
        (2, width),
        (2, width_half),
        (taps_count, width_half),
        (width_half,),
        (2, width_half),
        (width_half,),
        (2, hidden_half),
    ):
        size = 1
        for n in shape:
            size *= n
        taken.append(small[at : at + size].reshape(shape))
        at += size
    scales, out_bias_grad, branch_bias_grad, taps_grad, conv_bias_grad, gate_bias_grad, decay_grad, ffw_bias_grad = taken
    return (
        result,
        input_grad,
        jnp.stack([grad_branch_x, grad_oy[:, width_half:]]),
        grad_oy[:, :width_half].T,
        ffw_in_grad,
        ffw_out_grad,
        scales,
        branch_bias_grad,
        taps_grad,
        conv_bias_grad,
        gate_grad,
        gate_bias_grad,
        decay_grad,
        out_bias_grad,
        ffw_bias_grad,
    )


def solution(mesh):
    count = mesh.shape["dp"]
    grid = Mesh(
        mesh.devices.reshape(count // INNER, INNER, mesh.shape["tensor"]), ("o", "i", "tensor")
    )
    in_specs = (
        P(DP, None),
        P(DP),
        P(DP, None),
        P(None, DP, "tensor"),
        P("tensor", DP),
        P(None, DP, "tensor"),
        P("tensor", DP),
        P(),
        P(None, "tensor"),
        P(None, "tensor"),
        P("tensor"),
        P(None, "tensor", None, None),
        P(None, "tensor"),
        P("tensor"),
        P(),
        P(None, "tensor"),
    )
    out_specs = (
        P(DP, None),
        P(DP, None),
        P(None, DP, "tensor"),
        P("tensor", DP),
        P(None, DP, "tensor"),
        P("tensor", DP),
        P(),
        P(None, "tensor"),
        P(None, "tensor"),
        P("tensor"),
        P(None, "tensor", DP, None),
        P(None, "tensor"),
        P("tensor"),
        P(),
        P(None, "tensor"),
    )

    return jax.shard_map(
        per_device, mesh=grid, in_specs=in_specs, out_specs=out_specs, check_vma=False
    )
```

```python
import functools

import jax
import jax.numpy as jnp
from jax import lax
from jax.experimental import pallas as pl
from jax.experimental.pallas import tpu as pltpu
from jax.sharding import Mesh
from jax.sharding import PartitionSpec as P


INNER = 4
DP = ("o", "i")
EPS = 1e-06
F32 = jnp.float32
BF16 = jnp.bfloat16


def swap(value):
    return lax.ppermute(value, "tensor", [(0, 1), (1, 0)])


def ring(value):
    count = lax.axis_size("o")
    return lax.ppermute(value, "o", [(k, (k + 1) % count) for k in range(count)])


def from_behind(value, steps):
    count = lax.axis_size(DP)
    first, last = max(0, -steps), min(count, count - steps)
    return lax.ppermute(value, DP, [(k, k + steps) for k in range(first, last)])


def sum_over_all(value):
    count, bit = lax.axis_size(DP), 1
    while bit < count:
        value = value + lax.ppermute(value, DP, [(k, k ^ bit) for k in range(count)])
        bit *= 2
    return value


def half_of(value, which):
    rows = value.shape[0] // 2
    return lax.dynamic_slice_in_dim(value, which * rows, rows, 0)


def join_halves(own, other, core):
    first = jnp.where(core == 0, own, other)
    second = jnp.where(core == 0, other, own)
    return jnp.concatenate([first, second], axis=0)


def run_scan(reverse, keep_ref, drive_ref, cum_ref, state_ref):
    rows, width = keep_ref.shape
    groups = rows // 8
    place = lax.broadcasted_iota(jnp.int32, (8, width), 0)

    def step(k, carried):
        before_a, before_b = carried
        group = groups - 1 - k if reverse else k
        at = pl.ds(pl.multiple_of(group * 8, 8), 8)
        a, b = keep_ref[at, :], drive_ref[at, :]
        for d in (1, 2, 4):
            far_a = pltpu.roll(a, 8 - d if reverse else d, 0)
            far_b = pltpu.roll(b, 8 - d if reverse else d, 0)
            inside = place < 8 - d if reverse else place >= d
            b = jnp.where(inside, a * far_b + b, b)
            a = jnp.where(inside, a * far_a, a)
        b = a * before_b + b
        a = a * before_a
        cum_ref[at, :] = a
        state_ref[at, :] = b
        edge = slice(0, 1) if reverse else slice(7, 8)
        return (a[edge], b[edge])

    return lax.fori_loop(
        0, groups, step, (jnp.ones((1, width), F32), jnp.zeros((1, width), F32))
    )


def scan_kernel(reverse, keep_ref, drive_ref, cum_ref, state_ref):
    run_scan(reverse, keep_ref, drive_ref, cum_ref, state_ref)


def local_scan(keep, drive, reverse):
    rows, width = keep.shape
    block = 256
    spec = pl.BlockSpec((rows, block), lambda j: (0, j))
    shape = jax.ShapeDtypeStruct((rows, width), F32)
    return pl.pallas_call(
        functools.partial(scan_kernel, reverse),
        grid=(width // block,),
        in_specs=[spec, spec],
        out_specs=[spec, spec],
        out_shape=[shape, shape],
        cost_estimate=pl.CostEstimate(
            flops=20 * rows * width, bytes_accessed=16 * rows * width, transcendentals=0
        ),
    )(keep, drive)


HALO = 8


def mix_kernel(branch_ref, mask_ref, taps_ref, rows_ref, gate_ref, *refs):
    conv_ref, decay_gate_ref, input_gate_ref, cum_ref, state_ref, ends_ref, keep, drive = refs
    rows = conv_ref.shape[0]
    conv = rows_ref[0:1, :] + taps_ref[0:1, :] * branch_ref[HALO : HALO + rows, :]
    for k in range(1, taps_ref.shape[0]):
        shifted = branch_ref[HALO - k : HALO - k + rows, :] * mask_ref[:, k : k + 1]
        conv = conv + taps_ref[k : k + 1, :] * shifted
    low = conv.astype(BF16)
    conv_ref[...] = low
    decay_gate = jax.nn.sigmoid(mm(low, gate_ref[0, 0]) + rows_ref[1:2, :])
    input_gate = jax.nn.sigmoid(mm(low, gate_ref[1, 0]) + rows_ref[2:3, :])
    decay_gate_ref[...] = decay_gate
    input_gate_ref[...] = input_gate
    reset = mask_ref[:, 0:1]
    log_decay = -8.0 * decay_gate * rows_ref[3:4, :]
    multiplier = jnp.sqrt(jnp.maximum(1.0 - jnp.exp(2.0 * log_decay), 0.001))
    keep[...] = jnp.exp(log_decay) * (1.0 - reset)
    drive[...] = low.astype(F32) * input_gate * (multiplier * (1.0 - reset) + reset)
    ends_ref[0:1, :], ends_ref[1:2, :] = run_scan(False, keep, drive, cum_ref, state_ref)


def mix(branch, masks, taps, row_params, gate_weights):
    rows, width = branch.shape[0] - HALO, branch.shape[1]
    block = gate_weights.shape[2]
    over = lambda n: pl.BlockSpec((n, block), lambda h: (0, h))
    full = jax.ShapeDtypeStruct((rows, width), F32)
    return pl.pallas_call(
        mix_kernel,
        grid=(width // block,),
        in_specs=[
            over(rows + HALO),
            pl.BlockSpec(masks.shape, lambda h: (0, 0)),
            over(taps.shape[0]),
            over(row_params.shape[0]),
            pl.BlockSpec((2, 1, block, block), lambda h: (0, h, 0, 0)),
        ],
        out_specs=[over(rows)] * 5 + [over(2)],
        out_shape=[
            jax.ShapeDtypeStruct((rows, width), BF16),
            full,
            full,
            full,
            full,
            jax.ShapeDtypeStruct((2, width), F32),
        ],
        scratch_shapes=[pltpu.VMEM((rows, block), F32)] * 2,
        cost_estimate=pl.CostEstimate(
            flops=4 * rows * width * block,
            bytes_accessed=22 * rows * width,
            transcendentals=8 * rows * width,
        ),
    )(branch, masks, taps, row_params, gate_weights)


MESH_ID = pl.DeviceIdType.MESH
VMEM = pl.BlockSpec(memory_space=pltpu.VMEM)
ANY = pl.BlockSpec(memory_space=pl.ANY)


def enter_kernel(outer, inner, reverse, ends_ref, carry_ref, every, send_sem, recv_sem):
    count = outer * inner
    core = lax.axis_index("tensor")
    me = lax.axis_index("o") * inner + lax.axis_index("i")
    barrier = pltpu.get_barrier_semaphore()
    for k in range(1, count):
        peer = lax.rem(me + k, count)
        to = (peer // inner, lax.rem(peer, inner), core)
        pl.semaphore_signal(barrier, inc=1, device_id=to, device_id_type=MESH_ID)
    pl.semaphore_wait(barrier, count - 1)

    def copy(k, mine):
        peer = lax.rem(me + k, count)
        return pltpu.make_async_remote_copy(
            src_ref=ends_ref,
            dst_ref=every.at[me if mine else peer],
            send_sem=send_sem.at[k],
            recv_sem=recv_sem.at[me if mine else peer],
            device_id=(peer // inner, lax.rem(peer, inner), core),
            device_id_type=MESH_ID,
        )

    for k in range(1, count):
        copy(k, True).start()
    for k in range(1, count):
        copy(k, False).wait_recv()
    carried = jnp.zeros((1, ends_ref.shape[1]), F32)
    for k in range(count):
        at = count - 1 - k if reverse else k
        reached = at > me if reverse else at < me
        block = every[at]
        carried = jnp.where(reached, block[0:1] * carried + block[1:2], carried)
    carry_ref[...] = carried
    for k in range(1, count):
        copy(k, True).wait_send()


def entering(ends, reverse):
    outer, inner = lax.axis_size("o"), lax.axis_size("i")
    count, width = outer * inner, ends.shape[1]
    carried = pl.pallas_call(
        functools.partial(enter_kernel, outer, inner, reverse),
        in_specs=[VMEM],
        out_specs=VMEM,
        out_shape=jax.ShapeDtypeStruct((1, width), F32),
        scratch_shapes=[
            pltpu.VMEM((count, 2, width), F32),
            pltpu.SemaphoreType.DMA((count,)),
            pltpu.SemaphoreType.DMA((count,)),
        ],
        compiler_params=pltpu.CompilerParams(
            collective_id=2 if reverse else 1, has_side_effects=True
        ),
    )(ends)
    return carried[0]


def gather_kernel(outer, groups, parts, *refs):
    own, send = refs[:groups], refs[groups : groups + parts]
    refs = refs[groups + parts :]
    full, got = refs[:groups], refs[groups : groups + parts]
    line_send, line_recv, side_send, side_recv, half_send, half_recv, part_send, part_recv, local = refs[
        groups + parts :
    ]
    o, i, core = lax.axis_index("o"), lax.axis_index("i"), lax.axis_index("tensor")
    sides = (i + 1 - 2 * lax.rem(i, 2), lax.rem(i + 2, 4))
    far = lax.rem(sides[0] + 2, 4)
    lanes = own[0].shape[1] // 2

    barrier = pltpu.get_barrier_semaphore()
    for k in range(1, outer):
        pl.semaphore_signal(
            barrier, inc=1, device_id=(lax.rem(o + k, outer), i, core), device_id_type=MESH_ID
        )
    for side in sides:
        pl.semaphore_signal(barrier, inc=1, device_id=(o, side, core), device_id_type=MESH_ID)
    pl.semaphore_wait(barrier, outer + 1)

    def remote(src, dst, send_sem, recv_sem, to):
        return pltpu.make_async_remote_copy(
            src_ref=src,
            dst_ref=dst,
            send_sem=send_sem,
            recv_sem=recv_sem,
            device_id=to,
            device_id_type=MESH_ID,
        )

    def block(g, k, j):
        return full[g].at[k, j]

    def along_line(g, k, mine, step):
        return remote(
            own[g] if mine else block(g, k, i),
            block(g, k, i),
            line_send.at[g, k, step],
            line_recv.at[g, k],
            (o + 2 * step - 1, i, core),
        )

    def to_side(g, k, mine, side):
        return remote(
            own[g] if mine else block(g, k, i),
            block(g, k, i),
            side_send.at[g, k, side],
            side_recv.at[g, k, side],
            (o, sides[side], core),
        )

    def from_side(g, k, side):
        return remote(
            block(g, k, sides[side]),
            block(g, k, sides[side]),
            side_send.at[g, k, side],
            side_recv.at[g, k, side],
            (o, sides[side], core),
        )

    def half(g, k, side, to):
        part = full[g].at[k, side, :, pl.ds(lanes * to, lanes)]
        return remote(
            part, part, half_send.at[g, k, to], half_recv.at[g, k, to], (o, sides[to], core)
        )

    def visit(first, then):
        first(o)
        for d in range(1, outer):
            pl.when(o - d >= 0)(functools.partial(then, o - d, True))
            pl.when(o + d < outer)(functools.partial(then, o + d, False))

    for g in range(groups):
        pltpu.make_async_copy(own[g], block(g, o, i), local.at[g]).start()
        pl.when(o + 1 < outer)(lambda g=g: along_line(g, o, True, 1).start())
        pl.when(o > 0)(lambda g=g: along_line(g, o, True, 0).start())
        for side in range(2):
            to_side(g, o, True, side).start()

    def pass_on(k, from_left):
        for g in range(groups):
            along_line(g, k, False, 0).wait_recv()
            if from_left:
                pl.when(o + 1 < outer)(lambda g=g: along_line(g, k, False, 1).start())
            else:
                pl.when(o > 0)(lambda g=g: along_line(g, k, False, 0).start())
            for side in range(2):
                to_side(g, k, False, side).start()

    visit(lambda k: None, pass_on)

    def part(p, k, mine):
        peer = lax.rem(o + k, outer)
        return remote(
            send[p].at[peer],
            got[p].at[o if mine else peer],
            part_send.at[p, k],
            part_recv.at[p, o if mine else peer],
            (peer, i, core),
        )

    for p in range(parts):
        pltpu.make_async_copy(send[p].at[o], got[p].at[o], local.at[groups + p]).start()
        for k in range(1, outer):
            part(p, k, True).start()

    def turn(k, _=None):
        for g in range(groups):
            for side in range(2):
                from_side(g, k, side).wait_recv()
                half(g, k, sides[side], 1 - side).start()

    visit(turn, turn)

    def finish(k, _=None):
        for g in range(groups):
            for side in range(2):
                half(g, k, far, side).wait_recv()

    visit(finish, finish)
    for p in range(parts):
        for k in range(1, outer):
            part(p, k, False).wait_recv()

    def sent(k, from_left):
        for g in range(groups):
            if from_left is None or from_left:
                pl.when(o + 1 < outer)(lambda g=g: along_line(g, k, False, 1).wait_send())
            if not from_left:
                pl.when(o > 0)(lambda g=g: along_line(g, k, False, 0).wait_send())
            for side in range(2):
                to_side(g, k, False, side).wait_send()
                half(g, k, sides[side], 1 - side).wait_send()

    visit(functools.partial(sent, from_left=None), sent)
    for p in range(parts):
        for k in range(1, outer):
            part(p, k, True).wait_send()
    for g in range(groups):
        pltpu.make_async_copy(own[g], block(g, o, i), local.at[g]).wait()
    for p in range(parts):
        pltpu.make_async_copy(send[p].at[o], got[p].at[o], local.at[groups + p]).wait()


def gather_weights(own, send):
    outer, inner = lax.axis_size("o"), lax.axis_size("i")
    groups, parts = len(own), len(send)
    dma = pltpu.SemaphoreType.DMA
    out_shape = [jax.ShapeDtypeStruct((outer, inner, *w.shape), w.dtype) for w in own] + [
        jax.ShapeDtypeStruct(w.shape, w.dtype) for w in send
    ]
    result = pl.pallas_call(
        functools.partial(gather_kernel, outer, groups, parts),
        in_specs=[VMEM] * (groups + parts),
        out_specs=[ANY] * (groups + parts),
        out_shape=out_shape,
        scratch_shapes=[
            dma((groups, outer, 2)),
            dma((groups, outer)),
            dma((groups, outer, 2)),
            dma((groups, outer, 2)),
            dma((groups, outer, 2)),
            dma((groups, outer, 2)),
            dma((parts, outer)),
            dma((parts, outer)),
            dma((groups + parts,)),
        ],
        compiler_params=pltpu.CompilerParams(collective_id=0, has_side_effects=True),
    )(*own, *send)
    full = [w.reshape(-1, w.shape[-1]) for w in result[:groups]]
    return full, result[groups:]


def grads_kernel(plan, added, *refs):
    out_ref = refs[-1]
    inner, _, rows, _ = out_ref.shape
    take = rows - added
    if added:
        out_ref[:, 0, take:, :] = refs[-2][0]
    refs = iter(refs)
    at = 0
    for terms in plan:
        total = None
        for pieces in terms:
            a = [next(refs)[...] for _ in range(pieces)]
            term = mm_tn(jnp.concatenate(a) if pieces > 1 else a[0], next(refs)[...])
            total = term if total is None else total + term
        size = total.shape[1]
        out_ref[:, 0, :take, at : at + size] = total.astype(BF16).reshape(inner, take, size)
        at += size


def grads_rows(columns, extra=None):
    outer, inner = lax.axis_size("o"), lax.axis_size("i")
    width = columns[0][0][0][0].shape[1]
    block = width // outer
    rows = block // inner
    size = sum(terms[0][1].shape[1] for terms in columns)
    tokens = sum(b.shape[0] for _, b in columns[0])
    added = 0 if extra is None else extra.shape[2]
    if block % 128:
        whole = [
            sum(mm_tn(jnp.concatenate(a), b) for a, b in terms).astype(BF16) for terms in columns
        ]
        whole = jnp.concatenate(whole, axis=1).reshape(outer, inner, rows, size)
        if added:
            whole = jnp.concatenate([whole, extra], axis=2)
        return whole.transpose(1, 0, 2, 3).reshape(inner, -1, size)
    specs, given = [], []
    for terms in columns:
        for a, b in terms:
            for piece in a:
                specs.append(pl.BlockSpec((piece.shape[0], block), lambda k: (0, k)))
                given.append(piece)
            specs.append(pl.BlockSpec(b.shape, lambda k: (0, 0)))
            given.append(b)
    if added:
        specs.append(pl.BlockSpec((1, inner, added, size), lambda k: (k, 0, 0, 0)))
        given.append(extra)
    plan = tuple(tuple(len(a) for a, _ in terms) for terms in columns)
    result = pl.pallas_call(
        functools.partial(grads_kernel, plan, added),
        grid=(outer,),
        in_specs=specs,
        out_specs=pl.BlockSpec((inner, 1, rows + added, size), lambda k: (0, k, 0, 0)),
        out_shape=jax.ShapeDtypeStruct((inner, outer, rows + added, size), BF16),
        cost_estimate=pl.CostEstimate(
            flops=2 * tokens * width * size,
            bytes_accessed=2 * (tokens * (width + size) + width * size),
            transcendentals=0,
        ),
    )(*given)
    return result.reshape(inner, -1, size)


def gelu_tanh(values):
    return jax.nn.gelu(values, approximate=True)


def geglu(gate_vals, up_vals):
    return gelu_tanh(gate_vals) * up_vals


def norm_back(values, scaling, delta):
    inverse = lax.rsqrt(jnp.mean(values * values, axis=-1, keepdims=True) + EPS)
    unit = values * inverse
    scaled = delta * (1.0 + scaling)
    moved = inverse * (scaled - unit * jnp.mean(scaled * unit, axis=-1, keepdims=True))
    return moved, jnp.sum(delta * unit, axis=0)


def rms_norm(values, scaling):
    inverse = lax.rsqrt(jnp.mean(values * values, axis=-1, keepdims=True) + EPS)
    return values * inverse * (1.0 + scaling)


def dot(a, b, contract):
    return lax.dot_general(a, b, ((contract[0], contract[1]), ((), ())), preferred_element_type=F32)


def mm(a, b):
    return dot(a, b, ((1,), (0,)))


def mm_nt(a, b):
    return dot(a, b, ((1,), (1,)))


def mm_tn(a, b):
    return dot(a, b, ((0,), (0,)))


def gather_slots(half):
    slots = []
    for k in range(lax.axis_size("o")):
        if k:
            half = ring(half)
        slots.append([half, swap(half)])
    return slots


def both_cores(part):
    rows = part.shape[0] // 2
    return part[:rows] + swap(part[rows:].astype(BF16)).astype(F32)


def reduce_slots(sums):
    total = sums[0]
    for part in sums[1:]:
        low = total.astype(BF16)
        moved = ring(low)
        total = part + moved.astype(F32)
    return total


def send_direct(halves):
    count = len(halves)
    return [halves[0]] + [
        lax.ppermute(halves[k], "o", [(j, (j - k) % count) for j in range(count)])
        for k in range(1, count)
    ]


def spread(value):
    return lax.all_to_all(value, "o", 0, 0, tiled=True)


def gather_inner(whole):
    return lax.all_gather(whole, "i", axis=1, tiled=True).reshape(-1, whole.shape[-1])


def sum_inner(rows):
    own = lax.psum_scatter(
        rows.reshape(-1, rows.shape[-1]), "i", scatter_dimension=0, tiled=True
    )
    return own.reshape(lax.axis_size("o"), -1, rows.shape[-1])


def send_parts(parts):
    count, at = lax.axis_size("o"), lax.axis_index("o")
    moved = [lax.dynamic_index_in_dim(parts, at, 0, False)]
    for k in range(1, count):
        part = lax.dynamic_index_in_dim(parts, lax.rem(at + k, count), 0, False)
        moved.append(lax.ppermute(part, "o", [(j, (j + k) % count) for j in range(count)]))
    return moved


def cuts_of(size):
    first = size // 2 // 128 * 128 + 128 if size > 512 else size
    return ((0, first), (first, size - first)) if size > first else ((0, size),)


def per_device(
    inputs,
    segment_ids,
    cotangent,
    branch_weight,
    out_weight,
    ffw_in,
    ffw_out,
    norm_scales,
    branch_bias,
    conv_weight,
    conv_bias,
    gate_weights,
    gate_bias,
    decay_param,
    out_bias,
    ffw_bias,
):
    outer, inner = lax.axis_size("o"), lax.axis_size("i")
    count = outer * inner
    core, along = lax.axis_index("tensor"), lax.axis_index("o")
    tok_rows, width = inputs.shape
    part_width = width // count
    hidden_half = ffw_out.shape[0]
    hidden_part = hidden_half // outer
    taps_count = conv_weight.shape[0]
    rim_rows = taps_count - 1
    heads_half, block_size = gate_weights.shape[1], gate_weights.shape[2]
    width_half = heads_half * block_size

    cuts = cuts_of(hidden_part)
    ffw_out_t = ffw_out.T
    packed = [
        jnp.stack(
            [
                jnp.concatenate(
                    [
                        w[:, k * hidden_part + start : k * hidden_part + start + size]
                        for w in (ffw_in[0], ffw_in[1], ffw_out_t)
                    ],
                    axis=1,
                )
                for k in range(outer)
            ]
        )
        for start, size in cuts
    ]
    (branch_x_full, branch_y_full, out_full_t), parts = gather_weights(
        [branch_weight[0], branch_weight[1], out_weight.T], packed
    )
    ffw_parts = []
    for k, (_, size) in enumerate(cuts):
        whole = gather_inner(parts[k])
        ffw_parts.append((whole[:, : 2 * size], whole[:, 2 * size :]))
    cot_own, branch_x_full = lax.optimization_barrier((half_of(cotangent, core), branch_x_full))
    cot_moved = ring(cot_own)

    source_half = half_of(inputs, core).astype(F32)
    seg_marks = (segment_ids + 1).astype(F32)
    halo = from_behind(
        jnp.concatenate(
            [
                inputs[tok_rows - HALO :].astype(F32),
                jnp.broadcast_to(seg_marks[tok_rows - HALO :, None], (HALO, 128)),
            ],
            axis=1,
        ),
        1,
    )
    marks_after = from_behind(seg_marks[:rim_rows], -1)
    normed_ext = rms_norm(
        jnp.concatenate([halo[:, :width], inputs.astype(F32)], axis=0), norm_scales[0]
    ).astype(BF16)
    normed_low = normed_ext[HALO:]
    marks_ext = jnp.concatenate([halo[:, width], seg_marks])
    same = [
        (marks_ext[HALO - k : HALO - k + tok_rows] == seg_marks).astype(F32)
        for k in range(taps_count)
    ]
    masks = jnp.stack([1.0 - same[1], *same[1:], *[same[0]] * (8 - taps_count)], axis=1)
    branch_ext = mm(normed_ext, branch_x_full) + branch_bias[0]
    branch_y = mm(normed_low, branch_y_full) + branch_bias[1]
    rate = jax.nn.softplus(decay_param)
    row_params = jnp.stack([conv_bias, gate_bias[0], gate_bias[1], rate] + [rate] * 4)
    conv_low, decay_gate, input_gate, cumulative, local_state, ends = mix(
        branch_ext, masks, conv_weight, row_params, gate_weights
    )
    conv_blocks = conv_low.reshape(tok_rows, heads_half, block_size)
    ends, cot_moved = lax.optimization_barrier((ends, cot_moved))
    carry_in = entering(ends, False)
    carry_in, cot_moved = lax.optimization_barrier((carry_in, cot_moved))
    cot_halves = [cot_own, cot_moved]
    for _ in range(2, outer):
        cot_halves.append(ring(cot_halves[-1]))
    states = local_state + cumulative * carry_in
    branch_act, gelu_back = jax.vjp(gelu_tanh, branch_y)
    mixed_in = (states * branch_act).astype(BF16)
    mixed_part = mm_nt(mixed_in, out_full_t)
    residual = (
        source_half
        + half_of(mixed_part, core)
        + swap(half_of(mixed_part, 1 - core))
        + out_bias[0]
    )

    normed_slots = gather_slots(rms_norm(residual, norm_scales[1]).astype(BF16))
    cot_slots = [[half, swap(half)] for half in cot_halves[:outer]]
    normed_joined = [jnp.concatenate(slot) for slot in normed_slots]
    cot_joined = [jnp.concatenate(slot) for slot in cot_slots]
    bias_part = lax.dynamic_slice_in_dim(ffw_bias, along * hidden_part, hidden_part, 1)
    slots = range(outer)
    hidden_of, delta_of, inner_sums, bias_sums, rows = [], [], [], [], None
    for p, (start, size) in enumerate(cuts):
        if rows is not None:
            rows, normed_joined, cot_joined = lax.optimization_barrier(
                (rows, normed_joined, cot_joined)
            )
            inner_sums.append(sum_inner(rows))
        in_full, out_full = ffw_parts[p]
        bias_row = bias_part[:, start : start + size].reshape(2 * size)
        hiddens, deltas = [], []
        for k in slots:
            gate_up = mm(normed_joined[k], in_full) + bias_row
            hidden, hidden_back = jax.vjp(geglu, gate_up[:, :size], gate_up[:, size:])
            hiddens.append(hidden.astype(BF16))
            deltas.append(
                jnp.concatenate(hidden_back(mm(cot_joined[k], out_full)), axis=1).astype(BF16)
            )
        if p == len(cuts) - 1:
            delta_parts = [
                sum(mm_nt(d[k], w[0]) for d, w in zip(delta_of + [deltas], ffw_parts))
                for k in slots
            ]
            sums = [both_cores(part) for part in delta_parts[1:] + delta_parts[:1]]
            _, hiddens, deltas = lax.optimization_barrier((sums[0], hiddens, deltas))
        hidden_of.append(hiddens)
        delta_of.append(deltas)
        bias_sums.append(
            sum(jnp.sum(d, axis=0, dtype=F32) for d in deltas).reshape(2, size)
        )
        rows = grads_rows([list(zip(normed_slots, deltas)), list(zip(cot_slots, hiddens))])
    inner_sums.append(sum_inner(rows))
    delta_normed_two = reduce_slots(sums)
    result_parts = [
        sum(mm_nt(hidden_of[p][k], ffw_parts[p][1]) for p in range(len(cuts))) for k in slots
    ]
    result_parts = [both_cores(part) for part in result_parts]
    result_parts = [result_parts[0]] + [part.astype(BF16) for part in result_parts[1:]]
    delta_normed_two, result_parts, inner_sums[0] = lax.optimization_barrier(
        (delta_normed_two, result_parts, inner_sums[0])
    )
    grads = [spread(inner_sums[0])]
    grad_ffw_bias = lax.dynamic_update_slice_in_dim(
        jnp.zeros((2, hidden_half), F32),
        jnp.concatenate(bias_sums, axis=1),
        along * hidden_part,
        1,
    )

    cot_half = half_of(cotangent, core).astype(F32)
    delta_res_norm, grad_scale_two = norm_back(residual, norm_scales[1], delta_normed_two)
    delta_residual = cot_half + delta_res_norm
    delta_half = delta_residual.astype(BF16)
    delta_mixed = join_halves(delta_half, swap(delta_half), core)
    delta_mixed_in = mm(delta_mixed, out_full_t)
    delta_states = delta_mixed_in * branch_act
    (delta_branch_y,) = gelu_back(delta_mixed_in * states)
    delta_y_low = delta_branch_y.astype(BF16)
    oy_rows = grads_rows([[([delta_mixed], mixed_in)], [([normed_low], delta_y_low)]])
    grad_oy_inner = sum_inner(oy_rows)
    reset = masks[:, :1]
    log_decay = -8.0 * decay_gate * rate
    decay = jnp.exp(log_decay)
    keep_rate = decay * (1.0 - reset)
    alpha_next = jnp.concatenate([keep_rate[1:], jnp.ones((1, width_half), F32)], axis=0)
    suffix, local_adjoint = local_scan(alpha_next, delta_states, True)
    leaving = entering(
        jnp.stack([keep_rate[0] * suffix[0], keep_rate[0] * local_adjoint[0]]), True
    )
    leaving, inner_sums[1:] = lax.optimization_barrier((leaving, inner_sums[1:]))
    for k in range(1, len(cuts)):
        grads.append(spread(inner_sums[k]))
    adjoint = local_adjoint + suffix * leaving
    states_before = jnp.concatenate([carry_in[None, :], states[: tok_rows - 1]], axis=0)
    conv_float = conv_low.astype(F32)
    room = -jnp.expm1(2.0 * log_decay)
    multiplier = jnp.sqrt(jnp.maximum(room, 0.001)) * (1.0 - reset) + reset
    drawn = adjoint * input_gate
    delta_log = keep_rate * (
        adjoint * states_before
        - jnp.where(room > 0.001, drawn * conv_float * decay / multiplier, 0.0)
    )
    decay_sum = jnp.sum(delta_log * decay_gate, axis=0)
    delta_conv_direct = drawn * multiplier
    delta_gates = jnp.stack(
        [
            delta_log * (-8.0 * rate) * decay_gate * (1.0 - decay_gate),
            delta_conv_direct * conv_float * (1.0 - input_gate),
        ]
    ).astype(BF16)
    grad_decay = -8.0 * decay_sum * jax.nn.sigmoid(decay_param)
    delta_blocks = delta_gates.reshape(2, tok_rows, heads_half, block_size)
    grad_gate_weights = jnp.einsum(
        "thb,gthc->ghbc", conv_blocks, delta_blocks, preferred_element_type=F32
    )
    gate_rows = (
        grad_gate_weights.reshape(2, heads_half, count, block_size // count, block_size)
        .transpose(2, 0, 1, 3, 4)
        .reshape(outer, inner, -1, width_half)
        .astype(BF16)
    )
    grad_gate_bias = jnp.sum(delta_gates, axis=1, dtype=F32)
    delta_conv = delta_conv_direct + jnp.einsum(
        "gthc,ghbc->thb", delta_blocks, gate_weights, preferred_element_type=F32
    ).reshape(tok_rows, width_half)
    rim_delta = from_behind(delta_conv[:rim_rows], -1)
    rim_delta, result_parts = lax.optimization_barrier((rim_delta, result_parts))
    result_moved = send_direct(result_parts)
    ffw_in_grad = jnp.concatenate(
        [
            grad[:, :, : 2 * size].reshape(outer, part_width, 2, size)
            for grad, (_, size) in zip(grads, cuts)
        ],
        axis=3,
    )
    ffw_in_grad = (
        ffw_in_grad.transpose(2, 1, 0, 3).reshape(2, part_width, hidden_half).astype(F32)
    )
    ffw_out_grad = jnp.concatenate(
        [grad[:, :, 2 * size :] for grad, (_, size) in zip(grads, cuts)], axis=2
    )
    ffw_out_grad = ffw_out_grad.transpose(0, 2, 1).reshape(hidden_half, part_width).astype(F32)
    padded_delta = jnp.concatenate([delta_conv, rim_delta], axis=0)
    next_marks = jnp.concatenate([seg_marks, marks_after], axis=0)
    delta_branch_x = jnp.zeros_like(delta_conv)
    conv_weight_rows = []
    for offset in range(taps_count):
        matches = (next_marks[offset : offset + tok_rows] == seg_marks).astype(F32)[:, None]
        delta_branch_x = (
            delta_branch_x
            + conv_weight[offset] * padded_delta[offset : offset + tok_rows] * matches
        )
        shifted = branch_ext[HALO - offset : HALO - offset + tok_rows] * same[offset][:, None]
        conv_weight_rows.append(jnp.sum(delta_conv * shifted, axis=0))
    grad_conv_bias = jnp.sum(delta_conv, axis=0)
    delta_x_low = delta_branch_x.astype(BF16)
    x_rows = grads_rows([[([normed_low], delta_x_low)]], gate_rows)
    grad_x_inner = sum_inner(x_rows)
    delta_part = mm_nt(delta_x_low, branch_x_full) + mm_nt(delta_y_low, branch_y_full)
    delta_normed = half_of(delta_part, core) + swap(
        half_of(delta_part, 1 - core).astype(BF16)
    ).astype(F32)
    delta_source_norm, grad_scale_one = norm_back(source_half, norm_scales[0], delta_normed)
    grad_half = delta_residual + delta_source_norm
    input_grad = join_halves(grad_half, swap(grad_half), core)

    halves = jnp.stack(
        [
            grad_scale_one,
            grad_scale_two,
            jnp.sum(delta_half, axis=0, dtype=F32),
            jnp.sum(cot_half, axis=0),
        ]
    )
    halves = halves + swap(halves)
    flat = [
        halves.reshape(-1),
        jnp.sum(delta_x_low, axis=0, dtype=F32),
        jnp.sum(delta_y_low, axis=0, dtype=F32),
        *conv_weight_rows,
        grad_conv_bias,
        grad_gate_bias.reshape(-1),
        grad_decay,
        grad_ffw_bias.reshape(-1),
    ]
    oy_moved = send_parts(grad_oy_inner)
    small = sum_over_all(jnp.concatenate(flat).reshape(-1, 128))
    result_half = residual + sum(part.astype(F32) for part in result_moved) + out_bias[1]
    result = join_halves(result_half, swap(result_half), core)
    grad_x_inner, input_grad, result, ffw_in_grad, ffw_out_grad = lax.optimization_barrier(
        (grad_x_inner, input_grad, result, ffw_in_grad, ffw_out_grad)
    )
    x_moved = send_parts(grad_x_inner)
    grad_oy = sum(part.astype(F32) for part in oy_moved)
    grad_x_gate = sum(part.astype(F32) for part in x_moved)
    grad_branch_x = grad_x_gate[:part_width]
    gate_grad = grad_x_gate[part_width:].reshape(2, heads_half, block_size // count, block_size)
    small = small.reshape(-1)
    at = 0
    taken = []
    for shape in (
        (2, width),
        (2, width),
        (2, width_half),
        (taps_count, width_half),
        (width_half,),
        (2, width_half),
        (width_half,),
        (2, hidden_half),
    ):
        size = 1
        for n in shape:
            size *= n
        taken.append(small[at : at + size].reshape(shape))
        at += size
    scales, out_bias_grad, branch_bias_grad, taps_grad, conv_bias_grad, gate_bias_grad, decay_grad, ffw_bias_grad = taken
    return (
        result,
        input_grad,
        jnp.stack([grad_branch_x, grad_oy[:, width_half:]]),
        grad_oy[:, :width_half].T,
        ffw_in_grad,
        ffw_out_grad,
        scales,
        branch_bias_grad,
        taps_grad,
        conv_bias_grad,
        gate_grad,
        gate_bias_grad,
        decay_grad,
        out_bias_grad,
        ffw_bias_grad,
    )


def solution(mesh):
    count = mesh.shape["dp"]
    grid = Mesh(
        mesh.devices.reshape(count // INNER, INNER, mesh.shape["tensor"]), ("o", "i", "tensor")
    )
    in_specs = (
        P(DP, None),
        P(DP),
        P(DP, None),
        P(None, DP, "tensor"),
        P("tensor", DP),
        P(None, DP, "tensor"),
        P("tensor", DP),
        P(),
        P(None, "tensor"),
        P(None, "tensor"),
        P("tensor"),
        P(None, "tensor", None, None),
        P(None, "tensor"),
        P("tensor"),
        P(),
        P(None, "tensor"),
    )
    out_specs = (
        P(DP, None),
        P(DP, None),
        P(None, DP, "tensor"),
        P("tensor", DP),
        P(None, DP, "tensor"),
        P("tensor", DP),
        P(),
        P(None, "tensor"),
        P(None, "tensor"),
        P("tensor"),
        P(None, "tensor", DP, None),
        P(None, "tensor"),
        P("tensor"),
        P(),
        P(None, "tensor"),
    )

    return jax.shard_map(
        per_device, mesh=grid, in_specs=in_specs, out_specs=out_specs, check_vma=False
    )
```

```python
import functools

import jax
import jax.numpy as jnp
from jax import lax
from jax.experimental import pallas as pl
from jax.experimental.pallas import tpu as pltpu
from jax.sharding import Mesh
from jax.sharding import PartitionSpec as P


INNER = 4
DP = ("o", "i")
EPS = 1e-06
F32 = jnp.float32
BF16 = jnp.bfloat16


def swap(value):
    return lax.ppermute(value, "tensor", [(0, 1), (1, 0)])


def ring(value):
    count = lax.axis_size("o")
    return lax.ppermute(value, "o", [(k, (k + 1) % count) for k in range(count)])


def from_behind(value, steps):
    count = lax.axis_size(DP)
    first, last = max(0, -steps), min(count, count - steps)
    return lax.ppermute(value, DP, [(k, k + steps) for k in range(first, last)])


def sum_over_all(value):
    count, bit = lax.axis_size(DP), 1
    while bit < count:
        value = value + lax.ppermute(value, DP, [(k, k ^ bit) for k in range(count)])
        bit *= 2
    return value


def half_of(value, which):
    rows = value.shape[0] // 2
    return lax.dynamic_slice_in_dim(value, which * rows, rows, 0)


def join_halves(own, other, core):
    first = jnp.where(core == 0, own, other)
    second = jnp.where(core == 0, other, own)
    return jnp.concatenate([first, second], axis=0)


def run_scan(reverse, keep_ref, drive_ref, cum_ref, state_ref):
    rows, width = keep_ref.shape
    groups = rows // 8
    place = lax.broadcasted_iota(jnp.int32, (8, width), 0)

    def step(k, carried):
        before_a, before_b = carried
        group = groups - 1 - k if reverse else k
        at = pl.ds(pl.multiple_of(group * 8, 8), 8)
        a, b = keep_ref[at, :], drive_ref[at, :]
        for d in (1, 2, 4):
            far_a = pltpu.roll(a, 8 - d if reverse else d, 0)
            far_b = pltpu.roll(b, 8 - d if reverse else d, 0)
            inside = place < 8 - d if reverse else place >= d
            b = jnp.where(inside, a * far_b + b, b)
            a = jnp.where(inside, a * far_a, a)
        b = a * before_b + b
        a = a * before_a
        cum_ref[at, :] = a
        state_ref[at, :] = b
        edge = slice(0, 1) if reverse else slice(7, 8)
        return (a[edge], b[edge])

    return lax.fori_loop(
        0, groups, step, (jnp.ones((1, width), F32), jnp.zeros((1, width), F32))
    )


def scan_kernel(reverse, keep_ref, drive_ref, cum_ref, state_ref):
    run_scan(reverse, keep_ref, drive_ref, cum_ref, state_ref)


def local_scan(keep, drive, reverse):
    rows, width = keep.shape
    block = 256
    spec = pl.BlockSpec((rows, block), lambda j: (0, j))
    shape = jax.ShapeDtypeStruct((rows, width), F32)
    return pl.pallas_call(
        functools.partial(scan_kernel, reverse),
        grid=(width // block,),
        in_specs=[spec, spec],
        out_specs=[spec, spec],
        out_shape=[shape, shape],
        cost_estimate=pl.CostEstimate(
            flops=20 * rows * width, bytes_accessed=16 * rows * width, transcendentals=0
        ),
    )(keep, drive)


HALO = 16


def mix_kernel(branch_ref, mask_ref, taps_ref, rows_ref, gate_ref, *refs):
    conv_ref, decay_gate_ref, input_gate_ref, cum_ref, state_ref, ends_ref, keep, drive = refs
    rows = conv_ref.shape[0]
    conv = rows_ref[0:1, :] + taps_ref[0:1, :] * branch_ref[HALO : HALO + rows, :]
    for k in range(1, taps_ref.shape[0]):
        shifted = branch_ref[HALO - k : HALO - k + rows, :] * mask_ref[:, k : k + 1]
        conv = conv + taps_ref[k : k + 1, :] * shifted
    low = conv.astype(BF16)
    conv_ref[...] = low
    decay_gate = jax.nn.sigmoid(mm(low, gate_ref[0, 0]) + rows_ref[1:2, :])
    input_gate = jax.nn.sigmoid(mm(low, gate_ref[1, 0]) + rows_ref[2:3, :])
    decay_gate_ref[...] = decay_gate
    input_gate_ref[...] = input_gate
    reset = mask_ref[:, 0:1]
    log_decay = -8.0 * decay_gate * rows_ref[3:4, :]
    multiplier = jnp.sqrt(jnp.maximum(1.0 - jnp.exp(2.0 * log_decay), 0.001))
    keep[...] = jnp.exp(log_decay) * (1.0 - reset)
    drive[...] = low.astype(F32) * input_gate * (multiplier * (1.0 - reset) + reset)
    ends_ref[0:1, :], ends_ref[1:2, :] = run_scan(False, keep, drive, cum_ref, state_ref)


def mix(branch, masks, taps, row_params, gate_weights):
    rows, width = branch.shape[0] - HALO, branch.shape[1]
    block = gate_weights.shape[2]
    over = lambda n: pl.BlockSpec((n, block), lambda h: (0, h))
    full = jax.ShapeDtypeStruct((rows, width), F32)
    return pl.pallas_call(
        mix_kernel,
        grid=(width // block,),
        in_specs=[
            over(rows + HALO),
            pl.BlockSpec(masks.shape, lambda h: (0, 0)),
            over(taps.shape[0]),
            over(row_params.shape[0]),
            pl.BlockSpec((2, 1, block, block), lambda h: (0, h, 0, 0)),
        ],
        out_specs=[over(rows)] * 5 + [over(2)],
        out_shape=[
            jax.ShapeDtypeStruct((rows, width), BF16),
            full,
            full,
            full,
            full,
            jax.ShapeDtypeStruct((2, width), F32),
        ],
        scratch_shapes=[pltpu.VMEM((rows, block), F32)] * 2,
        cost_estimate=pl.CostEstimate(
            flops=4 * rows * width * block,
            bytes_accessed=22 * rows * width,
            transcendentals=8 * rows * width,
        ),
    )(branch, masks, taps, row_params, gate_weights)


MESH_ID = pl.DeviceIdType.MESH
VMEM = pl.BlockSpec(memory_space=pltpu.VMEM)
ANY = pl.BlockSpec(memory_space=pl.ANY)


def enter_kernel(outer, inner, reverse, ends_ref, carry_ref, every, send_sem, recv_sem):
    count = outer * inner
    core = lax.axis_index("tensor")
    me = lax.axis_index("o") * inner + lax.axis_index("i")
    barrier = pltpu.get_barrier_semaphore()
    for k in range(1, count):
        peer = lax.rem(me + k, count)
        to = (peer // inner, lax.rem(peer, inner), core)
        pl.semaphore_signal(barrier, inc=1, device_id=to, device_id_type=MESH_ID)
    pl.semaphore_wait(barrier, count - 1)

    def copy(k, mine):
        peer = lax.rem(me + k, count)
        return pltpu.make_async_remote_copy(
            src_ref=ends_ref,
            dst_ref=every.at[me if mine else peer],
            send_sem=send_sem.at[k],
            recv_sem=recv_sem.at[me if mine else peer],
            device_id=(peer // inner, lax.rem(peer, inner), core),
            device_id_type=MESH_ID,
        )

    for k in range(1, count):
        copy(k, True).start()
    for k in range(1, count):
        copy(k, False).wait_recv()
    carried = jnp.zeros((1, ends_ref.shape[1]), F32)
    for k in range(count):
        at = count - 1 - k if reverse else k
        reached = at > me if reverse else at < me
        block = every[at]
        carried = jnp.where(reached, block[0:1] * carried + block[1:2], carried)
    carry_ref[...] = carried
    for k in range(1, count):
        copy(k, True).wait_send()


def entering(ends, reverse):
    outer, inner = lax.axis_size("o"), lax.axis_size("i")
    count, width = outer * inner, ends.shape[1]
    carried = pl.pallas_call(
        functools.partial(enter_kernel, outer, inner, reverse),
        in_specs=[VMEM],
        out_specs=VMEM,
        out_shape=jax.ShapeDtypeStruct((1, width), F32),
        scratch_shapes=[
            pltpu.VMEM((count, 2, width), F32),
            pltpu.SemaphoreType.DMA((count,)),
            pltpu.SemaphoreType.DMA((count,)),
        ],
        compiler_params=pltpu.CompilerParams(
            collective_id=2 if reverse else 1, has_side_effects=True
        ),
    )(ends)
    return carried[0]


def gather_kernel(outer, inner, groups, cuts, *refs):
    parts = len(cuts)
    own, refs = refs[:groups], refs[groups:]
    in_ref, out_ref, source_ref, scale_ref, edge_ref, first_ref = refs[:6]
    refs = refs[6:]
    full, got, refs = refs[:groups], refs[groups : groups + parts], refs[groups + parts :]
    normed_ref, before_ref, after_ref = refs[:3]
    send, refs = refs[3 : 3 + parts], refs[3 + parts :]
    line_send, line_recv, side_send, side_recv, half_send, half_recv, part_send, part_recv = refs[:8]
    edge_send, edge_recv, local = refs[8:]
    o, i, core = lax.axis_index("o"), lax.axis_index("i"), lax.axis_index("tensor")
    sides = (i + 1 - 2 * lax.rem(i, 2), lax.rem(i + 2, 4))
    far = lax.rem(sides[0] + 2, 4)
    lanes = own[0].shape[1] // 2

    barrier = pltpu.get_barrier_semaphore()
    for k in range(1, outer):
        pl.semaphore_signal(
            barrier, inc=1, device_id=(lax.rem(o + k, outer), i, core), device_id_type=MESH_ID
        )
    for side in sides:
        pl.semaphore_signal(barrier, inc=1, device_id=(o, side, core), device_id_type=MESH_ID)
    count = outer * inner
    me = o * inner + i
    beside = []
    for step in (1, count - 1):
        at = lax.rem(me + step, count)
        beside.append((at // inner, lax.rem(at, inner), core))
        pl.semaphore_signal(barrier, inc=1, device_id=beside[-1], device_id_type=MESH_ID)
    pl.semaphore_wait(barrier, outer + 3)

    def remote(src, dst, send_sem, recv_sem, to):
        return pltpu.make_async_remote_copy(
            src_ref=src,
            dst_ref=dst,
            send_sem=send_sem,
            recv_sem=recv_sem,
            device_id=to,
            device_id_type=MESH_ID,
        )

    edges = [
        remote(edge_ref, before_ref, edge_send.at[0], edge_recv.at[0], beside[0]),
        remote(first_ref, after_ref, edge_send.at[1], edge_recv.at[1], beside[1]),
    ]
    for edge in edges:
        edge.start()

    def block(g, k, j):
        return full[g].at[k, j]

    def along_line(g, k, mine, step):
        return remote(
            own[g] if mine else block(g, k, i),
            block(g, k, i),
            line_send.at[g, k, step],
            line_recv.at[g, k],
            (o + 2 * step - 1, i, core),
        )

    def to_side(g, k, mine, side):
        return remote(
            own[g] if mine else block(g, k, i),
            block(g, k, i),
            side_send.at[g, k, side],
            side_recv.at[g, k, side],
            (o, sides[side], core),
        )

    def from_side(g, k, side):
        return remote(
            block(g, k, sides[side]),
            block(g, k, sides[side]),
            side_send.at[g, k, side],
            side_recv.at[g, k, side],
            (o, sides[side], core),
        )

    def half(g, k, side, to):
        part = full[g].at[k, side, :, pl.ds(lanes * to, lanes)]
        return remote(
            part, part, half_send.at[g, k, to], half_recv.at[g, k, to], (o, sides[to], core)
        )

    def visit(first, then):
        first(o)
        for d in range(1, outer):
            pl.when(o - d >= 0)(functools.partial(then, o - d, True))
            pl.when(o + d < outer)(functools.partial(then, o + d, False))

    for g in range(groups):
        pltpu.make_async_copy(own[g], block(g, o, i), local.at[g]).start()
        pl.when(o + 1 < outer)(lambda g=g: along_line(g, o, True, 1).start())
        pl.when(o > 0)(lambda g=g: along_line(g, o, True, 0).start())
        for side in range(2):
            to_side(g, o, True, side).start()

    hidden = in_ref.shape[2] // outer
    for p, (start, size) in enumerate(cuts):
        for k in range(outer):
            at = slice(k * hidden + start, k * hidden + start + size)
            send[p][k, :, :size] = in_ref[0, :, at]
            send[p][k, :, size : 2 * size] = in_ref[1, :, at]
            send[p][k, :, 2 * size :] = out_ref[:, at]
    tokens, width = source_ref.shape

    def normed(values):
        inverse = lax.rsqrt(jnp.mean(values * values, axis=-1, keepdims=True) + EPS)
        return (values * inverse * scale_ref[...]).astype(BF16)

    def norm_rows(k, _):
        at = pl.multiple_of(k * HALO, HALO)
        rows = source_ref[pl.ds(at, HALO), :].astype(F32)
        normed_ref[pl.ds(at + HALO, HALO), :] = normed(rows)
        return _

    lax.fori_loop(0, tokens // HALO, norm_rows, 0)
    for edge in edges:
        edge.wait()
    normed_ref[:HALO, :] = normed(before_ref[:, :width])

    def pass_on(k, from_left):
        for g in range(groups):
            along_line(g, k, False, 0).wait_recv()
            if from_left:
                pl.when(o + 1 < outer)(lambda g=g: along_line(g, k, False, 1).start())
            else:
                pl.when(o > 0)(lambda g=g: along_line(g, k, False, 0).start())
            for side in range(2):
                to_side(g, k, False, side).start()

    visit(lambda k: None, pass_on)

    def part(p, k, mine):
        peer = lax.rem(o + k, outer)
        return remote(
            send[p].at[peer],
            got[p].at[o if mine else peer],
            part_send.at[p, k],
            part_recv.at[p, o if mine else peer],
            (peer, i, core),
        )

    for p in range(parts):
        pltpu.make_async_copy(send[p].at[o], got[p].at[o], local.at[groups + p]).start()
        for k in range(1, outer):
            part(p, k, True).start()

    def turn(k, _=None):
        for g in range(groups):
            for side in range(2):
                from_side(g, k, side).wait_recv()
                half(g, k, sides[side], 1 - side).start()

    visit(turn, turn)

    def finish(k, _=None):
        for g in range(groups):
            for side in range(2):
                half(g, k, far, side).wait_recv()

    visit(finish, finish)
    for p in range(parts):
        for k in range(1, outer):
            part(p, k, False).wait_recv()

    def sent(k, from_left):
        for g in range(groups):
            if from_left is None or from_left:
                pl.when(o + 1 < outer)(lambda g=g: along_line(g, k, False, 1).wait_send())
            if not from_left:
                pl.when(o > 0)(lambda g=g: along_line(g, k, False, 0).wait_send())
            for side in range(2):
                to_side(g, k, False, side).wait_send()
                half(g, k, sides[side], 1 - side).wait_send()

    visit(functools.partial(sent, from_left=None), sent)
    for p in range(parts):
        for k in range(1, outer):
            part(p, k, True).wait_send()
    for g in range(groups):
        pltpu.make_async_copy(own[g], block(g, o, i), local.at[g]).wait()
    for p in range(parts):
        pltpu.make_async_copy(send[p].at[o], got[p].at[o], local.at[groups + p]).wait()


def gather_weights(own, ffw_in, ffw_out_t, source, scale, edge, first, cuts):
    outer, inner = lax.axis_size("o"), lax.axis_size("i")
    groups, parts = len(own), len(cuts)
    dma = pltpu.SemaphoreType.DMA
    blocks = [(outer, own[0].shape[0], 3 * size) for _, size in cuts]
    shape = jax.ShapeDtypeStruct
    out_shape = [shape((outer, inner, *w.shape), BF16) for w in own]
    out_shape += [shape(block, BF16) for block in blocks]
    out_shape += [
        shape((HALO + source.shape[0], source.shape[1]), BF16),
        shape(edge.shape, F32),
        shape(first.shape, F32),
    ]
    result = pl.pallas_call(
        functools.partial(gather_kernel, outer, inner, groups, cuts),
        in_specs=[VMEM] * (groups + 6),
        out_specs=[ANY] * (groups + parts) + [VMEM] * 3,
        out_shape=out_shape,
        scratch_shapes=[pltpu.VMEM(block, BF16) for block in blocks]
        + [
            dma((groups, outer, 2)),
            dma((groups, outer)),
            dma((groups, outer, 2)),
            dma((groups, outer, 2)),
            dma((groups, outer, 2)),
            dma((groups, outer, 2)),
            dma((parts, outer)),
            dma((parts, outer)),
            dma((2,)),
            dma((2,)),
            dma((groups + parts,)),
        ],
        compiler_params=pltpu.CompilerParams(collective_id=0, has_side_effects=True),
    )(*own, ffw_in, ffw_out_t, source, scale, edge, first)
    full = [w.reshape(-1, w.shape[-1]) for w in result[:groups]]
    return full, result[groups : groups + parts], result[groups + parts :]


def grads_kernel(plan, added, *refs):
    out_ref = refs[-1]
    inner, _, rows, _ = out_ref.shape
    take = rows - added
    if added:
        out_ref[:, 0, take:, :] = refs[-2][0]
    refs = iter(refs)
    at = 0
    for terms in plan:
        total = None
        for pieces in terms:
            a = [next(refs)[...] for _ in range(pieces)]
            term = mm_tn(jnp.concatenate(a) if pieces > 1 else a[0], next(refs)[...])
            total = term if total is None else total + term
        size = total.shape[1]
        out_ref[:, 0, :take, at : at + size] = total.astype(BF16).reshape(inner, take, size)
        at += size


def grads_rows(columns, extra=None):
    outer, inner = lax.axis_size("o"), lax.axis_size("i")
    width = columns[0][0][0][0].shape[1]
    block = width // outer
    rows = block // inner
    size = sum(terms[0][1].shape[1] for terms in columns)
    tokens = sum(b.shape[0] for _, b in columns[0])
    added = 0 if extra is None else extra.shape[2]
    if block % 128:
        whole = [
            sum(mm_tn(jnp.concatenate(a), b) for a, b in terms).astype(BF16) for terms in columns
        ]
        whole = jnp.concatenate(whole, axis=1).reshape(outer, inner, rows, size)
        if added:
            whole = jnp.concatenate([whole, extra], axis=2)
        return whole.transpose(1, 0, 2, 3).reshape(inner, -1, size)
    specs, given = [], []
    for terms in columns:
        for a, b in terms:
            for piece in a:
                specs.append(pl.BlockSpec((piece.shape[0], block), lambda k: (0, k)))
                given.append(piece)
            specs.append(pl.BlockSpec(b.shape, lambda k: (0, 0)))
            given.append(b)
    if added:
        specs.append(pl.BlockSpec((1, inner, added, size), lambda k: (k, 0, 0, 0)))
        given.append(extra)
    plan = tuple(tuple(len(a) for a, _ in terms) for terms in columns)
    result = pl.pallas_call(
        functools.partial(grads_kernel, plan, added),
        grid=(outer,),
        in_specs=specs,
        out_specs=pl.BlockSpec((inner, 1, rows + added, size), lambda k: (0, k, 0, 0)),
        out_shape=jax.ShapeDtypeStruct((inner, outer, rows + added, size), BF16),
        cost_estimate=pl.CostEstimate(
            flops=2 * tokens * width * size,
            bytes_accessed=2 * (tokens * (width + size) + width * size),
            transcendentals=0,
        ),
    )(*given)
    return result.reshape(inner, -1, size)


def gelu_tanh(values):
    return jax.nn.gelu(values, approximate=True)


def geglu(gate_vals, up_vals):
    return gelu_tanh(gate_vals) * up_vals


def norm_back(values, scaling, delta):
    inverse = lax.rsqrt(jnp.mean(values * values, axis=-1, keepdims=True) + EPS)
    unit = values * inverse
    scaled = delta * (1.0 + scaling)
    moved = inverse * (scaled - unit * jnp.mean(scaled * unit, axis=-1, keepdims=True))
    return moved, jnp.sum(delta * unit, axis=0)


def rms_norm(values, scaling):
    inverse = lax.rsqrt(jnp.mean(values * values, axis=-1, keepdims=True) + EPS)
    return values * inverse * (1.0 + scaling)


def dot(a, b, contract):
    return lax.dot_general(a, b, ((contract[0], contract[1]), ((), ())), preferred_element_type=F32)


def mm(a, b):
    return dot(a, b, ((1,), (0,)))


def mm_nt(a, b):
    return dot(a, b, ((1,), (1,)))


def mm_tn(a, b):
    return dot(a, b, ((0,), (0,)))


def gather_slots(half):
    slots = []
    for k in range(lax.axis_size("o")):
        if k:
            half = ring(half)
        slots.append([half, swap(half)])
    return slots


def both_cores(part):
    rows = part.shape[0] // 2
    return part[:rows] + swap(part[rows:].astype(BF16)).astype(F32)


def reduce_slots(sums):
    total = sums[0]
    for part in sums[1:]:
        low = total.astype(BF16)
        moved = ring(low)
        total = part + moved.astype(F32)
    return total


def send_direct(halves):
    count = len(halves)
    return [halves[0]] + [
        lax.ppermute(halves[k], "o", [(j, (j - k) % count) for j in range(count)])
        for k in range(1, count)
    ]


def spread(value):
    return lax.all_to_all(value, "o", 0, 0, tiled=True)


def gather_inner(whole):
    return lax.all_gather(whole, "i", axis=1, tiled=True).reshape(-1, whole.shape[-1])


def sum_inner(rows):
    own = lax.psum_scatter(
        rows.reshape(-1, rows.shape[-1]), "i", scatter_dimension=0, tiled=True
    )
    return own.reshape(lax.axis_size("o"), -1, rows.shape[-1])


def send_parts(parts):
    count, at = lax.axis_size("o"), lax.axis_index("o")
    moved = [lax.dynamic_index_in_dim(parts, at, 0, False)]
    for k in range(1, count):
        part = lax.dynamic_index_in_dim(parts, lax.rem(at + k, count), 0, False)
        moved.append(lax.ppermute(part, "o", [(j, (j + k) % count) for j in range(count)]))
    return moved


def cuts_of(size):
    first = size // 2 // 128 * 128 + 128 if size > 512 else size
    return ((0, first), (first, size - first)) if size > first else ((0, size),)


def per_device(
    inputs,
    segment_ids,
    cotangent,
    branch_weight,
    out_weight,
    ffw_in,
    ffw_out,
    norm_scales,
    branch_bias,
    conv_weight,
    conv_bias,
    gate_weights,
    gate_bias,
    decay_param,
    out_bias,
    ffw_bias,
):
    outer, inner = lax.axis_size("o"), lax.axis_size("i")
    count = outer * inner
    core, along = lax.axis_index("tensor"), lax.axis_index("o")
    tok_rows, width = inputs.shape
    part_width = width // count
    hidden_half = ffw_out.shape[0]
    hidden_part = hidden_half // outer
    taps_count = conv_weight.shape[0]
    rim_rows = taps_count - 1
    heads_half, block_size = gate_weights.shape[1], gate_weights.shape[2]
    width_half = heads_half * block_size

    cuts = cuts_of(hidden_part)
    seg_marks = (segment_ids + 1).astype(F32)
    lanes = jnp.broadcast_to(seg_marks[:, None], (tok_rows, 128))
    (branch_x_full, branch_y_full, out_full_t), parts, (normed_ext, before, after) = (
        gather_weights(
            [branch_weight[0], branch_weight[1], out_weight.T],
            ffw_in,
            ffw_out.T,
            inputs,
            1.0 + norm_scales[:1],
            jnp.concatenate([inputs[tok_rows - HALO :].astype(F32), lanes[-HALO:]], axis=1),
            lanes[:HALO],
            cuts,
        )
    )
    ffw_parts = []
    for k, (_, size) in enumerate(cuts):
        whole = gather_inner(parts[k])
        ffw_parts.append((whole[:, : 2 * size], whole[:, 2 * size :]))
    cot_own, branch_x_full = lax.optimization_barrier((half_of(cotangent, core), branch_x_full))
    cot_halves = [cot_own, ring(cot_own)]

    source_half = half_of(inputs, core).astype(F32)
    place = lax.axis_index(DP)
    marks_before = jnp.where(place == 0, 0.0, before[:, width])
    marks_after = jnp.where(place == count - 1, 0.0, after[:rim_rows, 0])
    normed_low = normed_ext[HALO:]
    marks_ext = jnp.concatenate([marks_before, seg_marks])
    same = [
        (marks_ext[HALO - k : HALO - k + tok_rows] == seg_marks).astype(F32)
        for k in range(taps_count)
    ]
    masks = jnp.stack([1.0 - same[1], *same[1:], *[same[0]] * (8 - taps_count)], axis=1)
    branch_ext = mm(normed_ext, branch_x_full) + branch_bias[0]
    branch_y = mm(normed_low, branch_y_full) + branch_bias[1]
    rate = jax.nn.softplus(decay_param)
    row_params = jnp.stack([conv_bias, gate_bias[0], gate_bias[1], rate] + [rate] * 4)
    conv_low, decay_gate, input_gate, cumulative, local_state, ends = mix(
        branch_ext, masks, conv_weight, row_params, gate_weights
    )
    conv_blocks = conv_low.reshape(tok_rows, heads_half, block_size)
    carry_in = entering(ends, False)
    carry_in, cot_halves[-1] = lax.optimization_barrier((carry_in, cot_halves[-1]))
    for k in range(2, outer):
        cot_halves.append(ring(cot_halves[-1]))
    states = local_state + cumulative * carry_in
    branch_act, gelu_back = jax.vjp(gelu_tanh, branch_y)
    mixed_in = (states * branch_act).astype(BF16)
    mixed_part = mm_nt(mixed_in, out_full_t)
    residual = (
        source_half
        + half_of(mixed_part, core)
        + swap(half_of(mixed_part, 1 - core))
        + out_bias[0]
    )

    normed_slots = gather_slots(rms_norm(residual, norm_scales[1]).astype(BF16))
    cot_slots = [[half, swap(half)] for half in cot_halves[:outer]]
    normed_joined = [jnp.concatenate(slot) for slot in normed_slots]
    cot_joined = [jnp.concatenate(slot) for slot in cot_slots]
    bias_part = lax.dynamic_slice_in_dim(ffw_bias, along * hidden_part, hidden_part, 1)
    slots = range(outer)
    hidden_of, delta_of, inner_sums, bias_sums, rows = [], [], [], [], None
    for p, (start, size) in enumerate(cuts):
        if rows is not None:
            rows, normed_joined, cot_joined = lax.optimization_barrier(
                (rows, normed_joined, cot_joined)
            )
            inner_sums.append(sum_inner(rows))
        in_full, out_full = ffw_parts[p]
        bias_row = bias_part[:, start : start + size].reshape(2 * size)
        hiddens, deltas = [], []
        for k in slots:
            gate_up = mm(normed_joined[k], in_full) + bias_row
            hidden, hidden_back = jax.vjp(geglu, gate_up[:, :size], gate_up[:, size:])
            hiddens.append(hidden.astype(BF16))
            deltas.append(
                jnp.concatenate(hidden_back(mm(cot_joined[k], out_full)), axis=1).astype(BF16)
            )
        if p == len(cuts) - 1:
            delta_parts = [
                sum(mm_nt(d[k], w[0]) for d, w in zip(delta_of + [deltas], ffw_parts))
                for k in slots
            ]
            sums = [both_cores(part) for part in delta_parts[1:] + delta_parts[:1]]
            _, hiddens, deltas = lax.optimization_barrier((sums[0], hiddens, deltas))
        hidden_of.append(hiddens)
        delta_of.append(deltas)
        bias_sums.append(
            sum(jnp.sum(d, axis=0, dtype=F32) for d in deltas).reshape(2, size)
        )
        rows = grads_rows([list(zip(normed_slots, deltas)), list(zip(cot_slots, hiddens))])
    inner_sums.append(sum_inner(rows))
    delta_normed_two = reduce_slots(sums)
    result_parts = [
        sum(mm_nt(hidden_of[p][k], ffw_parts[p][1]) for p in range(len(cuts))) for k in slots
    ]
    result_parts = [both_cores(part) for part in result_parts]
    result_parts = [result_parts[0]] + [part.astype(BF16) for part in result_parts[1:]]
    delta_normed_two, result_parts, inner_sums[0] = lax.optimization_barrier(
        (delta_normed_two, result_parts, inner_sums[0])
    )
    grads = [spread(inner_sums[0])]
    grad_ffw_bias = lax.dynamic_update_slice_in_dim(
        jnp.zeros((2, hidden_half), F32),
        jnp.concatenate(bias_sums, axis=1),
        along * hidden_part,
        1,
    )

    cot_half = half_of(cotangent, core).astype(F32)
    delta_res_norm, grad_scale_two = norm_back(residual, norm_scales[1], delta_normed_two)
    delta_residual = cot_half + delta_res_norm
    delta_half = delta_residual.astype(BF16)
    delta_mixed = join_halves(delta_half, swap(delta_half), core)
    delta_mixed_in = mm(delta_mixed, out_full_t)
    delta_states = delta_mixed_in * branch_act
    (delta_branch_y,) = gelu_back(delta_mixed_in * states)
    delta_y_low = delta_branch_y.astype(BF16)
    oy_rows = grads_rows([[([delta_mixed], mixed_in)], [([normed_low], delta_y_low)]])
    grad_oy_inner = sum_inner(oy_rows)
    reset = masks[:, :1]
    log_decay = -8.0 * decay_gate * rate
    decay = jnp.exp(log_decay)
    keep_rate = decay * (1.0 - reset)
    alpha_next = jnp.concatenate([keep_rate[1:], jnp.ones((1, width_half), F32)], axis=0)
    suffix, local_adjoint = local_scan(alpha_next, delta_states, True)
    leaving = entering(
        jnp.stack([keep_rate[0] * suffix[0], keep_rate[0] * local_adjoint[0]]), True
    )
    leaving, inner_sums[1:] = lax.optimization_barrier((leaving, inner_sums[1:]))
    for k in range(1, len(cuts)):
        grads.append(spread(inner_sums[k]))
    adjoint = local_adjoint + suffix * leaving
    states_before = jnp.concatenate([carry_in[None, :], states[: tok_rows - 1]], axis=0)
    conv_float = conv_low.astype(F32)
    room = -jnp.expm1(2.0 * log_decay)
    multiplier = jnp.sqrt(jnp.maximum(room, 0.001)) * (1.0 - reset) + reset
    drawn = adjoint * input_gate
    delta_log = keep_rate * (
        adjoint * states_before
        - jnp.where(room > 0.001, drawn * conv_float * decay / multiplier, 0.0)
    )
    decay_sum = jnp.sum(delta_log * decay_gate, axis=0)
    delta_conv_direct = drawn * multiplier
    delta_gates = jnp.stack(
        [
            delta_log * (-8.0 * rate) * decay_gate * (1.0 - decay_gate),
            delta_conv_direct * conv_float * (1.0 - input_gate),
        ]
    ).astype(BF16)
    grad_decay = -8.0 * decay_sum * jax.nn.sigmoid(decay_param)
    delta_blocks = delta_gates.reshape(2, tok_rows, heads_half, block_size)
    grad_gate_weights = jnp.einsum(
        "thb,gthc->ghbc", conv_blocks, delta_blocks, preferred_element_type=F32
    )
    gate_rows = (
        grad_gate_weights.reshape(2, heads_half, count, block_size // count, block_size)
        .transpose(2, 0, 1, 3, 4)
        .reshape(outer, inner, -1, width_half)
        .astype(BF16)
    )
    grad_gate_bias = jnp.sum(delta_gates, axis=1, dtype=F32)
    delta_conv = delta_conv_direct + jnp.einsum(
        "gthc,ghbc->thb", delta_blocks, gate_weights, preferred_element_type=F32
    ).reshape(tok_rows, width_half)
    rim_delta = from_behind(delta_conv[:rim_rows], -1)
    rim_delta, result_parts = lax.optimization_barrier((rim_delta, result_parts))
    result_moved = send_direct(result_parts)
    ffw_in_grad = jnp.concatenate(
        [
            grad[:, :, : 2 * size].reshape(outer, part_width, 2, size)
            for grad, (_, size) in zip(grads, cuts)
        ],
        axis=3,
    )
    ffw_in_grad = (
        ffw_in_grad.transpose(2, 1, 0, 3).reshape(2, part_width, hidden_half).astype(F32)
    )
    ffw_out_grad = jnp.concatenate(
        [grad[:, :, 2 * size :] for grad, (_, size) in zip(grads, cuts)], axis=2
    )
    ffw_out_grad = ffw_out_grad.transpose(0, 2, 1).reshape(hidden_half, part_width).astype(F32)
    padded_delta = jnp.concatenate([delta_conv, rim_delta], axis=0)
    next_marks = jnp.concatenate([seg_marks, marks_after], axis=0)
    delta_branch_x = jnp.zeros_like(delta_conv)
    conv_weight_rows = []
    for offset in range(taps_count):
        matches = (next_marks[offset : offset + tok_rows] == seg_marks).astype(F32)[:, None]
        delta_branch_x = (
            delta_branch_x
            + conv_weight[offset] * padded_delta[offset : offset + tok_rows] * matches
        )
        shifted = branch_ext[HALO - offset : HALO - offset + tok_rows] * same[offset][:, None]
        conv_weight_rows.append(jnp.sum(delta_conv * shifted, axis=0))
    grad_conv_bias = jnp.sum(delta_conv, axis=0)
    delta_x_low = delta_branch_x.astype(BF16)
    x_rows = grads_rows([[([normed_low], delta_x_low)]], gate_rows)
    grad_x_inner = sum_inner(x_rows)
    delta_part = mm_nt(delta_x_low, branch_x_full) + mm_nt(delta_y_low, branch_y_full)
    delta_normed = half_of(delta_part, core) + swap(
        half_of(delta_part, 1 - core).astype(BF16)
    ).astype(F32)
    delta_source_norm, grad_scale_one = norm_back(source_half, norm_scales[0], delta_normed)
    grad_half = delta_residual + delta_source_norm
    input_grad = join_halves(grad_half, swap(grad_half), core)

    halves = jnp.stack(
        [
            grad_scale_one,
            grad_scale_two,
            jnp.sum(delta_half, axis=0, dtype=F32),
            jnp.sum(cot_half, axis=0),
        ]
    )
    halves = halves + swap(halves)
    flat = [
        halves.reshape(-1),
        jnp.sum(delta_x_low, axis=0, dtype=F32),
        jnp.sum(delta_y_low, axis=0, dtype=F32),
        *conv_weight_rows,
        grad_conv_bias,
        grad_gate_bias.reshape(-1),
        grad_decay,
        grad_ffw_bias.reshape(-1),
    ]
    oy_moved = send_parts(grad_oy_inner)
    small = sum_over_all(jnp.concatenate(flat).reshape(-1, 128))
    result_half = residual + sum(part.astype(F32) for part in result_moved) + out_bias[1]
    result = join_halves(result_half, swap(result_half), core)
    grad_x_inner, input_grad, result, ffw_in_grad, ffw_out_grad = lax.optimization_barrier(
        (grad_x_inner, input_grad, result, ffw_in_grad, ffw_out_grad)
    )
    x_moved = send_parts(grad_x_inner)
    grad_oy = sum(part.astype(F32) for part in oy_moved)
    grad_x_gate = sum(part.astype(F32) for part in x_moved)
    grad_branch_x = grad_x_gate[:part_width]
    gate_grad = grad_x_gate[part_width:].reshape(2, heads_half, block_size // count, block_size)
    small = small.reshape(-1)
    at = 0
    taken = []
    for shape in (
        (2, width),
        (2, width),
        (2, width_half),
        (taps_count, width_half),
        (width_half,),
        (2, width_half),
        (width_half,),
        (2, hidden_half),
    ):
        size = 1
        for n in shape:
            size *= n
        taken.append(small[at : at + size].reshape(shape))
        at += size
    scales, out_bias_grad, branch_bias_grad, taps_grad, conv_bias_grad, gate_bias_grad, decay_grad, ffw_bias_grad = taken
    return (
        result,
        input_grad,
        jnp.stack([grad_branch_x, grad_oy[:, width_half:]]),
        grad_oy[:, :width_half].T,
        ffw_in_grad,
        ffw_out_grad,
        scales,
        branch_bias_grad,
        taps_grad,
        conv_bias_grad,
        gate_grad,
        gate_bias_grad,
        decay_grad,
        out_bias_grad,
        ffw_bias_grad,
    )


def solution(mesh):
    count = mesh.shape["dp"]
    grid = Mesh(
        mesh.devices.reshape(count // INNER, INNER, mesh.shape["tensor"]), ("o", "i", "tensor")
    )
    in_specs = (
        P(DP, None),
        P(DP),
        P(DP, None),
        P(None, DP, "tensor"),
        P("tensor", DP),
        P(None, DP, "tensor"),
        P("tensor", DP),
        P(),
        P(None, "tensor"),
        P(None, "tensor"),
        P("tensor"),
        P(None, "tensor", None, None),
        P(None, "tensor"),
        P("tensor"),
        P(),
        P(None, "tensor"),
    )
    out_specs = (
        P(DP, None),
        P(DP, None),
        P(None, DP, "tensor"),
        P("tensor", DP),
        P(None, DP, "tensor"),
        P("tensor", DP),
        P(),
        P(None, "tensor"),
        P(None, "tensor"),
        P("tensor"),
        P(None, "tensor", DP, None),
        P(None, "tensor"),
        P("tensor"),
        P(),
        P(None, "tensor"),
    )

    return jax.shard_map(
        per_device, mesh=grid, in_specs=in_specs, out_specs=out_specs, check_vma=False
    )
```

```python
import functools

import jax
import jax.numpy as jnp
from jax import lax
from jax.experimental import pallas as pl
from jax.experimental.pallas import tpu as pltpu
from jax.sharding import Mesh
from jax.sharding import PartitionSpec as P


INNER = 4
DP = ("o", "i")
EPS = 1e-06
F32 = jnp.float32
BF16 = jnp.bfloat16


def swap(value):
    return lax.ppermute(value, "tensor", [(0, 1), (1, 0)])


def ring(value):
    count = lax.axis_size("o")
    return lax.ppermute(value, "o", [(k, (k + 1) % count) for k in range(count)])


def from_behind(value, steps):
    count = lax.axis_size(DP)
    first, last = max(0, -steps), min(count, count - steps)
    return lax.ppermute(value, DP, [(k, k + steps) for k in range(first, last)])


def sum_over_all(value):
    count, bit = lax.axis_size(DP), 1
    while bit < count:
        value = value + lax.ppermute(value, DP, [(k, k ^ bit) for k in range(count)])
        bit *= 2
    return value


def half_of(value, which):
    rows = value.shape[0] // 2
    return lax.dynamic_slice_in_dim(value, which * rows, rows, 0)


def join_halves(own, other, core):
    first = jnp.where(core == 0, own, other)
    second = jnp.where(core == 0, other, own)
    return jnp.concatenate([first, second], axis=0)


def run_scan(reverse, keep_ref, drive_ref, cum_ref, state_ref):
    rows, width = keep_ref.shape
    groups = rows // 8
    place = lax.broadcasted_iota(jnp.int32, (8, width), 0)

    def step(k, carried):
        before_a, before_b = carried
        group = groups - 1 - k if reverse else k
        at = pl.ds(pl.multiple_of(group * 8, 8), 8)
        a, b = keep_ref[at, :], drive_ref[at, :]
        for d in (1, 2, 4):
            far_a = pltpu.roll(a, 8 - d if reverse else d, 0)
            far_b = pltpu.roll(b, 8 - d if reverse else d, 0)
            inside = place < 8 - d if reverse else place >= d
            b = jnp.where(inside, a * far_b + b, b)
            a = jnp.where(inside, a * far_a, a)
        b = a * before_b + b
        a = a * before_a
        cum_ref[at, :] = a
        state_ref[at, :] = b
        edge = slice(0, 1) if reverse else slice(7, 8)
        return (a[edge], b[edge])

    return lax.fori_loop(
        0, groups, step, (jnp.ones((1, width), F32), jnp.zeros((1, width), F32))
    )


def scan_kernel(reverse, keep_ref, drive_ref, cum_ref, state_ref):
    run_scan(reverse, keep_ref, drive_ref, cum_ref, state_ref)


def local_scan(keep, drive, reverse):
    rows, width = keep.shape
    block = 256
    spec = pl.BlockSpec((rows, block), lambda j: (0, j))
    shape = jax.ShapeDtypeStruct((rows, width), F32)
    return pl.pallas_call(
        functools.partial(scan_kernel, reverse),
        grid=(width // block,),
        in_specs=[spec, spec],
        out_specs=[spec, spec],
        out_shape=[shape, shape],
        cost_estimate=pl.CostEstimate(
            flops=20 * rows * width, bytes_accessed=16 * rows * width, transcendentals=0
        ),
    )(keep, drive)


HALO = 16


def mix_kernel(branch_ref, mask_ref, taps_ref, rows_ref, gate_ref, *refs):
    conv_ref, decay_gate_ref, input_gate_ref, cum_ref, state_ref, ends_ref, keep, drive = refs
    rows = conv_ref.shape[0]
    conv = rows_ref[0:1, :] + taps_ref[0:1, :] * branch_ref[HALO : HALO + rows, :]
    for k in range(1, taps_ref.shape[0]):
        shifted = branch_ref[HALO - k : HALO - k + rows, :] * mask_ref[:, k : k + 1]
        conv = conv + taps_ref[k : k + 1, :] * shifted
    low = conv.astype(BF16)
    conv_ref[...] = low
    decay_gate = jax.nn.sigmoid(mm(low, gate_ref[0, 0]) + rows_ref[1:2, :])
    input_gate = jax.nn.sigmoid(mm(low, gate_ref[1, 0]) + rows_ref[2:3, :])
    decay_gate_ref[...] = decay_gate
    input_gate_ref[...] = input_gate
    reset = mask_ref[:, 0:1]
    log_decay = -8.0 * decay_gate * rows_ref[3:4, :]
    multiplier = jnp.sqrt(jnp.maximum(1.0 - jnp.exp(2.0 * log_decay), 0.001))
    keep[...] = jnp.exp(log_decay) * (1.0 - reset)
    drive[...] = low.astype(F32) * input_gate * (multiplier * (1.0 - reset) + reset)
    ends_ref[0:1, :], ends_ref[1:2, :] = run_scan(False, keep, drive, cum_ref, state_ref)


def mix(branch, masks, taps, row_params, gate_weights):
    rows, width = branch.shape[0] - HALO, branch.shape[1]
    block = gate_weights.shape[2]
    over = lambda n: pl.BlockSpec((n, block), lambda h: (0, h))
    full = jax.ShapeDtypeStruct((rows, width), F32)
    return pl.pallas_call(
        mix_kernel,
        grid=(width // block,),
        in_specs=[
            over(rows + HALO),
            pl.BlockSpec(masks.shape, lambda h: (0, 0)),
            over(taps.shape[0]),
            over(row_params.shape[0]),
            pl.BlockSpec((2, 1, block, block), lambda h: (0, h, 0, 0)),
        ],
        out_specs=[over(rows)] * 5 + [over(2)],
        out_shape=[
            jax.ShapeDtypeStruct((rows, width), BF16),
            full,
            full,
            full,
            full,
            jax.ShapeDtypeStruct((2, width), F32),
        ],
        scratch_shapes=[pltpu.VMEM((rows, block), F32)] * 2,
        cost_estimate=pl.CostEstimate(
            flops=4 * rows * width * block,
            bytes_accessed=22 * rows * width,
            transcendentals=8 * rows * width,
        ),
    )(branch, masks, taps, row_params, gate_weights)


MESH_ID = pl.DeviceIdType.MESH
VMEM = pl.BlockSpec(memory_space=pltpu.VMEM)
ANY = pl.BlockSpec(memory_space=pl.ANY)


def enter_kernel(outer, inner, reverse, ends_ref, carry_ref, every, send_sem, recv_sem):
    count = outer * inner
    core = lax.axis_index("tensor")
    me = lax.axis_index("o") * inner + lax.axis_index("i")
    barrier = pltpu.get_barrier_semaphore()
    for k in range(1, count):
        peer = lax.rem(me + k, count)
        to = (peer // inner, lax.rem(peer, inner), core)
        pl.semaphore_signal(barrier, inc=1, device_id=to, device_id_type=MESH_ID)
    pl.semaphore_wait(barrier, count - 1)

    def copy(k, mine):
        peer = lax.rem(me + k, count)
        return pltpu.make_async_remote_copy(
            src_ref=ends_ref,
            dst_ref=every.at[me if mine else peer],
            send_sem=send_sem.at[k],
            recv_sem=recv_sem.at[me if mine else peer],
            device_id=(peer // inner, lax.rem(peer, inner), core),
            device_id_type=MESH_ID,
        )

    for k in range(1, count):
        copy(k, True).start()
    for k in range(1, count):
        copy(k, False).wait_recv()
    carried = jnp.zeros((1, ends_ref.shape[1]), F32)
    for k in range(count):
        at = count - 1 - k if reverse else k
        reached = at > me if reverse else at < me
        block = every[at]
        carried = jnp.where(reached, block[0:1] * carried + block[1:2], carried)
    carry_ref[...] = carried
    for k in range(1, count):
        copy(k, True).wait_send()


def entering(ends, reverse):
    outer, inner = lax.axis_size("o"), lax.axis_size("i")
    count, width = outer * inner, ends.shape[1]
    carried = pl.pallas_call(
        functools.partial(enter_kernel, outer, inner, reverse),
        in_specs=[VMEM],
        out_specs=VMEM,
        out_shape=jax.ShapeDtypeStruct((1, width), F32),
        scratch_shapes=[
            pltpu.VMEM((count, 2, width), F32),
            pltpu.SemaphoreType.DMA((count,)),
            pltpu.SemaphoreType.DMA((count,)),
        ],
        compiler_params=pltpu.CompilerParams(
            collective_id=2 if reverse else 1, has_side_effects=True
        ),
    )(ends)
    return carried[0]


def gather_kernel(outer, inner, groups, cuts, *refs):
    parts = len(cuts)
    own, refs = refs[:groups], refs[groups:]
    in_ref, out_ref, source_ref, scale_ref, edge_ref, first_ref = refs[:6]
    refs = refs[6:]
    full, got, refs = refs[:groups], refs[groups : groups + parts], refs[groups + parts :]
    normed_ref, before_ref, after_ref = refs[:3]
    send, refs = refs[3 : 3 + parts], refs[3 + parts :]
    line_send, line_recv, side_send, side_recv, half_send, half_recv, part_send, part_recv = refs[:8]
    edge_send, edge_recv, local = refs[8:]
    o, i, core = lax.axis_index("o"), lax.axis_index("i"), lax.axis_index("tensor")
    sides = (i + 1 - 2 * lax.rem(i, 2), lax.rem(i + 2, 4))
    far = lax.rem(sides[0] + 2, 4)
    lanes = own[0].shape[1] // 2

    barrier = pltpu.get_barrier_semaphore()
    for k in range(1, outer):
        pl.semaphore_signal(
            barrier, inc=1, device_id=(lax.rem(o + k, outer), i, core), device_id_type=MESH_ID
        )
    for side in sides:
        pl.semaphore_signal(barrier, inc=1, device_id=(o, side, core), device_id_type=MESH_ID)
    count = outer * inner
    me = o * inner + i
    beside = []
    for step in (1, count - 1):
        at = lax.rem(me + step, count)
        beside.append((at // inner, lax.rem(at, inner), core))
        pl.semaphore_signal(barrier, inc=1, device_id=beside[-1], device_id_type=MESH_ID)
    pl.semaphore_wait(barrier, outer + 3)

    def remote(src, dst, send_sem, recv_sem, to):
        return pltpu.make_async_remote_copy(
            src_ref=src,
            dst_ref=dst,
            send_sem=send_sem,
            recv_sem=recv_sem,
            device_id=to,
            device_id_type=MESH_ID,
        )

    edges = [
        remote(edge_ref, before_ref, edge_send.at[0], edge_recv.at[0], beside[0]),
        remote(first_ref, after_ref, edge_send.at[1], edge_recv.at[1], beside[1]),
    ]
    for edge in edges:
        edge.start()

    def block(g, k, j):
        return full[g].at[k, j]

    def along_line(g, k, mine, step):
        return remote(
            own[g] if mine else block(g, k, i),
            block(g, k, i),
            line_send.at[g, k, step],
            line_recv.at[g, k],
            (o + 2 * step - 1, i, core),
        )

    def to_side(g, k, mine, side):
        return remote(
            own[g] if mine else block(g, k, i),
            block(g, k, i),
            side_send.at[g, k, side],
            side_recv.at[g, k, side],
            (o, sides[side], core),
        )

    def from_side(g, k, side):
        return remote(
            block(g, k, sides[side]),
            block(g, k, sides[side]),
            side_send.at[g, k, side],
            side_recv.at[g, k, side],
            (o, sides[side], core),
        )

    def half(g, k, side, to):
        part = full[g].at[k, side, :, pl.ds(lanes * to, lanes)]
        return remote(
            part, part, half_send.at[g, k, to], half_recv.at[g, k, to], (o, sides[to], core)
        )

    def visit(first, then):
        first(o)
        for d in range(1, outer):
            pl.when(o - d >= 0)(functools.partial(then, o - d, True))
            pl.when(o + d < outer)(functools.partial(then, o + d, False))

    for g in range(groups):
        pltpu.make_async_copy(own[g], block(g, o, i), local.at[g]).start()
        pl.when(o + 1 < outer)(lambda g=g: along_line(g, o, True, 1).start())
        pl.when(o > 0)(lambda g=g: along_line(g, o, True, 0).start())
        for side in range(2):
            to_side(g, o, True, side).start()

    hidden = in_ref.shape[2] // outer
    for p, (start, size) in enumerate(cuts):
        for k in range(outer):
            at = slice(k * hidden + start, k * hidden + start + size)
            send[p][k, :, :size] = in_ref[0, :, at]
            send[p][k, :, size : 2 * size] = in_ref[1, :, at]
            send[p][k, :, 2 * size :] = out_ref[:, at]
    tokens, width = source_ref.shape

    def normed(values):
        inverse = lax.rsqrt(jnp.mean(values * values, axis=-1, keepdims=True) + EPS)
        return (values * inverse * scale_ref[...]).astype(BF16)

    def norm_rows(k, _):
        at = pl.multiple_of(k * HALO, HALO)
        rows = source_ref[pl.ds(at, HALO), :].astype(F32)
        normed_ref[pl.ds(at + HALO, HALO), :] = normed(rows)
        return _

    lax.fori_loop(0, tokens // HALO, norm_rows, 0)
    for edge in edges:
        edge.wait()
    normed_ref[:HALO, :] = normed(before_ref[:, :width])

    def pass_on(k, from_left):
        for g in range(groups):
            along_line(g, k, False, 0).wait_recv()
            if from_left:
                pl.when(o + 1 < outer)(lambda g=g: along_line(g, k, False, 1).start())
            else:
                pl.when(o > 0)(lambda g=g: along_line(g, k, False, 0).start())
            for side in range(2):
                to_side(g, k, False, side).start()

    visit(lambda k: None, pass_on)

    def part(p, k, mine):
        peer = lax.rem(o + k, outer)
        return remote(
            send[p].at[peer],
            got[p].at[o if mine else peer],
            part_send.at[p, k],
            part_recv.at[p, o if mine else peer],
            (peer, i, core),
        )

    for p in range(parts):
        pltpu.make_async_copy(send[p].at[o], got[p].at[o], local.at[groups + p]).start()
        for k in range(1, outer):
            part(p, k, True).start()

    def turn(k, _=None):
        for g in range(groups):
            for side in range(2):
                from_side(g, k, side).wait_recv()
                half(g, k, sides[side], 1 - side).start()

    visit(turn, turn)

    def finish(k, _=None):
        for g in range(groups):
            for side in range(2):
                half(g, k, far, side).wait_recv()

    visit(finish, finish)
    for p in range(parts):
        for k in range(1, outer):
            part(p, k, False).wait_recv()

    def sent(k, from_left):
        for g in range(groups):
            if from_left is None or from_left:
                pl.when(o + 1 < outer)(lambda g=g: along_line(g, k, False, 1).wait_send())
            if not from_left:
                pl.when(o > 0)(lambda g=g: along_line(g, k, False, 0).wait_send())
            for side in range(2):
                to_side(g, k, False, side).wait_send()
                half(g, k, sides[side], 1 - side).wait_send()

    visit(functools.partial(sent, from_left=None), sent)
    for p in range(parts):
        for k in range(1, outer):
            part(p, k, True).wait_send()
    for g in range(groups):
        pltpu.make_async_copy(own[g], block(g, o, i), local.at[g]).wait()
    for p in range(parts):
        pltpu.make_async_copy(send[p].at[o], got[p].at[o], local.at[groups + p]).wait()


def gather_weights(own, ffw_in, ffw_out_t, source, scale, edge, first, cuts):
    outer, inner = lax.axis_size("o"), lax.axis_size("i")
    groups, parts = len(own), len(cuts)
    dma = pltpu.SemaphoreType.DMA
    blocks = [(outer, own[0].shape[0], 3 * size) for _, size in cuts]
    shape = jax.ShapeDtypeStruct
    out_shape = [shape((outer, inner, *w.shape), BF16) for w in own]
    out_shape += [shape(block, BF16) for block in blocks]
    out_shape += [
        shape((HALO + source.shape[0], source.shape[1]), BF16),
        shape(edge.shape, F32),
        shape(first.shape, F32),
    ]
    result = pl.pallas_call(
        functools.partial(gather_kernel, outer, inner, groups, cuts),
        in_specs=[VMEM] * (groups + 6),
        out_specs=[ANY] * (groups + parts) + [VMEM] * 3,
        out_shape=out_shape,
        scratch_shapes=[pltpu.VMEM(block, BF16) for block in blocks]
        + [
            dma((groups, outer, 2)),
            dma((groups, outer)),
            dma((groups, outer, 2)),
            dma((groups, outer, 2)),
            dma((groups, outer, 2)),
            dma((groups, outer, 2)),
            dma((parts, outer)),
            dma((parts, outer)),
            dma((2,)),
            dma((2,)),
            dma((groups + parts,)),
        ],
        compiler_params=pltpu.CompilerParams(collective_id=0, has_side_effects=True),
    )(*own, ffw_in, ffw_out_t, source, scale, edge, first)
    full = [w.reshape(-1, w.shape[-1]) for w in result[:groups]]
    return full, result[groups : groups + parts], result[groups + parts :]


def grads_kernel(plan, added, *refs):
    out_ref = refs[-1]
    inner, _, rows, _ = out_ref.shape
    take = rows - added
    if added:
        out_ref[:, 0, take:, :] = refs[-2][0]
    refs = iter(refs)
    at = 0
    for terms in plan:
        total = None
        for pieces in terms:
            a = [next(refs)[...] for _ in range(pieces)]
            term = mm_tn(jnp.concatenate(a) if pieces > 1 else a[0], next(refs)[...])
            total = term if total is None else total + term
        size = total.shape[1]
        out_ref[:, 0, :take, at : at + size] = total.astype(BF16).reshape(inner, take, size)
        at += size


def grads_rows(columns, extra=None):
    outer, inner = lax.axis_size("o"), lax.axis_size("i")
    width = columns[0][0][0][0].shape[1]
    block = width // outer
    rows = block // inner
    size = sum(terms[0][1].shape[1] for terms in columns)
    tokens = sum(b.shape[0] for _, b in columns[0])
    added = 0 if extra is None else extra.shape[2]
    if block % 128:
        whole = [
            sum(mm_tn(jnp.concatenate(a), b) for a, b in terms).astype(BF16) for terms in columns
        ]
        whole = jnp.concatenate(whole, axis=1).reshape(outer, inner, rows, size)
        if added:
            whole = jnp.concatenate([whole, extra], axis=2)
        return whole.transpose(1, 0, 2, 3).reshape(inner, -1, size)
    specs, given = [], []
    for terms in columns:
        for a, b in terms:
            for piece in a:
                specs.append(pl.BlockSpec((piece.shape[0], block), lambda k: (0, k)))
                given.append(piece)
            specs.append(pl.BlockSpec(b.shape, lambda k: (0, 0)))
            given.append(b)
    if added:
        specs.append(pl.BlockSpec((1, inner, added, size), lambda k: (k, 0, 0, 0)))
        given.append(extra)
    plan = tuple(tuple(len(a) for a, _ in terms) for terms in columns)
    result = pl.pallas_call(
        functools.partial(grads_kernel, plan, added),
        grid=(outer,),
        in_specs=specs,
        out_specs=pl.BlockSpec((inner, 1, rows + added, size), lambda k: (0, k, 0, 0)),
        out_shape=jax.ShapeDtypeStruct((inner, outer, rows + added, size), BF16),
        cost_estimate=pl.CostEstimate(
            flops=2 * tokens * width * size,
            bytes_accessed=2 * (tokens * (width + size) + width * size),
            transcendentals=0,
        ),
    )(*given)
    return result.reshape(inner, -1, size)


def gelu_tanh(values):
    return jax.nn.gelu(values, approximate=True)


def geglu(gate_vals, up_vals):
    return gelu_tanh(gate_vals) * up_vals


def norm_back(values, scaling, delta):
    inverse = lax.rsqrt(jnp.mean(values * values, axis=-1, keepdims=True) + EPS)
    unit = values * inverse
    scaled = delta * (1.0 + scaling)
    moved = inverse * (scaled - unit * jnp.mean(scaled * unit, axis=-1, keepdims=True))
    return moved, jnp.sum(delta * unit, axis=0)


def rms_norm(values, scaling):
    inverse = lax.rsqrt(jnp.mean(values * values, axis=-1, keepdims=True) + EPS)
    return values * inverse * (1.0 + scaling)


def dot(a, b, contract):
    return lax.dot_general(a, b, ((contract[0], contract[1]), ((), ())), preferred_element_type=F32)


def mm(a, b):
    return dot(a, b, ((1,), (0,)))


def mm_nt(a, b):
    return dot(a, b, ((1,), (1,)))


def mm_tn(a, b):
    return dot(a, b, ((0,), (0,)))


def gather_slots(half):
    slots = []
    for k in range(lax.axis_size("o")):
        if k:
            half = ring(half)
        slots.append([half, swap(half)])
    return slots


def both_cores(part):
    rows = part.shape[0] // 2
    return part[:rows] + swap(part[rows:].astype(BF16)).astype(F32)


def ring_sum(parts):
    total = parts[0].astype(F32)
    for part in parts[1:]:
        low = total.astype(BF16)
        moved = ring(low)
        total = part.astype(F32) + moved.astype(F32)
    return total


def ring_order(parts):
    count, at = lax.axis_size("o"), lax.axis_index("o")
    return [
        lax.dynamic_index_in_dim(parts, lax.rem(at - k + count, count), 0, False)
        for k in [*range(1, count), 0]
    ]


def spread(value):
    return lax.all_to_all(value, "o", 0, 0, tiled=True)


def gather_inner(whole):
    return lax.all_gather(whole, "i", axis=1, tiled=True).reshape(-1, whole.shape[-1])


def sum_inner(rows):
    own = lax.psum_scatter(
        rows.reshape(-1, rows.shape[-1]), "i", scatter_dimension=0, tiled=True
    )
    return own.reshape(lax.axis_size("o"), -1, rows.shape[-1])


def cuts_of(size):
    first = size // 2 // 128 * 128 + 128 if size > 512 else size
    return ((0, first), (first, size - first)) if size > first else ((0, size),)


def per_device(
    inputs,
    segment_ids,
    cotangent,
    branch_weight,
    out_weight,
    ffw_in,
    ffw_out,
    norm_scales,
    branch_bias,
    conv_weight,
    conv_bias,
    gate_weights,
    gate_bias,
    decay_param,
    out_bias,
    ffw_bias,
):
    outer, inner = lax.axis_size("o"), lax.axis_size("i")
    count = outer * inner
    core, along = lax.axis_index("tensor"), lax.axis_index("o")
    tok_rows, width = inputs.shape
    part_width = width // count
    hidden_half = ffw_out.shape[0]
    hidden_part = hidden_half // outer
    taps_count = conv_weight.shape[0]
    rim_rows = taps_count - 1
    heads_half, block_size = gate_weights.shape[1], gate_weights.shape[2]
    width_half = heads_half * block_size

    cuts = cuts_of(hidden_part)
    seg_marks = (segment_ids + 1).astype(F32)
    lanes = jnp.broadcast_to(seg_marks[:, None], (tok_rows, 128))
    (branch_x_full, branch_y_full, out_full_t), parts, (normed_ext, before, after) = (
        gather_weights(
            [branch_weight[0], branch_weight[1], out_weight.T],
            ffw_in,
            ffw_out.T,
            inputs,
            1.0 + norm_scales[:1],
            jnp.concatenate([inputs[tok_rows - HALO :].astype(F32), lanes[-HALO:]], axis=1),
            lanes[:HALO],
            cuts,
        )
    )
    ffw_parts = []
    for k, (_, size) in enumerate(cuts):
        whole = gather_inner(parts[k])
        ffw_parts.append((whole[:, : 2 * size], whole[:, 2 * size :]))
    cot_own, branch_x_full = lax.optimization_barrier((half_of(cotangent, core), branch_x_full))
    cot_halves = [cot_own, ring(cot_own)]

    source_half = half_of(inputs, core).astype(F32)
    place = lax.axis_index(DP)
    marks_before = jnp.where(place == 0, 0.0, before[:, width])
    marks_after = jnp.where(place == count - 1, 0.0, after[:rim_rows, 0])
    normed_low = normed_ext[HALO:]
    marks_ext = jnp.concatenate([marks_before, seg_marks])
    same = [
        (marks_ext[HALO - k : HALO - k + tok_rows] == seg_marks).astype(F32)
        for k in range(taps_count)
    ]
    masks = jnp.stack([1.0 - same[1], *same[1:], *[same[0]] * (8 - taps_count)], axis=1)
    branch_ext = mm(normed_ext, branch_x_full) + branch_bias[0]
    branch_y = mm(normed_low, branch_y_full) + branch_bias[1]
    rate = jax.nn.softplus(decay_param)
    row_params = jnp.stack([conv_bias, gate_bias[0], gate_bias[1], rate] + [rate] * 4)
    conv_low, decay_gate, input_gate, cumulative, local_state, ends = mix(
        branch_ext, masks, conv_weight, row_params, gate_weights
    )
    conv_blocks = conv_low.reshape(tok_rows, heads_half, block_size)
    for k in range(2, min(3, outer)):
        cot_halves.append(ring(cot_halves[-1]))
    carry_in = entering(ends, False)
    carry_in, cot_halves[-1] = lax.optimization_barrier((carry_in, cot_halves[-1]))
    for k in range(3, outer):
        cot_halves.append(ring(cot_halves[-1]))
    states = local_state + cumulative * carry_in
    branch_act, gelu_back = jax.vjp(gelu_tanh, branch_y)
    mixed_in = (states * branch_act).astype(BF16)
    mixed_part = mm_nt(mixed_in, out_full_t)
    residual = (
        source_half
        + half_of(mixed_part, core)
        + swap(half_of(mixed_part, 1 - core))
        + out_bias[0]
    )

    normed_slots = gather_slots(rms_norm(residual, norm_scales[1]).astype(BF16))
    cot_slots = [[half, swap(half)] for half in cot_halves[:outer]]
    normed_joined = [jnp.concatenate(slot) for slot in normed_slots]
    cot_joined = [jnp.concatenate(slot) for slot in cot_slots]
    bias_part = lax.dynamic_slice_in_dim(ffw_bias, along * hidden_part, hidden_part, 1)
    slots = range(outer)
    hidden_of, delta_of, inner_sums, bias_sums, rows = [], [], [], [], None
    for p, (start, size) in enumerate(cuts):
        if rows is not None:
            rows, normed_joined, cot_joined = lax.optimization_barrier(
                (rows, normed_joined, cot_joined)
            )
            inner_sums.append(sum_inner(rows))
        in_full, out_full = ffw_parts[p]
        bias_row = bias_part[:, start : start + size].reshape(2 * size)
        hiddens, deltas = [], []
        for k in slots:
            gate_up = mm(normed_joined[k], in_full) + bias_row
            hidden, hidden_back = jax.vjp(geglu, gate_up[:, :size], gate_up[:, size:])
            hiddens.append(hidden.astype(BF16))
            deltas.append(
                jnp.concatenate(hidden_back(mm(cot_joined[k], out_full)), axis=1).astype(BF16)
            )
        if p == len(cuts) - 1:
            delta_parts = [
                sum(mm_nt(d[k], w[0]) for d, w in zip(delta_of + [deltas], ffw_parts))
                for k in slots
            ]
            sums = [both_cores(part) for part in delta_parts[1:] + delta_parts[:1]]
            _, hiddens, deltas = lax.optimization_barrier((sums[0], hiddens, deltas))
        hidden_of.append(hiddens)
        delta_of.append(deltas)
        bias_sums.append(
            sum(jnp.sum(d, axis=0, dtype=F32) for d in deltas).reshape(2, size)
        )
        rows = grads_rows([list(zip(normed_slots, deltas)), list(zip(cot_slots, hiddens))])
    inner_sums.append(sum_inner(rows))
    delta_normed_two = ring_sum(sums)
    result_parts = [
        sum(mm_nt(hidden_of[p][k], ffw_parts[p][1]) for p in range(len(cuts))) for k in slots
    ]
    result_parts = [both_cores(part) for part in result_parts]
    result_parts = result_parts[1:] + result_parts[:1]
    delta_normed_two, result_parts, inner_sums[0] = lax.optimization_barrier(
        (delta_normed_two, result_parts, inner_sums[0])
    )
    grads = [spread(inner_sums[0])]
    grad_ffw_bias = lax.dynamic_update_slice_in_dim(
        jnp.zeros((2, hidden_half), F32),
        jnp.concatenate(bias_sums, axis=1),
        along * hidden_part,
        1,
    )

    cot_half = half_of(cotangent, core).astype(F32)
    delta_res_norm, grad_scale_two = norm_back(residual, norm_scales[1], delta_normed_two)
    delta_residual = cot_half + delta_res_norm
    delta_half = delta_residual.astype(BF16)
    delta_mixed = join_halves(delta_half, swap(delta_half), core)
    delta_mixed_in = mm(delta_mixed, out_full_t)
    delta_states = delta_mixed_in * branch_act
    (delta_branch_y,) = gelu_back(delta_mixed_in * states)
    delta_y_low = delta_branch_y.astype(BF16)
    oy_rows = grads_rows([[([delta_mixed], mixed_in)], [([normed_low], delta_y_low)]])
    grad_oy_inner = sum_inner(oy_rows)
    reset = masks[:, :1]
    log_decay = -8.0 * decay_gate * rate
    decay = jnp.exp(log_decay)
    keep_rate = decay * (1.0 - reset)
    alpha_next = jnp.concatenate([keep_rate[1:], jnp.ones((1, width_half), F32)], axis=0)
    suffix, local_adjoint = local_scan(alpha_next, delta_states, True)
    leaving = entering(
        jnp.stack([keep_rate[0] * suffix[0], keep_rate[0] * local_adjoint[0]]), True
    )
    leaving, inner_sums[1:] = lax.optimization_barrier((leaving, inner_sums[1:]))
    for k in range(1, len(cuts)):
        grads.append(spread(inner_sums[k]))
    adjoint = local_adjoint + suffix * leaving
    states_before = jnp.concatenate([carry_in[None, :], states[: tok_rows - 1]], axis=0)
    conv_float = conv_low.astype(F32)
    room = -jnp.expm1(2.0 * log_decay)
    multiplier = jnp.sqrt(jnp.maximum(room, 0.001)) * (1.0 - reset) + reset
    drawn = adjoint * input_gate
    delta_log = keep_rate * (
        adjoint * states_before
        - jnp.where(room > 0.001, drawn * conv_float * decay / multiplier, 0.0)
    )
    decay_sum = jnp.sum(delta_log * decay_gate, axis=0)
    delta_conv_direct = drawn * multiplier
    delta_gates = jnp.stack(
        [
            delta_log * (-8.0 * rate) * decay_gate * (1.0 - decay_gate),
            delta_conv_direct * conv_float * (1.0 - input_gate),
        ]
    ).astype(BF16)
    grad_decay = -8.0 * decay_sum * jax.nn.sigmoid(decay_param)
    delta_blocks = delta_gates.reshape(2, tok_rows, heads_half, block_size)
    grad_gate_weights = jnp.einsum(
        "thb,gthc->ghbc", conv_blocks, delta_blocks, preferred_element_type=F32
    )
    gate_rows = (
        grad_gate_weights.reshape(2, heads_half, count, block_size // count, block_size)
        .transpose(2, 0, 1, 3, 4)
        .reshape(outer, inner, -1, width_half)
        .astype(BF16)
    )
    grad_gate_bias = jnp.sum(delta_gates, axis=1, dtype=F32)
    delta_conv = delta_conv_direct + jnp.einsum(
        "gthc,ghbc->thb", delta_blocks, gate_weights, preferred_element_type=F32
    ).reshape(tok_rows, width_half)
    rim_delta = from_behind(delta_conv[:rim_rows], -1)
    rim_delta, result_parts = lax.optimization_barrier((rim_delta, result_parts))
    result_sum = ring_sum(result_parts)
    ffw_in_grad = jnp.concatenate(
        [
            grad[:, :, : 2 * size].reshape(outer, part_width, 2, size)
            for grad, (_, size) in zip(grads, cuts)
        ],
        axis=3,
    )
    ffw_in_grad = (
        ffw_in_grad.transpose(2, 1, 0, 3).reshape(2, part_width, hidden_half).astype(F32)
    )
    ffw_out_grad = jnp.concatenate(
        [grad[:, :, 2 * size :] for grad, (_, size) in zip(grads, cuts)], axis=2
    )
    ffw_out_grad = ffw_out_grad.transpose(0, 2, 1).reshape(hidden_half, part_width).astype(F32)
    padded_delta = jnp.concatenate([delta_conv, rim_delta], axis=0)
    next_marks = jnp.concatenate([seg_marks, marks_after], axis=0)
    delta_branch_x = jnp.zeros_like(delta_conv)
    conv_weight_rows = []
    for offset in range(taps_count):
        matches = (next_marks[offset : offset + tok_rows] == seg_marks).astype(F32)[:, None]
        delta_branch_x = (
            delta_branch_x
            + conv_weight[offset] * padded_delta[offset : offset + tok_rows] * matches
        )
        shifted = branch_ext[HALO - offset : HALO - offset + tok_rows] * same[offset][:, None]
        conv_weight_rows.append(jnp.sum(delta_conv * shifted, axis=0))
    grad_conv_bias = jnp.sum(delta_conv, axis=0)
    delta_x_low = delta_branch_x.astype(BF16)
    x_rows = grads_rows([[([normed_low], delta_x_low)]], gate_rows)
    grad_x_inner = sum_inner(x_rows)
    delta_part = mm_nt(delta_x_low, branch_x_full) + mm_nt(delta_y_low, branch_y_full)
    delta_normed = half_of(delta_part, core) + swap(
        half_of(delta_part, 1 - core).astype(BF16)
    ).astype(F32)
    delta_source_norm, grad_scale_one = norm_back(source_half, norm_scales[0], delta_normed)
    grad_half = delta_residual + delta_source_norm
    input_grad = join_halves(grad_half, swap(grad_half), core)

    halves = jnp.stack(
        [
            grad_scale_one,
            grad_scale_two,
            jnp.sum(delta_half, axis=0, dtype=F32),
            jnp.sum(cot_half, axis=0),
        ]
    )
    halves = halves + swap(halves)
    flat = [
        halves.reshape(-1),
        jnp.sum(delta_x_low, axis=0, dtype=F32),
        jnp.sum(delta_y_low, axis=0, dtype=F32),
        *conv_weight_rows,
        grad_conv_bias,
        grad_gate_bias.reshape(-1),
        grad_decay,
        grad_ffw_bias.reshape(-1),
    ]
    grad_oy_inner, ffw_in_grad, ffw_out_grad = lax.optimization_barrier(
        (grad_oy_inner, ffw_in_grad, ffw_out_grad)
    )
    grad_oy = ring_sum(ring_order(grad_oy_inner))
    small = sum_over_all(jnp.concatenate(flat).reshape(-1, 128))
    result_half = residual + result_sum + out_bias[1]
    result = join_halves(result_half, swap(result_half), core)
    grad_x_gate = ring_sum(ring_order(grad_x_inner))
    grad_branch_x = grad_x_gate[:part_width]
    gate_grad = grad_x_gate[part_width:].reshape(2, heads_half, block_size // count, block_size)
    small = small.reshape(-1)
    at = 0
    taken = []
    for shape in (
        (2, width),
        (2, width),
        (2, width_half),
        (taps_count, width_half),
        (width_half,),
        (2, width_half),
        (width_half,),
        (2, hidden_half),
    ):
        size = 1
        for n in shape:
            size *= n
        taken.append(small[at : at + size].reshape(shape))
        at += size
    scales, out_bias_grad, branch_bias_grad, taps_grad, conv_bias_grad, gate_bias_grad, decay_grad, ffw_bias_grad = taken
    return (
        result,
        input_grad,
        jnp.stack([grad_branch_x, grad_oy[:, width_half:]]),
        grad_oy[:, :width_half].T,
        ffw_in_grad,
        ffw_out_grad,
        scales,
        branch_bias_grad,
        taps_grad,
        conv_bias_grad,
        gate_grad,
        gate_bias_grad,
        decay_grad,
        out_bias_grad,
        ffw_bias_grad,
    )


def solution(mesh):
    count = mesh.shape["dp"]
    grid = Mesh(
        mesh.devices.reshape(count // INNER, INNER, mesh.shape["tensor"]), ("o", "i", "tensor")
    )
    in_specs = (
        P(DP, None),
        P(DP),
        P(DP, None),
        P(None, DP, "tensor"),
        P("tensor", DP),
        P(None, DP, "tensor"),
        P("tensor", DP),
        P(),
        P(None, "tensor"),
        P(None, "tensor"),
        P("tensor"),
        P(None, "tensor", None, None),
        P(None, "tensor"),
        P("tensor"),
        P(),
        P(None, "tensor"),
    )
    out_specs = (
        P(DP, None),
        P(DP, None),
        P(None, DP, "tensor"),
        P("tensor", DP),
        P(None, DP, "tensor"),
        P("tensor", DP),
        P(),
        P(None, "tensor"),
        P(None, "tensor"),
        P("tensor"),
        P(None, "tensor", DP, None),
        P(None, "tensor"),
        P("tensor"),
        P(),
        P(None, "tensor"),
    )

    return jax.shard_map(
        per_device, mesh=grid, in_specs=in_specs, out_specs=out_specs, check_vma=False
    )
```

```python
import functools

import jax
import jax.numpy as jnp
from jax import lax
from jax.experimental import pallas as pl
from jax.experimental.pallas import tpu as pltpu
from jax.sharding import Mesh
from jax.sharding import PartitionSpec as P


INNER = 4
DP = ("o", "i")
EPS = 1e-06
F32 = jnp.float32
BF16 = jnp.bfloat16


def swap(value):
    return lax.ppermute(value, "tensor", [(0, 1), (1, 0)])


def ring(value):
    count = lax.axis_size("o")
    return lax.ppermute(value, "o", [(k, (k + 1) % count) for k in range(count)])


def from_behind(value, steps):
    count = lax.axis_size(DP)
    first, last = max(0, -steps), min(count, count - steps)
    return lax.ppermute(value, DP, [(k, k + steps) for k in range(first, last)])


def sum_over_all(value):
    count, bit = lax.axis_size(DP), 1
    while bit < count:
        value = value + lax.ppermute(value, DP, [(k, k ^ bit) for k in range(count)])
        bit *= 2
    return value


def half_of(value, which):
    rows = value.shape[0] // 2
    return lax.dynamic_slice_in_dim(value, which * rows, rows, 0)


def join_halves(own, other, core):
    first = jnp.where(core == 0, own, other)
    second = jnp.where(core == 0, other, own)
    return jnp.concatenate([first, second], axis=0)


def run_scan(reverse, keep_ref, drive_ref, cum_ref, state_ref):
    rows, width = keep_ref.shape
    groups = rows // 8
    place = lax.broadcasted_iota(jnp.int32, (8, width), 0)

    def step(k, carried):
        before_a, before_b = carried
        group = groups - 1 - k if reverse else k
        at = pl.ds(pl.multiple_of(group * 8, 8), 8)
        a, b = keep_ref[at, :], drive_ref[at, :]
        for d in (1, 2, 4):
            far_a = pltpu.roll(a, 8 - d if reverse else d, 0)
            far_b = pltpu.roll(b, 8 - d if reverse else d, 0)
            inside = place < 8 - d if reverse else place >= d
            b = jnp.where(inside, a * far_b + b, b)
            a = jnp.where(inside, a * far_a, a)
        b = a * before_b + b
        a = a * before_a
        cum_ref[at, :] = a
        state_ref[at, :] = b
        edge = slice(0, 1) if reverse else slice(7, 8)
        return (a[edge], b[edge])

    return lax.fori_loop(
        0, groups, step, (jnp.ones((1, width), F32), jnp.zeros((1, width), F32))
    )


def scan_kernel(reverse, keep_ref, drive_ref, cum_ref, state_ref):
    run_scan(reverse, keep_ref, drive_ref, cum_ref, state_ref)


def local_scan(keep, drive, reverse):
    rows, width = keep.shape
    block = 256
    spec = pl.BlockSpec((rows, block), lambda j: (0, j))
    shape = jax.ShapeDtypeStruct((rows, width), F32)
    return pl.pallas_call(
        functools.partial(scan_kernel, reverse),
        grid=(width // block,),
        in_specs=[spec, spec],
        out_specs=[spec, spec],
        out_shape=[shape, shape],
        cost_estimate=pl.CostEstimate(
            flops=20 * rows * width, bytes_accessed=16 * rows * width, transcendentals=0
        ),
    )(keep, drive)


HALO = 16


def mix_kernel(branch_ref, mask_ref, taps_ref, rows_ref, gate_ref, *refs):
    conv_ref, decay_gate_ref, input_gate_ref, cum_ref, state_ref, ends_ref, keep, drive = refs
    rows = conv_ref.shape[0]
    conv = rows_ref[0:1, :] + taps_ref[0:1, :] * branch_ref[HALO : HALO + rows, :]
    for k in range(1, taps_ref.shape[0]):
        shifted = branch_ref[HALO - k : HALO - k + rows, :] * mask_ref[:, k : k + 1]
        conv = conv + taps_ref[k : k + 1, :] * shifted
    low = conv.astype(BF16)
    conv_ref[...] = low
    decay_gate = jax.nn.sigmoid(mm(low, gate_ref[0, 0]) + rows_ref[1:2, :])
    input_gate = jax.nn.sigmoid(mm(low, gate_ref[1, 0]) + rows_ref[2:3, :])
    decay_gate_ref[...] = decay_gate
    input_gate_ref[...] = input_gate
    reset = mask_ref[:, 0:1]
    log_decay = -8.0 * decay_gate * rows_ref[3:4, :]
    multiplier = jnp.sqrt(jnp.maximum(1.0 - jnp.exp(2.0 * log_decay), 0.001))
    keep[...] = jnp.exp(log_decay) * (1.0 - reset)
    drive[...] = low.astype(F32) * input_gate * (multiplier * (1.0 - reset) + reset)
    ends_ref[0:1, :], ends_ref[1:2, :] = run_scan(False, keep, drive, cum_ref, state_ref)


def mix(branch, masks, taps, row_params, gate_weights):
    rows, width = branch.shape[0] - HALO, branch.shape[1]
    block = gate_weights.shape[2]
    over = lambda n: pl.BlockSpec((n, block), lambda h: (0, h))
    full = jax.ShapeDtypeStruct((rows, width), F32)
    return pl.pallas_call(
        mix_kernel,
        grid=(width // block,),
        in_specs=[
            over(rows + HALO),
            pl.BlockSpec(masks.shape, lambda h: (0, 0)),
            over(taps.shape[0]),
            over(row_params.shape[0]),
            pl.BlockSpec((2, 1, block, block), lambda h: (0, h, 0, 0)),
        ],
        out_specs=[over(rows)] * 5 + [over(2)],
        out_shape=[
            jax.ShapeDtypeStruct((rows, width), BF16),
            full,
            full,
            full,
            full,
            jax.ShapeDtypeStruct((2, width), F32),
        ],
        scratch_shapes=[pltpu.VMEM((rows, block), F32)] * 2,
        cost_estimate=pl.CostEstimate(
            flops=4 * rows * width * block,
            bytes_accessed=22 * rows * width,
            transcendentals=8 * rows * width,
        ),
    )(branch, masks, taps, row_params, gate_weights)


MESH_ID = pl.DeviceIdType.MESH
VMEM = pl.BlockSpec(memory_space=pltpu.VMEM)
ANY = pl.BlockSpec(memory_space=pl.ANY)


def enter_kernel(outer, inner, reverse, ends_ref, carry_ref, every, send_sem, recv_sem):
    count = outer * inner
    core = lax.axis_index("tensor")
    me = lax.axis_index("o") * inner + lax.axis_index("i")
    barrier = pltpu.get_barrier_semaphore()
    for k in range(1, count):
        peer = lax.rem(me + k, count)
        to = (peer // inner, lax.rem(peer, inner), core)
        pl.semaphore_signal(barrier, inc=1, device_id=to, device_id_type=MESH_ID)
    pl.semaphore_wait(barrier, count - 1)

    def copy(k, mine):
        peer = lax.rem(me + k, count)
        return pltpu.make_async_remote_copy(
            src_ref=ends_ref,
            dst_ref=every.at[me if mine else peer],
            send_sem=send_sem.at[k],
            recv_sem=recv_sem.at[me if mine else peer],
            device_id=(peer // inner, lax.rem(peer, inner), core),
            device_id_type=MESH_ID,
        )

    for k in range(1, count):
        copy(k, True).start()
    for k in range(1, count):
        copy(k, False).wait_recv()
    carried = jnp.zeros((1, ends_ref.shape[1]), F32)
    for k in range(count):
        at = count - 1 - k if reverse else k
        reached = at > me if reverse else at < me
        block = every[at]
        carried = jnp.where(reached, block[0:1] * carried + block[1:2], carried)
    carry_ref[...] = carried
    for k in range(1, count):
        copy(k, True).wait_send()


def entering(ends, reverse):
    outer, inner = lax.axis_size("o"), lax.axis_size("i")
    count, width = outer * inner, ends.shape[1]
    carried = pl.pallas_call(
        functools.partial(enter_kernel, outer, inner, reverse),
        in_specs=[VMEM],
        out_specs=VMEM,
        out_shape=jax.ShapeDtypeStruct((1, width), F32),
        scratch_shapes=[
            pltpu.VMEM((count, 2, width), F32),
            pltpu.SemaphoreType.DMA((count,)),
            pltpu.SemaphoreType.DMA((count,)),
        ],
        compiler_params=pltpu.CompilerParams(
            collective_id=2 if reverse else 1, has_side_effects=True
        ),
    )(ends)
    return carried[0]


def gather_kernel(outer, inner, groups, cuts, *refs):
    parts = len(cuts)
    own, refs = refs[:groups], refs[groups:]
    in_ref, out_ref, source_ref, scale_ref, edge_ref, first_ref = refs[:6]
    refs = refs[6:]
    full, got, refs = refs[:groups], refs[groups : groups + parts], refs[groups + parts :]
    normed_ref, before_ref, after_ref = refs[:3]
    send, refs = refs[3 : 3 + parts], refs[3 + parts :]
    line_send, line_recv, side_send, side_recv, half_send, half_recv, part_send, part_recv = refs[:8]
    edge_send, edge_recv, local = refs[8:]
    o, i, core = lax.axis_index("o"), lax.axis_index("i"), lax.axis_index("tensor")
    sides = (i + 1 - 2 * lax.rem(i, 2), lax.rem(i + 2, 4))
    far = lax.rem(sides[0] + 2, 4)
    lanes = own[0].shape[1] // 2

    barrier = pltpu.get_barrier_semaphore()
    for k in range(1, outer):
        pl.semaphore_signal(
            barrier, inc=1, device_id=(lax.rem(o + k, outer), i, core), device_id_type=MESH_ID
        )
    for side in sides:
        pl.semaphore_signal(barrier, inc=1, device_id=(o, side, core), device_id_type=MESH_ID)
    count = outer * inner
    me = o * inner + i
    beside = []
    for step in (1, count - 1):
        at = lax.rem(me + step, count)
        beside.append((at // inner, lax.rem(at, inner), core))
        pl.semaphore_signal(barrier, inc=1, device_id=beside[-1], device_id_type=MESH_ID)
    pl.semaphore_wait(barrier, outer + 3)

    def remote(src, dst, send_sem, recv_sem, to):
        return pltpu.make_async_remote_copy(
            src_ref=src,
            dst_ref=dst,
            send_sem=send_sem,
            recv_sem=recv_sem,
            device_id=to,
            device_id_type=MESH_ID,
        )

    edges = [
        remote(edge_ref, before_ref, edge_send.at[0], edge_recv.at[0], beside[0]),
        remote(first_ref, after_ref, edge_send.at[1], edge_recv.at[1], beside[1]),
    ]
    for edge in edges:
        edge.start()

    def block(g, k, j):
        return full[g].at[k, j]

    def along_line(g, k, mine, step):
        return remote(
            own[g] if mine else block(g, k, i),
            block(g, k, i),
            line_send.at[g, k, step],
            line_recv.at[g, k],
            (o + 2 * step - 1, i, core),
        )

    def to_side(g, k, mine, side):
        return remote(
            own[g] if mine else block(g, k, i),
            block(g, k, i),
            side_send.at[g, k, side],
            side_recv.at[g, k, side],
            (o, sides[side], core),
        )

    def from_side(g, k, side):
        return remote(
            block(g, k, sides[side]),
            block(g, k, sides[side]),
            side_send.at[g, k, side],
            side_recv.at[g, k, side],
            (o, sides[side], core),
        )

    def half(g, k, side, to):
        part = full[g].at[k, side, :, pl.ds(lanes * to, lanes)]
        return remote(
            part, part, half_send.at[g, k, to], half_recv.at[g, k, to], (o, sides[to], core)
        )

    def visit(first, then):
        first(o)
        for d in range(1, outer):
            pl.when(o - d >= 0)(functools.partial(then, o - d, True))
            pl.when(o + d < outer)(functools.partial(then, o + d, False))

    for g in range(groups):
        pltpu.make_async_copy(own[g], block(g, o, i), local.at[g]).start()
        pl.when(o + 1 < outer)(lambda g=g: along_line(g, o, True, 1).start())
        pl.when(o > 0)(lambda g=g: along_line(g, o, True, 0).start())
        for side in range(2):
            to_side(g, o, True, side).start()

    hidden = in_ref.shape[2] // outer
    for p, (start, size) in enumerate(cuts):
        for k in range(outer):
            at = slice(k * hidden + start, k * hidden + start + size)
            send[p][k, :, :size] = in_ref[0, :, at]
            send[p][k, :, size : 2 * size] = in_ref[1, :, at]
            send[p][k, :, 2 * size :] = out_ref[:, at]
    tokens, width = source_ref.shape

    def normed(values):
        inverse = lax.rsqrt(jnp.mean(values * values, axis=-1, keepdims=True) + EPS)
        return (values * inverse * scale_ref[...]).astype(BF16)

    def norm_rows(k, _):
        at = pl.multiple_of(k * HALO, HALO)
        rows = source_ref[pl.ds(at, HALO), :].astype(F32)
        normed_ref[pl.ds(at + HALO, HALO), :] = normed(rows)
        return _

    lax.fori_loop(0, tokens // HALO, norm_rows, 0)
    for edge in edges:
        edge.wait()
    normed_ref[:HALO, :] = normed(before_ref[:, :width])

    def pass_on(k, from_left):
        for g in range(groups):
            along_line(g, k, False, 0).wait_recv()
            if from_left:
                pl.when(o + 1 < outer)(lambda g=g: along_line(g, k, False, 1).start())
            else:
                pl.when(o > 0)(lambda g=g: along_line(g, k, False, 0).start())
            for side in range(2):
                to_side(g, k, False, side).start()

    visit(lambda k: None, pass_on)

    def part(p, k, mine):
        peer = lax.rem(o + k, outer)
        return remote(
            send[p].at[peer],
            got[p].at[o if mine else peer],
            part_send.at[p, k],
            part_recv.at[p, o if mine else peer],
            (peer, i, core),
        )

    for p in range(parts):
        pltpu.make_async_copy(send[p].at[o], got[p].at[o], local.at[groups + p]).start()
        for k in range(1, outer):
            part(p, k, True).start()

    def turn(k, _=None):
        for g in range(groups):
            for side in range(2):
                from_side(g, k, side).wait_recv()
                half(g, k, sides[side], 1 - side).start()

    visit(turn, turn)

    def finish(k, _=None):
        for g in range(groups):
            for side in range(2):
                half(g, k, far, side).wait_recv()

    visit(finish, finish)
    for p in range(parts):
        for k in range(1, outer):
            part(p, k, False).wait_recv()

    def sent(k, from_left):
        for g in range(groups):
            if from_left is None or from_left:
                pl.when(o + 1 < outer)(lambda g=g: along_line(g, k, False, 1).wait_send())
            if not from_left:
                pl.when(o > 0)(lambda g=g: along_line(g, k, False, 0).wait_send())
            for side in range(2):
                to_side(g, k, False, side).wait_send()
                half(g, k, sides[side], 1 - side).wait_send()

    visit(functools.partial(sent, from_left=None), sent)
    for p in range(parts):
        for k in range(1, outer):
            part(p, k, True).wait_send()
    for g in range(groups):
        pltpu.make_async_copy(own[g], block(g, o, i), local.at[g]).wait()
    for p in range(parts):
        pltpu.make_async_copy(send[p].at[o], got[p].at[o], local.at[groups + p]).wait()


def gather_weights(own, ffw_in, ffw_out_t, source, scale, edge, first, cuts):
    outer, inner = lax.axis_size("o"), lax.axis_size("i")
    groups, parts = len(own), len(cuts)
    dma = pltpu.SemaphoreType.DMA
    blocks = [(outer, own[0].shape[0], 3 * size) for _, size in cuts]
    shape = jax.ShapeDtypeStruct
    out_shape = [shape((outer, inner, *w.shape), BF16) for w in own]
    out_shape += [shape(block, BF16) for block in blocks]
    out_shape += [
        shape((HALO + source.shape[0], source.shape[1]), BF16),
        shape(edge.shape, F32),
        shape(first.shape, F32),
    ]
    result = pl.pallas_call(
        functools.partial(gather_kernel, outer, inner, groups, cuts),
        in_specs=[VMEM] * (groups + 6),
        out_specs=[ANY] * (groups + parts) + [VMEM] * 3,
        out_shape=out_shape,
        scratch_shapes=[pltpu.VMEM(block, BF16) for block in blocks]
        + [
            dma((groups, outer, 2)),
            dma((groups, outer)),
            dma((groups, outer, 2)),
            dma((groups, outer, 2)),
            dma((groups, outer, 2)),
            dma((groups, outer, 2)),
            dma((parts, outer)),
            dma((parts, outer)),
            dma((2,)),
            dma((2,)),
            dma((groups + parts,)),
        ],
        compiler_params=pltpu.CompilerParams(collective_id=0, has_side_effects=True),
    )(*own, ffw_in, ffw_out_t, source, scale, edge, first)
    full = [w.reshape(-1, w.shape[-1]) for w in result[:groups]]
    return full, result[groups : groups + parts], result[groups + parts :]


def grads_kernel(plan, added, *refs):
    out_ref = refs[-1]
    inner, _, rows, _ = out_ref.shape
    take = rows - added
    if added:
        out_ref[:, 0, take:, :] = refs[-2][0]
    refs = iter(refs)
    at = 0
    for terms in plan:
        total = None
        for pieces in terms:
            a = [next(refs)[...] for _ in range(pieces)]
            term = mm_tn(jnp.concatenate(a) if pieces > 1 else a[0], next(refs)[...])
            total = term if total is None else total + term
        size = total.shape[1]
        out_ref[:, 0, :take, at : at + size] = total.astype(BF16).reshape(inner, take, size)
        at += size


def grads_rows(columns, extra=None):
    outer, inner = lax.axis_size("o"), lax.axis_size("i")
    width = columns[0][0][0][0].shape[1]
    block = width // outer
    rows = block // inner
    size = sum(terms[0][1].shape[1] for terms in columns)
    tokens = sum(b.shape[0] for _, b in columns[0])
    added = 0 if extra is None else extra.shape[2]
    if block % 128:
        whole = [
            sum(mm_tn(jnp.concatenate(a), b) for a, b in terms).astype(BF16) for terms in columns
        ]
        whole = jnp.concatenate(whole, axis=1).reshape(outer, inner, rows, size)
        if added:
            whole = jnp.concatenate([whole, extra], axis=2)
        return whole.transpose(1, 0, 2, 3).reshape(inner, -1, size)
    specs, given = [], []
    for terms in columns:
        for a, b in terms:
            for piece in a:
                specs.append(pl.BlockSpec((piece.shape[0], block), lambda k: (0, k)))
                given.append(piece)
            specs.append(pl.BlockSpec(b.shape, lambda k: (0, 0)))
            given.append(b)
    if added:
        specs.append(pl.BlockSpec((1, inner, added, size), lambda k: (k, 0, 0, 0)))
        given.append(extra)
    plan = tuple(tuple(len(a) for a, _ in terms) for terms in columns)
    result = pl.pallas_call(
        functools.partial(grads_kernel, plan, added),
        grid=(outer,),
        in_specs=specs,
        out_specs=pl.BlockSpec((inner, 1, rows + added, size), lambda k: (0, k, 0, 0)),
        out_shape=jax.ShapeDtypeStruct((inner, outer, rows + added, size), BF16),
        cost_estimate=pl.CostEstimate(
            flops=2 * tokens * width * size,
            bytes_accessed=2 * (tokens * (width + size) + width * size),
            transcendentals=0,
        ),
    )(*given)
    return result.reshape(inner, -1, size)


def unpack_kernel(cuts, *refs):
    parts, in_ref, out_ref = refs[:-2], refs[-2], refs[-1]
    outer = parts[0].shape[0]
    hidden = out_ref.shape[1] // outer
    for part, (start, size) in zip(parts, cuts):
        for k in range(outer):
            at = slice(k * hidden + start, k * hidden + start + size)
            in_ref[0, :, at] = part[k, :, :size].astype(F32)
            in_ref[1, :, at] = part[k, :, size : 2 * size].astype(F32)
            out_ref[:, at] = part[k, :, 2 * size :].astype(F32)


def unpack(parts, cuts, hidden):
    rows = parts[0].shape[1]
    return pl.pallas_call(
        functools.partial(unpack_kernel, cuts),
        in_specs=[VMEM] * len(parts),
        out_specs=[VMEM] * 2,
        out_shape=[
            jax.ShapeDtypeStruct((2, rows, hidden), F32),
            jax.ShapeDtypeStruct((rows, hidden), F32),
        ],
        cost_estimate=pl.CostEstimate(
            flops=0, bytes_accessed=18 * rows * hidden, transcendentals=0
        ),
    )(*parts)


def gelu_tanh(values):
    return jax.nn.gelu(values, approximate=True)


def geglu(gate_vals, up_vals):
    return gelu_tanh(gate_vals) * up_vals


def norm_back(values, scaling, delta):
    inverse = lax.rsqrt(jnp.mean(values * values, axis=-1, keepdims=True) + EPS)
    unit = values * inverse
    scaled = delta * (1.0 + scaling)
    moved = inverse * (scaled - unit * jnp.mean(scaled * unit, axis=-1, keepdims=True))
    return moved, jnp.sum(delta * unit, axis=0)


def rms_norm(values, scaling):
    inverse = lax.rsqrt(jnp.mean(values * values, axis=-1, keepdims=True) + EPS)
    return values * inverse * (1.0 + scaling)


def dot(a, b, contract):
    return lax.dot_general(a, b, ((contract[0], contract[1]), ((), ())), preferred_element_type=F32)


def mm(a, b):
    return dot(a, b, ((1,), (0,)))


def mm_nt(a, b):
    return dot(a, b, ((1,), (1,)))


def mm_tn(a, b):
    return dot(a, b, ((0,), (0,)))


def gather_slots(half):
    slots = []
    for k in range(lax.axis_size("o")):
        if k:
            half = ring(half)
        slots.append([half, swap(half)])
    return slots


def both_cores(part):
    rows = part.shape[0] // 2
    return part[:rows] + swap(part[rows:].astype(BF16)).astype(F32)


def ring_sum(parts):
    total = parts[0].astype(F32)
    for part in parts[1:]:
        low = total.astype(BF16)
        moved = ring(low)
        total = part.astype(F32) + moved.astype(F32)
    return total


def direct_sum(parts, axis, peer):
    count, at = lax.axis_size(axis), lax.axis_index(axis)
    total = lax.dynamic_index_in_dim(parts, at, 0, False).astype(F32)
    for k in range(1, count):
        part = lax.dynamic_index_in_dim(parts, peer(at, k), 0, False)
        moved = lax.ppermute(part, axis, [(j, peer(j, k)) for j in range(count)])
        total = total + moved.astype(F32)
    return total


def ring_order(parts):
    count, at = lax.axis_size("o"), lax.axis_index("o")
    return [
        lax.dynamic_index_in_dim(parts, lax.rem(at - k + count, count), 0, False)
        for k in [*range(1, count), 0]
    ]


def spread(value):
    return lax.all_to_all(value, "o", 0, 0, tiled=True)


def gather_inner(whole):
    return lax.all_gather(whole, "i", axis=1, tiled=True).reshape(-1, whole.shape[-1])


def sum_inner(rows):
    own = lax.psum_scatter(
        rows.reshape(-1, rows.shape[-1]), "i", scatter_dimension=0, tiled=True
    )
    return own.reshape(lax.axis_size("o"), -1, rows.shape[-1])


def cuts_of(size):
    first = size // 2 // 128 * 128 + 128 if size > 512 else size
    return ((0, first), (first, size - first)) if size > first else ((0, size),)


def per_device(
    inputs,
    segment_ids,
    cotangent,
    branch_weight,
    out_weight,
    ffw_in,
    ffw_out,
    norm_scales,
    branch_bias,
    conv_weight,
    conv_bias,
    gate_weights,
    gate_bias,
    decay_param,
    out_bias,
    ffw_bias,
):
    outer, inner = lax.axis_size("o"), lax.axis_size("i")
    count = outer * inner
    core, along = lax.axis_index("tensor"), lax.axis_index("o")
    tok_rows, width = inputs.shape
    hidden_half = ffw_out.shape[0]
    hidden_part = hidden_half // outer
    taps_count = conv_weight.shape[0]
    rim_rows = taps_count - 1
    heads_half, block_size = gate_weights.shape[1], gate_weights.shape[2]
    width_half = heads_half * block_size

    cuts = cuts_of(hidden_part)
    seg_marks = (segment_ids + 1).astype(F32)
    lanes = jnp.broadcast_to(seg_marks[:, None], (tok_rows, 128))
    (branch_x_full, branch_y_full, out_full_t), parts, (normed_ext, before, after) = (
        gather_weights(
            [branch_weight[0], branch_weight[1], out_weight.T],
            ffw_in,
            ffw_out.T,
            inputs,
            1.0 + norm_scales[:1],
            jnp.concatenate([inputs[tok_rows - HALO :].astype(F32), lanes[-HALO:]], axis=1),
            lanes[:HALO],
            cuts,
        )
    )
    ffw_parts = []
    for k, (_, size) in enumerate(cuts):
        whole = gather_inner(parts[k])
        ffw_parts.append((whole[:, : 2 * size], whole[:, 2 * size :]))
    cot_own, branch_x_full = lax.optimization_barrier((half_of(cotangent, core), branch_x_full))
    cot_halves = [cot_own, ring(cot_own)]

    source_half = half_of(inputs, core).astype(F32)
    place = lax.axis_index(DP)
    marks_before = jnp.where(place == 0, 0.0, before[:, width])
    marks_after = jnp.where(place == count - 1, 0.0, after[:rim_rows, 0])
    normed_low = normed_ext[HALO:]
    marks_ext = jnp.concatenate([marks_before, seg_marks])
    same = [
        (marks_ext[HALO - k : HALO - k + tok_rows] == seg_marks).astype(F32)
        for k in range(taps_count)
    ]
    masks = jnp.stack([1.0 - same[1], *same[1:], *[same[0]] * (8 - taps_count)], axis=1)
    branch_ext = mm(normed_ext, branch_x_full) + branch_bias[0]
    branch_y = mm(normed_low, branch_y_full) + branch_bias[1]
    rate = jax.nn.softplus(decay_param)
    row_params = jnp.stack([conv_bias, gate_bias[0], gate_bias[1], rate] + [rate] * 4)
    conv_low, decay_gate, input_gate, cumulative, local_state, ends = mix(
        branch_ext, masks, conv_weight, row_params, gate_weights
    )
    conv_blocks = conv_low.reshape(tok_rows, heads_half, block_size)
    for k in range(2, min(3, outer)):
        cot_halves.append(ring(cot_halves[-1]))
    carry_in = entering(ends, False)
    carry_in, cot_halves[-1] = lax.optimization_barrier((carry_in, cot_halves[-1]))
    for k in range(3, outer):
        cot_halves.append(ring(cot_halves[-1]))
    states = local_state + cumulative * carry_in
    branch_act, gelu_back = jax.vjp(gelu_tanh, branch_y)
    mixed_in = (states * branch_act).astype(BF16)
    mixed_part = mm_nt(mixed_in, out_full_t)
    residual = (
        source_half
        + half_of(mixed_part, core)
        + swap(half_of(mixed_part, 1 - core))
        + out_bias[0]
    )

    normed_slots = gather_slots(rms_norm(residual, norm_scales[1]).astype(BF16))
    cot_slots = [[half, swap(half)] for half in cot_halves[:outer]]
    normed_joined = [jnp.concatenate(slot) for slot in normed_slots]
    cot_joined = [jnp.concatenate(slot) for slot in cot_slots]
    bias_part = lax.dynamic_slice_in_dim(ffw_bias, along * hidden_part, hidden_part, 1)
    slots = range(outer)
    hidden_of, delta_of, inner_sums, bias_sums, rows = [], [], [], [], None
    for p, (start, size) in enumerate(cuts):
        if rows is not None:
            rows, normed_joined, cot_joined = lax.optimization_barrier(
                (rows, normed_joined, cot_joined)
            )
            inner_sums.append(sum_inner(rows))
        in_full, out_full = ffw_parts[p]
        bias_row = bias_part[:, start : start + size].reshape(2 * size)
        hiddens, deltas = [], []
        for k in slots:
            gate_up = mm(normed_joined[k], in_full) + bias_row
            hidden, hidden_back = jax.vjp(geglu, gate_up[:, :size], gate_up[:, size:])
            hiddens.append(hidden.astype(BF16))
            deltas.append(
                jnp.concatenate(hidden_back(mm(cot_joined[k], out_full)), axis=1).astype(BF16)
            )
        if p == len(cuts) - 1:
            delta_parts = [
                sum(mm_nt(d[k], w[0]) for d, w in zip(delta_of + [deltas], ffw_parts))
                for k in slots
            ]
            sums = [both_cores(part) for part in delta_parts[1:] + delta_parts[:1]]
            _, hiddens, deltas = lax.optimization_barrier((sums[0], hiddens, deltas))
        hidden_of.append(hiddens)
        delta_of.append(deltas)
        bias_sums.append(
            sum(jnp.sum(d, axis=0, dtype=F32) for d in deltas).reshape(2, size)
        )
        rows = grads_rows([list(zip(normed_slots, deltas)), list(zip(cot_slots, hiddens))])
    inner_sums.append(sum_inner(rows))
    delta_normed_two = ring_sum(sums)
    result_parts = [
        sum(mm_nt(hidden_of[p][k], ffw_parts[p][1]) for p in range(len(cuts))) for k in slots
    ]
    result_parts = [both_cores(part) for part in result_parts]
    result_parts = result_parts[1:] + result_parts[:1]
    delta_normed_two, result_parts, inner_sums[0] = lax.optimization_barrier(
        (delta_normed_two, result_parts, inner_sums[0])
    )
    grads = [spread(inner_sums[0])]
    grad_ffw_bias = lax.dynamic_update_slice_in_dim(
        jnp.zeros((2, hidden_half), F32),
        jnp.concatenate(bias_sums, axis=1),
        along * hidden_part,
        1,
    )

    cot_half = half_of(cotangent, core).astype(F32)
    delta_res_norm, grad_scale_two = norm_back(residual, norm_scales[1], delta_normed_two)
    delta_residual = cot_half + delta_res_norm
    delta_half = delta_residual.astype(BF16)
    delta_mixed = join_halves(delta_half, swap(delta_half), core)
    delta_mixed_in = mm(delta_mixed, out_full_t)
    delta_states = delta_mixed_in * branch_act
    (delta_branch_y,) = gelu_back(delta_mixed_in * states)
    delta_y_low = delta_branch_y.astype(BF16)
    oy_rows = grads_rows([[([delta_mixed], mixed_in)], [([normed_low], delta_y_low)]])
    grad_oy_inner = sum_inner(oy_rows)
    reset = masks[:, :1]
    log_decay = -8.0 * decay_gate * rate
    decay = jnp.exp(log_decay)
    keep_rate = decay * (1.0 - reset)
    alpha_next = jnp.concatenate([keep_rate[1:], jnp.ones((1, width_half), F32)], axis=0)
    suffix, local_adjoint = local_scan(alpha_next, delta_states, True)
    leaving = entering(
        jnp.stack([keep_rate[0] * suffix[0], keep_rate[0] * local_adjoint[0]]), True
    )
    leaving, inner_sums[1:] = lax.optimization_barrier((leaving, inner_sums[1:]))
    for k in range(1, len(cuts)):
        grads.append(spread(inner_sums[k]))
    adjoint = local_adjoint + suffix * leaving
    states_before = jnp.concatenate([carry_in[None, :], states[: tok_rows - 1]], axis=0)
    conv_float = conv_low.astype(F32)
    room = -jnp.expm1(2.0 * log_decay)
    multiplier = jnp.sqrt(jnp.maximum(room, 0.001)) * (1.0 - reset) + reset
    drawn = adjoint * input_gate
    delta_log = keep_rate * (
        adjoint * states_before
        - jnp.where(room > 0.001, drawn * conv_float * decay / multiplier, 0.0)
    )
    decay_sum = jnp.sum(delta_log * decay_gate, axis=0)
    delta_conv_direct = drawn * multiplier
    delta_gates = jnp.stack(
        [
            delta_log * (-8.0 * rate) * decay_gate * (1.0 - decay_gate),
            delta_conv_direct * conv_float * (1.0 - input_gate),
        ]
    ).astype(BF16)
    grad_decay = -8.0 * decay_sum * jax.nn.sigmoid(decay_param)
    delta_blocks = delta_gates.reshape(2, tok_rows, heads_half, block_size)
    grad_gate_weights = jnp.einsum(
        "thb,gthc->ghbc", conv_blocks, delta_blocks, preferred_element_type=F32
    )
    gate_rows = (
        grad_gate_weights.reshape(2, heads_half, count, block_size // count, block_size)
        .transpose(2, 0, 1, 3, 4)
        .astype(BF16)
    )
    gate_rows = gate_rows.reshape(outer, inner, -1, block_size).transpose(1, 0, 2, 3)
    gate_part = direct_sum(gate_rows, "i", lambda j, k: j ^ k).astype(BF16)
    gate_grad = direct_sum(gate_part, "o", lambda j, k: (j + k) % outer)
    gate_grad = gate_grad.reshape(2, heads_half, block_size // count, block_size)
    grad_gate_bias = jnp.sum(delta_gates, axis=1, dtype=F32)
    delta_conv = delta_conv_direct + jnp.einsum(
        "gthc,ghbc->thb", delta_blocks, gate_weights, preferred_element_type=F32
    ).reshape(tok_rows, width_half)
    rim_delta = from_behind(delta_conv[:rim_rows], -1)
    rim_delta, result_parts = lax.optimization_barrier((rim_delta, result_parts))
    result_sum = ring_sum(result_parts)
    ffw_in_grad, ffw_out_grad = unpack(grads, cuts, hidden_half)
    padded_delta = jnp.concatenate([delta_conv, rim_delta], axis=0)
    next_marks = jnp.concatenate([seg_marks, marks_after], axis=0)
    delta_branch_x = jnp.zeros_like(delta_conv)
    conv_weight_rows = []
    for offset in range(taps_count):
        matches = (next_marks[offset : offset + tok_rows] == seg_marks).astype(F32)[:, None]
        delta_branch_x = (
            delta_branch_x
            + conv_weight[offset] * padded_delta[offset : offset + tok_rows] * matches
        )
        shifted = branch_ext[HALO - offset : HALO - offset + tok_rows] * same[offset][:, None]
        conv_weight_rows.append(jnp.sum(delta_conv * shifted, axis=0))
    grad_conv_bias = jnp.sum(delta_conv, axis=0)
    delta_x_low = delta_branch_x.astype(BF16)
    x_rows = grads_rows([[([normed_low], delta_x_low)]])
    grad_x_inner = sum_inner(x_rows)
    delta_part = mm_nt(delta_x_low, branch_x_full) + mm_nt(delta_y_low, branch_y_full)
    delta_normed = half_of(delta_part, core) + swap(
        half_of(delta_part, 1 - core).astype(BF16)
    ).astype(F32)
    delta_source_norm, grad_scale_one = norm_back(source_half, norm_scales[0], delta_normed)
    grad_half = delta_residual + delta_source_norm
    input_grad = join_halves(grad_half, swap(grad_half), core)

    halves = jnp.stack(
        [
            grad_scale_one,
            grad_scale_two,
            jnp.sum(delta_half, axis=0, dtype=F32),
            jnp.sum(cot_half, axis=0),
        ]
    )
    halves = halves + swap(halves)
    flat = [
        halves.reshape(-1),
        jnp.sum(delta_x_low, axis=0, dtype=F32),
        jnp.sum(delta_y_low, axis=0, dtype=F32),
        *conv_weight_rows,
        grad_conv_bias,
        grad_gate_bias.reshape(-1),
        grad_decay,
        grad_ffw_bias.reshape(-1),
    ]
    grad_oy = ring_sum(ring_order(grad_oy_inner))
    small = sum_over_all(jnp.concatenate(flat).reshape(-1, 128))
    result_half = residual + result_sum + out_bias[1]
    result = join_halves(result_half, swap(result_half), core)
    grad_branch_x = ring_sum(ring_order(grad_x_inner))
    small = small.reshape(-1)
    at = 0
    taken = []
    for shape in (
        (2, width),
        (2, width),
        (2, width_half),
        (taps_count, width_half),
        (width_half,),
        (2, width_half),
        (width_half,),
        (2, hidden_half),
    ):
        size = 1
        for n in shape:
            size *= n
        taken.append(small[at : at + size].reshape(shape))
        at += size
    scales, out_bias_grad, branch_bias_grad, taps_grad, conv_bias_grad, gate_bias_grad, decay_grad, ffw_bias_grad = taken
    return (
        result,
        input_grad,
        jnp.stack([grad_branch_x, grad_oy[:, width_half:]]),
        grad_oy[:, :width_half].T,
        ffw_in_grad,
        ffw_out_grad.T,
        scales,
        branch_bias_grad,
        taps_grad,
        conv_bias_grad,
        gate_grad,
        gate_bias_grad,
        decay_grad,
        out_bias_grad,
        ffw_bias_grad,
    )


def solution(mesh):
    count = mesh.shape["dp"]
    grid = Mesh(
        mesh.devices.reshape(count // INNER, INNER, mesh.shape["tensor"]), ("o", "i", "tensor")
    )
    in_specs = (
        P(DP, None),
        P(DP),
        P(DP, None),
        P(None, DP, "tensor"),
        P("tensor", DP),
        P(None, DP, "tensor"),
        P("tensor", DP),
        P(),
        P(None, "tensor"),
        P(None, "tensor"),
        P("tensor"),
        P(None, "tensor", None, None),
        P(None, "tensor"),
        P("tensor"),
        P(),
        P(None, "tensor"),
    )
    out_specs = (
        P(DP, None),
        P(DP, None),
        P(None, DP, "tensor"),
        P("tensor", DP),
        P(None, DP, "tensor"),
        P("tensor", DP),
        P(),
        P(None, "tensor"),
        P(None, "tensor"),
        P("tensor"),
        P(None, "tensor", DP, None),
        P(None, "tensor"),
        P("tensor"),
        P(),
        P(None, "tensor"),
    )

    return jax.shard_map(
        per_device, mesh=grid, in_specs=in_specs, out_specs=out_specs, check_vma=False
    )
```

```python
import functools

import jax
import jax.numpy as jnp
from jax import lax
from jax.experimental import pallas as pl
from jax.experimental.pallas import tpu as pltpu
from jax.sharding import Mesh
from jax.sharding import PartitionSpec as P


INNER = 4
DP = ("o", "i")
EPS = 1e-06
F32 = jnp.float32
BF16 = jnp.bfloat16


def swap(value):
    return lax.ppermute(value, "tensor", [(0, 1), (1, 0)])


def ring(value):
    count = lax.axis_size("o")
    return lax.ppermute(value, "o", [(k, (k + 1) % count) for k in range(count)])


def from_behind(value, steps):
    count = lax.axis_size(DP)
    first, last = max(0, -steps), min(count, count - steps)
    return lax.ppermute(value, DP, [(k, k + steps) for k in range(first, last)])


def sum_over_all(value):
    count, bit = lax.axis_size(DP), 1
    while bit < count:
        value = value + lax.ppermute(value, DP, [(k, k ^ bit) for k in range(count)])
        bit *= 2
    return value


def half_of(value, which):
    rows = value.shape[0] // 2
    return lax.dynamic_slice_in_dim(value, which * rows, rows, 0)


def join_halves(own, other, core):
    first = jnp.where(core == 0, own, other)
    second = jnp.where(core == 0, other, own)
    return jnp.concatenate([first, second], axis=0)


def run_scan(reverse, keep_ref, drive_ref, cum_ref, state_ref):
    rows, width = keep_ref.shape
    groups = rows // 8
    place = lax.broadcasted_iota(jnp.int32, (8, width), 0)

    def step(k, carried):
        before_a, before_b = carried
        group = groups - 1 - k if reverse else k
        at = pl.ds(pl.multiple_of(group * 8, 8), 8)
        a, b = keep_ref[at, :], drive_ref[at, :]
        for d in (1, 2, 4):
            far_a = pltpu.roll(a, 8 - d if reverse else d, 0)
            far_b = pltpu.roll(b, 8 - d if reverse else d, 0)
            inside = place < 8 - d if reverse else place >= d
            b = jnp.where(inside, a * far_b + b, b)
            a = jnp.where(inside, a * far_a, a)
        b = a * before_b + b
        a = a * before_a
        cum_ref[at, :] = a
        state_ref[at, :] = b
        edge = slice(0, 1) if reverse else slice(7, 8)
        return (a[edge], b[edge])

    return lax.fori_loop(
        0, groups, step, (jnp.ones((1, width), F32), jnp.zeros((1, width), F32))
    )


def scan_kernel(reverse, keep_ref, drive_ref, cum_ref, state_ref):
    run_scan(reverse, keep_ref, drive_ref, cum_ref, state_ref)


def local_scan(keep, drive, reverse):
    rows, width = keep.shape
    block = 256
    spec = pl.BlockSpec((rows, block), lambda j: (0, j))
    shape = jax.ShapeDtypeStruct((rows, width), F32)
    return pl.pallas_call(
        functools.partial(scan_kernel, reverse),
        grid=(width // block,),
        in_specs=[spec, spec],
        out_specs=[spec, spec],
        out_shape=[shape, shape],
        cost_estimate=pl.CostEstimate(
            flops=20 * rows * width, bytes_accessed=16 * rows * width, transcendentals=0
        ),
    )(keep, drive)


HALO = 16


def mix_kernel(branch_ref, mask_ref, taps_ref, rows_ref, gate_ref, *refs):
    conv_ref, decay_gate_ref, input_gate_ref, cum_ref, state_ref, ends_ref, keep, drive = refs
    rows = conv_ref.shape[0]
    conv = rows_ref[0:1, :] + taps_ref[0:1, :] * branch_ref[HALO : HALO + rows, :]
    for k in range(1, taps_ref.shape[0]):
        shifted = branch_ref[HALO - k : HALO - k + rows, :] * mask_ref[:, k : k + 1]
        conv = conv + taps_ref[k : k + 1, :] * shifted
    low = conv.astype(BF16)
    conv_ref[...] = low
    decay_gate = jax.nn.sigmoid(mm(low, gate_ref[0, 0]) + rows_ref[1:2, :])
    input_gate = jax.nn.sigmoid(mm(low, gate_ref[1, 0]) + rows_ref[2:3, :])
    decay_gate_ref[...] = decay_gate
    input_gate_ref[...] = input_gate
    reset = mask_ref[:, 0:1]
    log_decay = -8.0 * decay_gate * rows_ref[3:4, :]
    multiplier = jnp.sqrt(jnp.maximum(1.0 - jnp.exp(2.0 * log_decay), 0.001))
    keep[...] = jnp.exp(log_decay) * (1.0 - reset)
    drive[...] = low.astype(F32) * input_gate * (multiplier * (1.0 - reset) + reset)
    ends_ref[0:1, :], ends_ref[1:2, :] = run_scan(False, keep, drive, cum_ref, state_ref)


def mix(branch, masks, taps, row_params, gate_weights):
    rows, width = branch.shape[0] - HALO, branch.shape[1]
    block = gate_weights.shape[2]
    over = lambda n: pl.BlockSpec((n, block), lambda h: (0, h))
    full = jax.ShapeDtypeStruct((rows, width), F32)
    return pl.pallas_call(
        mix_kernel,
        grid=(width // block,),
        in_specs=[
            over(rows + HALO),
            pl.BlockSpec(masks.shape, lambda h: (0, 0)),
            over(taps.shape[0]),
            over(row_params.shape[0]),
            pl.BlockSpec((2, 1, block, block), lambda h: (0, h, 0, 0)),
        ],
        out_specs=[over(rows)] * 5 + [over(2)],
        out_shape=[
            jax.ShapeDtypeStruct((rows, width), BF16),
            full,
            full,
            full,
            full,
            jax.ShapeDtypeStruct((2, width), F32),
        ],
        scratch_shapes=[pltpu.VMEM((rows, block), F32)] * 2,
        cost_estimate=pl.CostEstimate(
            flops=4 * rows * width * block,
            bytes_accessed=22 * rows * width,
            transcendentals=8 * rows * width,
        ),
    )(branch, masks, taps, row_params, gate_weights)


MESH_ID = pl.DeviceIdType.MESH
VMEM = pl.BlockSpec(memory_space=pltpu.VMEM)
ANY = pl.BlockSpec(memory_space=pl.ANY)


def enter_kernel(outer, inner, reverse, ends_ref, carry_ref, every, send_sem, recv_sem):
    count = outer * inner
    core = lax.axis_index("tensor")
    me = lax.axis_index("o") * inner + lax.axis_index("i")
    barrier = pltpu.get_barrier_semaphore()
    for k in range(1, count):
        peer = lax.rem(me + k, count)
        to = (peer // inner, lax.rem(peer, inner), core)
        pl.semaphore_signal(barrier, inc=1, device_id=to, device_id_type=MESH_ID)
    pl.semaphore_wait(barrier, count - 1)

    def copy(k, mine):
        peer = lax.rem(me + k, count)
        return pltpu.make_async_remote_copy(
            src_ref=ends_ref,
            dst_ref=every.at[me if mine else peer],
            send_sem=send_sem.at[k],
            recv_sem=recv_sem.at[me if mine else peer],
            device_id=(peer // inner, lax.rem(peer, inner), core),
            device_id_type=MESH_ID,
        )

    for k in range(1, count):
        copy(k, True).start()
    for k in range(1, count):
        copy(k, False).wait_recv()
    carried = jnp.zeros((1, ends_ref.shape[1]), F32)
    for k in range(count):
        at = count - 1 - k if reverse else k
        reached = at > me if reverse else at < me
        block = every[at]
        carried = jnp.where(reached, block[0:1] * carried + block[1:2], carried)
    carry_ref[...] = carried
    for k in range(1, count):
        copy(k, True).wait_send()


def entering(ends, reverse):
    outer, inner = lax.axis_size("o"), lax.axis_size("i")
    count, width = outer * inner, ends.shape[1]
    carried = pl.pallas_call(
        functools.partial(enter_kernel, outer, inner, reverse),
        in_specs=[VMEM],
        out_specs=VMEM,
        out_shape=jax.ShapeDtypeStruct((1, width), F32),
        scratch_shapes=[
            pltpu.VMEM((count, 2, width), F32),
            pltpu.SemaphoreType.DMA((count,)),
            pltpu.SemaphoreType.DMA((count,)),
        ],
        compiler_params=pltpu.CompilerParams(
            collective_id=2 if reverse else 1, has_side_effects=True
        ),
    )(ends)
    return carried[0]


def gather_kernel(outer, inner, groups, cuts, *refs):
    parts = len(cuts)
    own, refs = refs[:groups], refs[groups:]
    in_ref, out_ref, source_ref, scale_ref, edge_ref, first_ref = refs[:6]
    refs = refs[6:]
    full, got, refs = refs[:groups], refs[groups : groups + parts], refs[groups + parts :]
    normed_ref, before_ref, after_ref = refs[:3]
    send, refs = refs[3 : 3 + parts], refs[3 + parts :]
    line_send, line_recv, side_send, side_recv, half_send, half_recv, part_send, part_recv = refs[:8]
    edge_send, edge_recv, local = refs[8:]
    o, i, core = lax.axis_index("o"), lax.axis_index("i"), lax.axis_index("tensor")
    sides = (i + 1 - 2 * lax.rem(i, 2), lax.rem(i + 2, 4))
    far = lax.rem(sides[0] + 2, 4)
    lanes = own[0].shape[1] // 2

    barrier = pltpu.get_barrier_semaphore()
    for k in range(1, outer):
        pl.semaphore_signal(
            barrier, inc=1, device_id=(lax.rem(o + k, outer), i, core), device_id_type=MESH_ID
        )
    for side in sides:
        pl.semaphore_signal(barrier, inc=1, device_id=(o, side, core), device_id_type=MESH_ID)
    count = outer * inner
    me = o * inner + i
    beside = []
    for step in (1, count - 1):
        at = lax.rem(me + step, count)
        beside.append((at // inner, lax.rem(at, inner), core))
        pl.semaphore_signal(barrier, inc=1, device_id=beside[-1], device_id_type=MESH_ID)
    pl.semaphore_wait(barrier, outer + 3)

    def remote(src, dst, send_sem, recv_sem, to):
        return pltpu.make_async_remote_copy(
            src_ref=src,
            dst_ref=dst,
            send_sem=send_sem,
            recv_sem=recv_sem,
            device_id=to,
            device_id_type=MESH_ID,
        )

    edges = [
        remote(edge_ref, before_ref, edge_send.at[0], edge_recv.at[0], beside[0]),
        remote(first_ref, after_ref, edge_send.at[1], edge_recv.at[1], beside[1]),
    ]
    for edge in edges:
        edge.start()

    def block(g, k, j):
        return full[g].at[k, j]

    def along_line(g, k, mine, step):
        return remote(
            own[g] if mine else block(g, k, i),
            block(g, k, i),
            line_send.at[g, k, step],
            line_recv.at[g, k],
            (o + 2 * step - 1, i, core),
        )

    def to_side(g, k, mine, side):
        return remote(
            own[g] if mine else block(g, k, i),
            block(g, k, i),
            side_send.at[g, k, side],
            side_recv.at[g, k, side],
            (o, sides[side], core),
        )

    def from_side(g, k, side):
        return remote(
            block(g, k, sides[side]),
            block(g, k, sides[side]),
            side_send.at[g, k, side],
            side_recv.at[g, k, side],
            (o, sides[side], core),
        )

    def half(g, k, side, to):
        part = full[g].at[k, side, :, pl.ds(lanes * to, lanes)]
        return remote(
            part, part, half_send.at[g, k, to], half_recv.at[g, k, to], (o, sides[to], core)
        )

    def visit(first, then):
        first(o)
        for d in range(1, outer):
            pl.when(o - d >= 0)(functools.partial(then, o - d, True))
            pl.when(o + d < outer)(functools.partial(then, o + d, False))

    for g in range(groups):
        pltpu.make_async_copy(own[g], block(g, o, i), local.at[g]).start()
        pl.when(o + 1 < outer)(lambda g=g: along_line(g, o, True, 1).start())
        pl.when(o > 0)(lambda g=g: along_line(g, o, True, 0).start())
        for side in range(2):
            to_side(g, o, True, side).start()

    hidden = in_ref.shape[2] // outer
    for p, (start, size) in enumerate(cuts):
        for k in range(outer):
            at = slice(k * hidden + start, k * hidden + start + size)
            send[p][k, :, :size] = in_ref[0, :, at]
            send[p][k, :, size : 2 * size] = in_ref[1, :, at]
            send[p][k, :, 2 * size :] = out_ref[:, at]
    tokens, width = source_ref.shape

    def normed(values):
        inverse = lax.rsqrt(jnp.mean(values * values, axis=-1, keepdims=True) + EPS)
        return (values * inverse * scale_ref[...]).astype(BF16)

    def norm_rows(k, _):
        at = pl.multiple_of(k * HALO, HALO)
        rows = source_ref[pl.ds(at, HALO), :].astype(F32)
        normed_ref[pl.ds(at + HALO, HALO), :] = normed(rows)
        return _

    lax.fori_loop(0, tokens // HALO, norm_rows, 0)
    for edge in edges:
        edge.wait()
    normed_ref[:HALO, :] = normed(before_ref[:, :width])

    def pass_on(k, from_left):
        for g in range(groups):
            along_line(g, k, False, 0).wait_recv()
            if from_left:
                pl.when(o + 1 < outer)(lambda g=g: along_line(g, k, False, 1).start())
            else:
                pl.when(o > 0)(lambda g=g: along_line(g, k, False, 0).start())
            for side in range(2):
                to_side(g, k, False, side).start()

    visit(lambda k: None, pass_on)

    def part(p, k, mine):
        peer = lax.rem(o + k, outer)
        return remote(
            send[p].at[peer],
            got[p].at[o if mine else peer],
            part_send.at[p, k],
            part_recv.at[p, o if mine else peer],
            (peer, i, core),
        )

    for p in range(parts):
        pltpu.make_async_copy(send[p].at[o], got[p].at[o], local.at[groups + p]).start()
        for k in range(1, outer):
            part(p, k, True).start()

    def turn(k, _=None):
        for g in range(groups):
            for side in range(2):
                from_side(g, k, side).wait_recv()
                half(g, k, sides[side], 1 - side).start()

    visit(turn, turn)

    def finish(k, _=None):
        for g in range(groups):
            for side in range(2):
                half(g, k, far, side).wait_recv()

    visit(finish, finish)
    for p in range(parts):
        for k in range(1, outer):
            part(p, k, False).wait_recv()

    def sent(k, from_left):
        for g in range(groups):
            if from_left is None or from_left:
                pl.when(o + 1 < outer)(lambda g=g: along_line(g, k, False, 1).wait_send())
            if not from_left:
                pl.when(o > 0)(lambda g=g: along_line(g, k, False, 0).wait_send())
            for side in range(2):
                to_side(g, k, False, side).wait_send()
                half(g, k, sides[side], 1 - side).wait_send()

    visit(functools.partial(sent, from_left=None), sent)
    for p in range(parts):
        for k in range(1, outer):
            part(p, k, True).wait_send()
    for g in range(groups):
        pltpu.make_async_copy(own[g], block(g, o, i), local.at[g]).wait()
    for p in range(parts):
        pltpu.make_async_copy(send[p].at[o], got[p].at[o], local.at[groups + p]).wait()


def gather_weights(own, ffw_in, ffw_out_t, source, scale, edge, first, cuts):
    outer, inner = lax.axis_size("o"), lax.axis_size("i")
    groups, parts = len(own), len(cuts)
    dma = pltpu.SemaphoreType.DMA
    blocks = [(outer, own[0].shape[0], 3 * size) for _, size in cuts]
    shape = jax.ShapeDtypeStruct
    out_shape = [shape((outer, inner, *w.shape), BF16) for w in own]
    out_shape += [shape(block, BF16) for block in blocks]
    out_shape += [
        shape((HALO + source.shape[0], source.shape[1]), BF16),
        shape(edge.shape, F32),
        shape(first.shape, F32),
    ]
    result = pl.pallas_call(
        functools.partial(gather_kernel, outer, inner, groups, cuts),
        in_specs=[VMEM] * (groups + 6),
        out_specs=[ANY] * (groups + parts) + [VMEM] * 3,
        out_shape=out_shape,
        scratch_shapes=[pltpu.VMEM(block, BF16) for block in blocks]
        + [
            dma((groups, outer, 2)),
            dma((groups, outer)),
            dma((groups, outer, 2)),
            dma((groups, outer, 2)),
            dma((groups, outer, 2)),
            dma((groups, outer, 2)),
            dma((parts, outer)),
            dma((parts, outer)),
            dma((2,)),
            dma((2,)),
            dma((groups + parts,)),
        ],
        compiler_params=pltpu.CompilerParams(collective_id=0, has_side_effects=True),
    )(*own, ffw_in, ffw_out_t, source, scale, edge, first)
    full = [w.reshape(-1, w.shape[-1]) for w in result[:groups]]
    return full, result[groups : groups + parts], result[groups + parts :]


def grads_kernel(plan, added, *refs):
    out_ref = refs[-1]
    inner, _, rows, _ = out_ref.shape
    take = rows - added
    if added:
        out_ref[:, 0, take:, :] = refs[-2][0]
    refs = iter(refs)
    at = 0
    for terms in plan:
        total = None
        for pieces in terms:
            a = [next(refs)[...] for _ in range(pieces)]
            term = mm_tn(jnp.concatenate(a) if pieces > 1 else a[0], next(refs)[...])
            total = term if total is None else total + term
        size = total.shape[1]
        out_ref[:, 0, :take, at : at + size] = total.astype(BF16).reshape(inner, take, size)
        at += size


def grads_rows(columns, extra=None):
    outer, inner = lax.axis_size("o"), lax.axis_size("i")
    width = columns[0][0][0][0].shape[1]
    block = width // outer
    rows = block // inner
    size = sum(terms[0][1].shape[1] for terms in columns)
    tokens = sum(b.shape[0] for _, b in columns[0])
    added = 0 if extra is None else extra.shape[2]
    if block % 128:
        whole = [
            sum(mm_tn(jnp.concatenate(a), b) for a, b in terms).astype(BF16) for terms in columns
        ]
        whole = jnp.concatenate(whole, axis=1).reshape(outer, inner, rows, size)
        if added:
            whole = jnp.concatenate([whole, extra], axis=2)
        return whole.transpose(1, 0, 2, 3).reshape(inner, -1, size)
    specs, given = [], []
    for terms in columns:
        for a, b in terms:
            for piece in a:
                specs.append(pl.BlockSpec((piece.shape[0], block), lambda k: (0, k)))
                given.append(piece)
            specs.append(pl.BlockSpec(b.shape, lambda k: (0, 0)))
            given.append(b)
    if added:
        specs.append(pl.BlockSpec((1, inner, added, size), lambda k: (k, 0, 0, 0)))
        given.append(extra)
    plan = tuple(tuple(len(a) for a, _ in terms) for terms in columns)
    result = pl.pallas_call(
        functools.partial(grads_kernel, plan, added),
        grid=(outer,),
        in_specs=specs,
        out_specs=pl.BlockSpec((inner, 1, rows + added, size), lambda k: (0, k, 0, 0)),
        out_shape=jax.ShapeDtypeStruct((inner, outer, rows + added, size), BF16),
        cost_estimate=pl.CostEstimate(
            flops=2 * tokens * width * size,
            bytes_accessed=2 * (tokens * (width + size) + width * size),
            transcendentals=0,
        ),
    )(*given)
    return result.reshape(inner, -1, size)


def unpack_kernel(cuts, *refs):
    parts, in_ref, out_ref = refs[:-2], refs[-2], refs[-1]
    outer = parts[0].shape[0]
    hidden = out_ref.shape[1] // outer
    for part, (start, size) in zip(parts, cuts):
        for k in range(outer):
            at = slice(k * hidden + start, k * hidden + start + size)
            in_ref[0, :, at] = part[k, :, :size].astype(F32)
            in_ref[1, :, at] = part[k, :, size : 2 * size].astype(F32)
            out_ref[:, at] = part[k, :, 2 * size :].astype(F32)


def unpack(parts, cuts, hidden):
    rows = parts[0].shape[1]
    return pl.pallas_call(
        functools.partial(unpack_kernel, cuts),
        in_specs=[VMEM] * len(parts),
        out_specs=[VMEM] * 2,
        out_shape=[
            jax.ShapeDtypeStruct((2, rows, hidden), F32),
            jax.ShapeDtypeStruct((rows, hidden), F32),
        ],
        cost_estimate=pl.CostEstimate(
            flops=0, bytes_accessed=18 * rows * hidden, transcendentals=0
        ),
    )(*parts)


def gelu_tanh(values):
    return jax.nn.gelu(values, approximate=True)


def geglu(gate_vals, up_vals):
    return gelu_tanh(gate_vals) * up_vals


def norm_back(values, scaling, delta):
    inverse = lax.rsqrt(jnp.mean(values * values, axis=-1, keepdims=True) + EPS)
    unit = values * inverse
    scaled = delta * (1.0 + scaling)
    moved = inverse * (scaled - unit * jnp.mean(scaled * unit, axis=-1, keepdims=True))
    return moved, jnp.sum(delta * unit, axis=0)


def rms_norm(values, scaling):
    inverse = lax.rsqrt(jnp.mean(values * values, axis=-1, keepdims=True) + EPS)
    return values * inverse * (1.0 + scaling)


def dot(a, b, contract):
    return lax.dot_general(a, b, ((contract[0], contract[1]), ((), ())), preferred_element_type=F32)


def mm(a, b):
    return dot(a, b, ((1,), (0,)))


def mm_nt(a, b):
    return dot(a, b, ((1,), (1,)))


def mm_tn(a, b):
    return dot(a, b, ((0,), (0,)))


def gather_slots(half):
    slots = []
    for k in range(lax.axis_size("o")):
        if k:
            half = ring(half)
        slots.append([half, swap(half)])
    return slots


def both_cores(part):
    rows = part.shape[0] // 2
    return part[:rows] + swap(part[rows:].astype(BF16)).astype(F32)


def ring_sum(parts):
    total = parts[0].astype(F32)
    for part in parts[1:]:
        low = total.astype(BF16)
        moved = ring(low)
        total = part.astype(F32) + moved.astype(F32)
    return total


def ring_order(parts):
    count, at = lax.axis_size("o"), lax.axis_index("o")
    return [
        lax.dynamic_index_in_dim(parts, lax.rem(at - k + count, count), 0, False)
        for k in [*range(1, count), 0]
    ]


def spread(value):
    return lax.all_to_all(value, "o", 0, 0, tiled=True)


def gather_inner(whole):
    return lax.all_gather(whole, "i", axis=1, tiled=True).reshape(-1, whole.shape[-1])


def sum_inner(rows):
    own = lax.psum_scatter(
        rows.reshape(-1, rows.shape[-1]), "i", scatter_dimension=0, tiled=True
    )
    return own.reshape(lax.axis_size("o"), -1, rows.shape[-1])


def cuts_of(size):
    first = size // 2 // 128 * 128 + 128 if size > 512 else size
    return ((0, first), (first, size - first)) if size > first else ((0, size),)


def per_device(
    inputs,
    segment_ids,
    cotangent,
    branch_weight,
    out_weight,
    ffw_in,
    ffw_out,
    norm_scales,
    branch_bias,
    conv_weight,
    conv_bias,
    gate_weights,
    gate_bias,
    decay_param,
    out_bias,
    ffw_bias,
):
    outer, inner = lax.axis_size("o"), lax.axis_size("i")
    count = outer * inner
    core, along = lax.axis_index("tensor"), lax.axis_index("o")
    tok_rows, width = inputs.shape
    part_width = width // count
    hidden_half = ffw_out.shape[0]
    hidden_part = hidden_half // outer
    taps_count = conv_weight.shape[0]
    rim_rows = taps_count - 1
    heads_half, block_size = gate_weights.shape[1], gate_weights.shape[2]
    width_half = heads_half * block_size

    cuts = cuts_of(hidden_part)
    seg_marks = (segment_ids + 1).astype(F32)
    lanes = jnp.broadcast_to(seg_marks[:, None], (tok_rows, 128))
    (branch_x_full, branch_y_full, out_full_t), parts, (normed_ext, before, after) = (
        gather_weights(
            [branch_weight[0], branch_weight[1], out_weight.T],
            ffw_in,
            ffw_out.T,
            inputs,
            1.0 + norm_scales[:1],
            jnp.concatenate([inputs[tok_rows - HALO :].astype(F32), lanes[-HALO:]], axis=1),
            lanes[:HALO],
            cuts,
        )
    )
    ffw_parts = []
    for k, (_, size) in enumerate(cuts):
        whole = gather_inner(parts[k])
        ffw_parts.append((whole[:, : 2 * size], whole[:, 2 * size :]))
    cot_own, branch_x_full = lax.optimization_barrier((half_of(cotangent, core), branch_x_full))
    cot_halves = [cot_own, ring(cot_own)]

    source_half = half_of(inputs, core).astype(F32)
    place = lax.axis_index(DP)
    marks_before = jnp.where(place == 0, 0.0, before[:, width])
    marks_after = jnp.where(place == count - 1, 0.0, after[:rim_rows, 0])
    normed_low = normed_ext[HALO:]
    marks_ext = jnp.concatenate([marks_before, seg_marks])
    same = [
        (marks_ext[HALO - k : HALO - k + tok_rows] == seg_marks).astype(F32)
        for k in range(taps_count)
    ]
    masks = jnp.stack([1.0 - same[1], *same[1:], *[same[0]] * (8 - taps_count)], axis=1)
    branch_ext = mm(normed_ext, branch_x_full) + branch_bias[0]
    branch_y = mm(normed_low, branch_y_full) + branch_bias[1]
    rate = jax.nn.softplus(decay_param)
    row_params = jnp.stack([conv_bias, gate_bias[0], gate_bias[1], rate] + [rate] * 4)
    conv_low, decay_gate, input_gate, cumulative, local_state, ends = mix(
        branch_ext, masks, conv_weight, row_params, gate_weights
    )
    conv_blocks = conv_low.reshape(tok_rows, heads_half, block_size)
    for k in range(2, min(3, outer)):
        cot_halves.append(ring(cot_halves[-1]))
    carry_in = entering(ends, False)
    carry_in, cot_halves[-1] = lax.optimization_barrier((carry_in, cot_halves[-1]))
    for k in range(3, outer):
        cot_halves.append(ring(cot_halves[-1]))
    states = local_state + cumulative * carry_in
    branch_act, gelu_back = jax.vjp(gelu_tanh, branch_y)
    mixed_in = (states * branch_act).astype(BF16)
    mixed_part = mm_nt(mixed_in, out_full_t)
    residual = (
        source_half
        + half_of(mixed_part, core)
        + swap(half_of(mixed_part, 1 - core))
        + out_bias[0]
    )

    normed_slots = gather_slots(rms_norm(residual, norm_scales[1]).astype(BF16))
    cot_slots = [[half, swap(half)] for half in cot_halves[:outer]]
    normed_joined = [jnp.concatenate(slot) for slot in normed_slots]
    cot_joined = [jnp.concatenate(slot) for slot in cot_slots]
    bias_part = lax.dynamic_slice_in_dim(ffw_bias, along * hidden_part, hidden_part, 1)
    slots = range(outer)
    hidden_of, delta_of, inner_sums, bias_sums, rows = [], [], [], [], None
    for p, (start, size) in enumerate(cuts):
        if rows is not None:
            rows, normed_joined, cot_joined = lax.optimization_barrier(
                (rows, normed_joined, cot_joined)
            )
            inner_sums.append(sum_inner(rows))
        in_full, out_full = ffw_parts[p]
        bias_row = bias_part[:, start : start + size].reshape(2 * size)
        hiddens, deltas = [], []
        for k in slots:
            gate_up = mm(normed_joined[k], in_full) + bias_row
            hidden, hidden_back = jax.vjp(geglu, gate_up[:, :size], gate_up[:, size:])
            hiddens.append(hidden.astype(BF16))
            deltas.append(
                jnp.concatenate(hidden_back(mm(cot_joined[k], out_full)), axis=1).astype(BF16)
            )
        if p == len(cuts) - 1:
            delta_parts = [
                sum(mm_nt(d[k], w[0]) for d, w in zip(delta_of + [deltas], ffw_parts))
                for k in slots
            ]
            sums = [both_cores(part) for part in delta_parts[1:] + delta_parts[:1]]
            _, hiddens, deltas = lax.optimization_barrier((sums[0], hiddens, deltas))
        hidden_of.append(hiddens)
        delta_of.append(deltas)
        bias_sums.append(
            sum(jnp.sum(d, axis=0, dtype=F32) for d in deltas).reshape(2, size)
        )
        rows = grads_rows([list(zip(normed_slots, deltas)), list(zip(cot_slots, hiddens))])
    inner_sums.append(sum_inner(rows))
    delta_normed_two = ring_sum(sums)
    result_parts = [
        sum(mm_nt(hidden_of[p][k], ffw_parts[p][1]) for p in range(len(cuts))) for k in slots
    ]
    result_parts = [both_cores(part) for part in result_parts]
    result_parts = result_parts[1:] + result_parts[:1]
    delta_normed_two, result_parts, inner_sums[0] = lax.optimization_barrier(
        (delta_normed_two, result_parts, inner_sums[0])
    )
    grads = [spread(inner_sums[0])]
    grad_ffw_bias = lax.dynamic_update_slice_in_dim(
        jnp.zeros((2, hidden_half), F32),
        jnp.concatenate(bias_sums, axis=1),
        along * hidden_part,
        1,
    )

    cot_half = half_of(cotangent, core).astype(F32)
    delta_res_norm, grad_scale_two = norm_back(residual, norm_scales[1], delta_normed_two)
    delta_residual = cot_half + delta_res_norm
    delta_half = delta_residual.astype(BF16)
    delta_mixed = join_halves(delta_half, swap(delta_half), core)
    delta_mixed_in = mm(delta_mixed, out_full_t)
    delta_states = delta_mixed_in * branch_act
    (delta_branch_y,) = gelu_back(delta_mixed_in * states)
    delta_y_low = delta_branch_y.astype(BF16)
    oy_rows = grads_rows([[([delta_mixed], mixed_in)], [([normed_low], delta_y_low)]])
    grad_oy_inner = sum_inner(oy_rows)
    reset = masks[:, :1]
    log_decay = -8.0 * decay_gate * rate
    decay = jnp.exp(log_decay)
    keep_rate = decay * (1.0 - reset)
    alpha_next = jnp.concatenate([keep_rate[1:], jnp.ones((1, width_half), F32)], axis=0)
    suffix, local_adjoint = local_scan(alpha_next, delta_states, True)
    leaving = entering(
        jnp.stack([keep_rate[0] * suffix[0], keep_rate[0] * local_adjoint[0]]), True
    )
    leaving, inner_sums[1:] = lax.optimization_barrier((leaving, inner_sums[1:]))
    for k in range(1, len(cuts)):
        grads.append(spread(inner_sums[k]))
    adjoint = local_adjoint + suffix * leaving
    states_before = jnp.concatenate([carry_in[None, :], states[: tok_rows - 1]], axis=0)
    conv_float = conv_low.astype(F32)
    room = -jnp.expm1(2.0 * log_decay)
    multiplier = jnp.sqrt(jnp.maximum(room, 0.001)) * (1.0 - reset) + reset
    drawn = adjoint * input_gate
    delta_log = keep_rate * (
        adjoint * states_before
        - jnp.where(room > 0.001, drawn * conv_float * decay / multiplier, 0.0)
    )
    decay_sum = jnp.sum(delta_log * decay_gate, axis=0)
    delta_conv_direct = drawn * multiplier
    delta_gates = jnp.stack(
        [
            delta_log * (-8.0 * rate) * decay_gate * (1.0 - decay_gate),
            delta_conv_direct * conv_float * (1.0 - input_gate),
        ]
    ).astype(BF16)
    grad_decay = -8.0 * decay_sum * jax.nn.sigmoid(decay_param)
    delta_blocks = delta_gates.reshape(2, tok_rows, heads_half, block_size)
    grad_gate_weights = jnp.einsum(
        "thb,gthc->ghbc", conv_blocks, delta_blocks, preferred_element_type=F32
    )
    gate_rows = (
        grad_gate_weights.reshape(2, heads_half, count, block_size // count, block_size)
        .transpose(2, 0, 1, 3, 4)
        .reshape(outer, inner, -1, width_half)
        .astype(BF16)
    )
    grad_gate_bias = jnp.sum(delta_gates, axis=1, dtype=F32)
    delta_conv = delta_conv_direct + jnp.einsum(
        "gthc,ghbc->thb", delta_blocks, gate_weights, preferred_element_type=F32
    ).reshape(tok_rows, width_half)
    rim_delta = from_behind(delta_conv[:rim_rows], -1)
    rim_delta, result_parts = lax.optimization_barrier((rim_delta, result_parts))
    result_sum = ring_sum(result_parts)
    ffw_in_grad, ffw_out_grad = unpack(grads, cuts, hidden_half)
    padded_delta = jnp.concatenate([delta_conv, rim_delta], axis=0)
    next_marks = jnp.concatenate([seg_marks, marks_after], axis=0)
    delta_branch_x = jnp.zeros_like(delta_conv)
    conv_weight_rows = []
    for offset in range(taps_count):
        matches = (next_marks[offset : offset + tok_rows] == seg_marks).astype(F32)[:, None]
        delta_branch_x = (
            delta_branch_x
            + conv_weight[offset] * padded_delta[offset : offset + tok_rows] * matches
        )
        shifted = branch_ext[HALO - offset : HALO - offset + tok_rows] * same[offset][:, None]
        conv_weight_rows.append(jnp.sum(delta_conv * shifted, axis=0))
    grad_conv_bias = jnp.sum(delta_conv, axis=0)
    delta_x_low = delta_branch_x.astype(BF16)
    x_rows = grads_rows([[([normed_low], delta_x_low)]], gate_rows)
    grad_x_inner = sum_inner(x_rows)
    delta_part = mm_nt(delta_x_low, branch_x_full) + mm_nt(delta_y_low, branch_y_full)
    delta_normed = half_of(delta_part, core) + swap(
        half_of(delta_part, 1 - core).astype(BF16)
    ).astype(F32)
    delta_source_norm, grad_scale_one = norm_back(source_half, norm_scales[0], delta_normed)
    grad_half = delta_residual + delta_source_norm
    input_grad = join_halves(grad_half, swap(grad_half), core)

    halves = jnp.stack(
        [
            grad_scale_one,
            grad_scale_two,
            jnp.sum(delta_half, axis=0, dtype=F32),
            jnp.sum(cot_half, axis=0),
        ]
    )
    halves = halves + swap(halves)
    flat = [
        halves.reshape(-1),
        jnp.sum(delta_x_low, axis=0, dtype=F32),
        jnp.sum(delta_y_low, axis=0, dtype=F32),
        *conv_weight_rows,
        grad_conv_bias,
        grad_gate_bias.reshape(-1),
        grad_decay,
        grad_ffw_bias.reshape(-1),
    ]
    grad_oy = ring_sum(ring_order(grad_oy_inner))
    small = sum_over_all(jnp.concatenate(flat).reshape(-1, 128))
    result_half = residual + result_sum + out_bias[1]
    result = join_halves(result_half, swap(result_half), core)
    grad_x_gate = ring_sum(ring_order(grad_x_inner))
    grad_branch_x = grad_x_gate[:part_width]
    gate_grad = grad_x_gate[part_width:].reshape(2, heads_half, block_size // count, block_size)
    small = small.reshape(-1)
    at = 0
    taken = []
    for shape in (
        (2, width),
        (2, width),
        (2, width_half),
        (taps_count, width_half),
        (width_half,),
        (2, width_half),
        (width_half,),
        (2, hidden_half),
    ):
        size = 1
        for n in shape:
            size *= n
        taken.append(small[at : at + size].reshape(shape))
        at += size
    scales, out_bias_grad, branch_bias_grad, taps_grad, conv_bias_grad, gate_bias_grad, decay_grad, ffw_bias_grad = taken
    return (
        result,
        input_grad,
        jnp.stack([grad_branch_x, grad_oy[:, width_half:]]),
        grad_oy[:, :width_half].T,
        ffw_in_grad,
        ffw_out_grad.T,
        scales,
        branch_bias_grad,
        taps_grad,
        conv_bias_grad,
        gate_grad,
        gate_bias_grad,
        decay_grad,
        out_bias_grad,
        ffw_bias_grad,
    )


def solution(mesh):
    count = mesh.shape["dp"]
    grid = Mesh(
        mesh.devices.reshape(count // INNER, INNER, mesh.shape["tensor"]), ("o", "i", "tensor")
    )
    in_specs = (
        P(DP, None),
        P(DP),
        P(DP, None),
        P(None, DP, "tensor"),
        P("tensor", DP),
        P(None, DP, "tensor"),
        P("tensor", DP),
        P(),
        P(None, "tensor"),
        P(None, "tensor"),
        P("tensor"),
        P(None, "tensor", None, None),
        P(None, "tensor"),
        P("tensor"),
        P(),
        P(None, "tensor"),
    )
    out_specs = (
        P(DP, None),
        P(DP, None),
        P(None, DP, "tensor"),
        P("tensor", DP),
        P(None, DP, "tensor"),
        P("tensor", DP),
        P(),
        P(None, "tensor"),
        P(None, "tensor"),
        P("tensor"),
        P(None, "tensor", DP, None),
        P(None, "tensor"),
        P("tensor"),
        P(),
        P(None, "tensor"),
    )

    return jax.shard_map(
        per_device, mesh=grid, in_specs=in_specs, out_specs=out_specs, check_vma=False
    )
```

```python
import functools

import jax
import jax.numpy as jnp
from jax import lax
from jax.experimental import pallas as pl
from jax.experimental.pallas import tpu as pltpu
from jax.sharding import Mesh
from jax.sharding import PartitionSpec as P


INNER = 4
DP = ("o", "i")
EPS = 1e-06
F32 = jnp.float32
BF16 = jnp.bfloat16


def swap(value):
    return lax.ppermute(value, "tensor", [(0, 1), (1, 0)])


def ring(value):
    count = lax.axis_size("o")
    return lax.ppermute(value, "o", [(k, (k + 1) % count) for k in range(count)])


def from_behind(value, steps):
    count = lax.axis_size(DP)
    first, last = max(0, -steps), min(count, count - steps)
    return lax.ppermute(value, DP, [(k, k + steps) for k in range(first, last)])


def sum_over_all(value):
    count, bit = lax.axis_size(DP), 1
    while bit < count:
        value = value + lax.ppermute(value, DP, [(k, k ^ bit) for k in range(count)])
        bit *= 2
    return value


def half_of(value, which):
    rows = value.shape[0] // 2
    return lax.dynamic_slice_in_dim(value, which * rows, rows, 0)


def join_halves(own, other, core):
    first = jnp.where(core == 0, own, other)
    second = jnp.where(core == 0, other, own)
    return jnp.concatenate([first, second], axis=0)


def run_scan(reverse, keep_ref, drive_ref, cum_ref, state_ref):
    rows, width = keep_ref.shape
    groups = rows // 8
    place = lax.broadcasted_iota(jnp.int32, (8, width), 0)

    def step(k, carried):
        before_a, before_b = carried
        group = groups - 1 - k if reverse else k
        at = pl.ds(pl.multiple_of(group * 8, 8), 8)
        a, b = keep_ref[at, :], drive_ref[at, :]
        for d in (1, 2, 4):
            far_a = pltpu.roll(a, 8 - d if reverse else d, 0)
            far_b = pltpu.roll(b, 8 - d if reverse else d, 0)
            inside = place < 8 - d if reverse else place >= d
            b = jnp.where(inside, a * far_b + b, b)
            a = jnp.where(inside, a * far_a, a)
        b = a * before_b + b
        a = a * before_a
        cum_ref[at, :] = a
        state_ref[at, :] = b
        edge = slice(0, 1) if reverse else slice(7, 8)
        return (a[edge], b[edge])

    return lax.fori_loop(
        0, groups, step, (jnp.ones((1, width), F32), jnp.zeros((1, width), F32))
    )


def scan_kernel(reverse, keep_ref, drive_ref, cum_ref, state_ref):
    run_scan(reverse, keep_ref, drive_ref, cum_ref, state_ref)


def local_scan(keep, drive, reverse):
    rows, width = keep.shape
    block = 256
    spec = pl.BlockSpec((rows, block), lambda j: (0, j))
    shape = jax.ShapeDtypeStruct((rows, width), F32)
    return pl.pallas_call(
        functools.partial(scan_kernel, reverse),
        grid=(width // block,),
        in_specs=[spec, spec],
        out_specs=[spec, spec],
        out_shape=[shape, shape],
        cost_estimate=pl.CostEstimate(
            flops=20 * rows * width, bytes_accessed=16 * rows * width, transcendentals=0
        ),
    )(keep, drive)


HALO = 16


def mix_kernel(branch_ref, mask_ref, taps_ref, rows_ref, gate_ref, *refs):
    conv_ref, decay_gate_ref, input_gate_ref, cum_ref, state_ref, ends_ref, keep, drive = refs
    rows = conv_ref.shape[0]
    conv = rows_ref[0:1, :] + taps_ref[0:1, :] * branch_ref[HALO : HALO + rows, :]
    for k in range(1, taps_ref.shape[0]):
        shifted = branch_ref[HALO - k : HALO - k + rows, :] * mask_ref[:, k : k + 1]
        conv = conv + taps_ref[k : k + 1, :] * shifted
    low = conv.astype(BF16)
    conv_ref[...] = low
    decay_gate = jax.nn.sigmoid(mm(low, gate_ref[0, 0]) + rows_ref[1:2, :])
    input_gate = jax.nn.sigmoid(mm(low, gate_ref[1, 0]) + rows_ref[2:3, :])
    decay_gate_ref[...] = decay_gate
    input_gate_ref[...] = input_gate
    reset = mask_ref[:, 0:1]
    log_decay = -8.0 * decay_gate * rows_ref[3:4, :]
    multiplier = jnp.sqrt(jnp.maximum(1.0 - jnp.exp(2.0 * log_decay), 0.001))
    keep[...] = jnp.exp(log_decay) * (1.0 - reset)
    drive[...] = low.astype(F32) * input_gate * (multiplier * (1.0 - reset) + reset)
    ends_ref[0:1, :], ends_ref[1:2, :] = run_scan(False, keep, drive, cum_ref, state_ref)


def mix(branch, masks, taps, row_params, gate_weights):
    rows, width = branch.shape[0] - HALO, branch.shape[1]
    block = gate_weights.shape[2]
    over = lambda n: pl.BlockSpec((n, block), lambda h: (0, h))
    full = jax.ShapeDtypeStruct((rows, width), F32)
    return pl.pallas_call(
        mix_kernel,
        grid=(width // block,),
        in_specs=[
            over(rows + HALO),
            pl.BlockSpec(masks.shape, lambda h: (0, 0)),
            over(taps.shape[0]),
            over(row_params.shape[0]),
            pl.BlockSpec((2, 1, block, block), lambda h: (0, h, 0, 0)),
        ],
        out_specs=[over(rows)] * 5 + [over(2)],
        out_shape=[
            jax.ShapeDtypeStruct((rows, width), BF16),
            full,
            full,
            full,
            full,
            jax.ShapeDtypeStruct((2, width), F32),
        ],
        scratch_shapes=[pltpu.VMEM((rows, block), F32)] * 2,
        cost_estimate=pl.CostEstimate(
            flops=4 * rows * width * block,
            bytes_accessed=22 * rows * width,
            transcendentals=8 * rows * width,
        ),
    )(branch, masks, taps, row_params, gate_weights)


MESH_ID = pl.DeviceIdType.MESH
VMEM = pl.BlockSpec(memory_space=pltpu.VMEM)
ANY = pl.BlockSpec(memory_space=pl.ANY)


def enter_kernel(outer, inner, reverse, ends_ref, carry_ref, every, send_sem, recv_sem):
    count = outer * inner
    core = lax.axis_index("tensor")
    me = lax.axis_index("o") * inner + lax.axis_index("i")
    barrier = pltpu.get_barrier_semaphore()
    for k in range(1, count):
        peer = lax.rem(me + k, count)
        to = (peer // inner, lax.rem(peer, inner), core)
        pl.semaphore_signal(barrier, inc=1, device_id=to, device_id_type=MESH_ID)
    pl.semaphore_wait(barrier, count - 1)

    def copy(k, mine):
        peer = lax.rem(me + k, count)
        return pltpu.make_async_remote_copy(
            src_ref=ends_ref,
            dst_ref=every.at[me if mine else peer],
            send_sem=send_sem.at[k],
            recv_sem=recv_sem.at[me if mine else peer],
            device_id=(peer // inner, lax.rem(peer, inner), core),
            device_id_type=MESH_ID,
        )

    for k in range(1, count):
        copy(k, True).start()
    for k in range(1, count):
        copy(k, False).wait_recv()
    carried = jnp.zeros((1, ends_ref.shape[1]), F32)
    for k in range(count):
        at = count - 1 - k if reverse else k
        reached = at > me if reverse else at < me
        block = every[at]
        carried = jnp.where(reached, block[0:1] * carried + block[1:2], carried)
    carry_ref[...] = carried
    for k in range(1, count):
        copy(k, True).wait_send()


def entering(ends, reverse):
    outer, inner = lax.axis_size("o"), lax.axis_size("i")
    count, width = outer * inner, ends.shape[1]
    carried = pl.pallas_call(
        functools.partial(enter_kernel, outer, inner, reverse),
        in_specs=[VMEM],
        out_specs=VMEM,
        out_shape=jax.ShapeDtypeStruct((1, width), F32),
        scratch_shapes=[
            pltpu.VMEM((count, 2, width), F32),
            pltpu.SemaphoreType.DMA((count,)),
            pltpu.SemaphoreType.DMA((count,)),
        ],
        compiler_params=pltpu.CompilerParams(
            collective_id=2 if reverse else 1, has_side_effects=True
        ),
    )(ends)
    return carried[0]


def gather_kernel(outer, inner, groups, cuts, *refs):
    parts = len(cuts)
    own, refs = refs[:groups], refs[groups:]
    in_ref, out_ref, source_ref, scale_ref, edge_ref, first_ref = refs[:6]
    refs = refs[6:]
    full, got, refs = refs[:groups], refs[groups : groups + parts], refs[groups + parts :]
    normed_ref, before_ref, after_ref = refs[:3]
    send, refs = refs[3 : 3 + parts], refs[3 + parts :]
    line_send, line_recv, side_send, side_recv, half_send, half_recv, part_send, part_recv = refs[:8]
    edge_send, edge_recv, local = refs[8:]
    o, i, core = lax.axis_index("o"), lax.axis_index("i"), lax.axis_index("tensor")
    sides = (i + 1 - 2 * lax.rem(i, 2), lax.rem(i + 2, 4))
    far = lax.rem(sides[0] + 2, 4)
    lanes = own[0].shape[1] // 2

    barrier = pltpu.get_barrier_semaphore()
    for k in range(1, outer):
        pl.semaphore_signal(
            barrier, inc=1, device_id=(lax.rem(o + k, outer), i, core), device_id_type=MESH_ID
        )
    for side in sides:
        pl.semaphore_signal(barrier, inc=1, device_id=(o, side, core), device_id_type=MESH_ID)
    count = outer * inner
    me = o * inner + i
    beside = []
    for step in (1, count - 1):
        at = lax.rem(me + step, count)
        beside.append((at // inner, lax.rem(at, inner), core))
        pl.semaphore_signal(barrier, inc=1, device_id=beside[-1], device_id_type=MESH_ID)
    pl.semaphore_wait(barrier, outer + 3)

    def remote(src, dst, send_sem, recv_sem, to):
        return pltpu.make_async_remote_copy(
            src_ref=src,
            dst_ref=dst,
            send_sem=send_sem,
            recv_sem=recv_sem,
            device_id=to,
            device_id_type=MESH_ID,
        )

    edges = [
        remote(edge_ref, before_ref, edge_send.at[0], edge_recv.at[0], beside[0]),
        remote(first_ref, after_ref, edge_send.at[1], edge_recv.at[1], beside[1]),
    ]
    for edge in edges:
        edge.start()

    def block(g, k, j):
        return full[g].at[k, j]

    def along_line(g, k, mine, step):
        return remote(
            own[g] if mine else block(g, k, i),
            block(g, k, i),
            line_send.at[g, k, step],
            line_recv.at[g, k],
            (o + 2 * step - 1, i, core),
        )

    def to_side(g, k, mine, side):
        return remote(
            own[g] if mine else block(g, k, i),
            block(g, k, i),
            side_send.at[g, k, side],
            side_recv.at[g, k, side],
            (o, sides[side], core),
        )

    def from_side(g, k, side):
        return remote(
            block(g, k, sides[side]),
            block(g, k, sides[side]),
            side_send.at[g, k, side],
            side_recv.at[g, k, side],
            (o, sides[side], core),
        )

    def half(g, k, side, to):
        part = full[g].at[k, side, :, pl.ds(lanes * to, lanes)]
        return remote(
            part, part, half_send.at[g, k, to], half_recv.at[g, k, to], (o, sides[to], core)
        )

    def visit(first, then):
        first(o)
        for d in range(1, outer):
            pl.when(o - d >= 0)(functools.partial(then, o - d, True))
            pl.when(o + d < outer)(functools.partial(then, o + d, False))

    for g in range(groups):
        pltpu.make_async_copy(own[g], block(g, o, i), local.at[g]).start()
        pl.when(o + 1 < outer)(lambda g=g: along_line(g, o, True, 1).start())
        pl.when(o > 0)(lambda g=g: along_line(g, o, True, 0).start())
        for side in range(2):
            to_side(g, o, True, side).start()

    hidden = in_ref.shape[2] // outer
    for p, (start, size) in enumerate(cuts):
        for k in range(outer):
            at = slice(k * hidden + start, k * hidden + start + size)
            send[p][k, :, :size] = in_ref[0, :, at]
            send[p][k, :, size : 2 * size] = in_ref[1, :, at]
            send[p][k, :, 2 * size :] = out_ref[:, at]
    tokens, width = source_ref.shape

    def normed(values):
        inverse = lax.rsqrt(jnp.mean(values * values, axis=-1, keepdims=True) + EPS)
        return (values * inverse * scale_ref[...]).astype(BF16)

    def norm_rows(k, _):
        at = pl.multiple_of(k * HALO, HALO)
        rows = source_ref[pl.ds(at, HALO), :].astype(F32)
        normed_ref[pl.ds(at + HALO, HALO), :] = normed(rows)
        return _

    lax.fori_loop(0, tokens // HALO, norm_rows, 0)
    for edge in edges:
        edge.wait()
    normed_ref[:HALO, :] = normed(before_ref[:, :width])

    def pass_on(k, from_left):
        for g in range(groups):
            along_line(g, k, False, 0).wait_recv()
            if from_left:
                pl.when(o + 1 < outer)(lambda g=g: along_line(g, k, False, 1).start())
            else:
                pl.when(o > 0)(lambda g=g: along_line(g, k, False, 0).start())
            for side in range(2):
                to_side(g, k, False, side).start()

    visit(lambda k: None, pass_on)

    def part(p, k, mine):
        peer = lax.rem(o + k, outer)
        return remote(
            send[p].at[peer],
            got[p].at[o if mine else peer],
            part_send.at[p, k],
            part_recv.at[p, o if mine else peer],
            (peer, i, core),
        )

    for p in range(parts):
        pltpu.make_async_copy(send[p].at[o], got[p].at[o], local.at[groups + p]).start()
        for k in range(1, outer):
            part(p, k, True).start()

    def turn(k, _=None):
        for g in range(groups):
            for side in range(2):
                from_side(g, k, side).wait_recv()
                half(g, k, sides[side], 1 - side).start()

    visit(turn, turn)

    def finish(k, _=None):
        for g in range(groups):
            for side in range(2):
                half(g, k, far, side).wait_recv()

    visit(finish, finish)
    for p in range(parts):
        for k in range(1, outer):
            part(p, k, False).wait_recv()

    def sent(k, from_left):
        for g in range(groups):
            if from_left is None or from_left:
                pl.when(o + 1 < outer)(lambda g=g: along_line(g, k, False, 1).wait_send())
            if not from_left:
                pl.when(o > 0)(lambda g=g: along_line(g, k, False, 0).wait_send())
            for side in range(2):
                to_side(g, k, False, side).wait_send()
                half(g, k, sides[side], 1 - side).wait_send()

    visit(functools.partial(sent, from_left=None), sent)
    for p in range(parts):
        for k in range(1, outer):
            part(p, k, True).wait_send()
    for g in range(groups):
        pltpu.make_async_copy(own[g], block(g, o, i), local.at[g]).wait()
    for p in range(parts):
        pltpu.make_async_copy(send[p].at[o], got[p].at[o], local.at[groups + p]).wait()


def gather_weights(own, ffw_in, ffw_out_t, source, scale, edge, first, cuts):
    outer, inner = lax.axis_size("o"), lax.axis_size("i")
    groups, parts = len(own), len(cuts)
    dma = pltpu.SemaphoreType.DMA
    blocks = [(outer, own[0].shape[0], 3 * size) for _, size in cuts]
    shape = jax.ShapeDtypeStruct
    out_shape = [shape((outer, inner, *w.shape), BF16) for w in own]
    out_shape += [shape(block, BF16) for block in blocks]
    out_shape += [
        shape((HALO + source.shape[0], source.shape[1]), BF16),
        shape(edge.shape, F32),
        shape(first.shape, F32),
    ]
    result = pl.pallas_call(
        functools.partial(gather_kernel, outer, inner, groups, cuts),
        in_specs=[VMEM] * (groups + 6),
        out_specs=[ANY] * (groups + parts) + [VMEM] * 3,
        out_shape=out_shape,
        scratch_shapes=[pltpu.VMEM(block, BF16) for block in blocks]
        + [
            dma((groups, outer, 2)),
            dma((groups, outer)),
            dma((groups, outer, 2)),
            dma((groups, outer, 2)),
            dma((groups, outer, 2)),
            dma((groups, outer, 2)),
            dma((parts, outer)),
            dma((parts, outer)),
            dma((2,)),
            dma((2,)),
            dma((groups + parts,)),
        ],
        compiler_params=pltpu.CompilerParams(collective_id=0, has_side_effects=True),
    )(*own, ffw_in, ffw_out_t, source, scale, edge, first)
    full = [w.reshape(-1, w.shape[-1]) for w in result[:groups]]
    return full, result[groups : groups + parts], result[groups + parts :]


def grads_kernel(plan, added, *refs):
    out_ref = refs[-1]
    inner, _, rows, _ = out_ref.shape
    take = rows - added
    if added:
        out_ref[:, 0, take:, :] = refs[-2][0]
    refs = iter(refs)
    at = 0
    for terms in plan:
        total = None
        for pieces in terms:
            a = [next(refs)[...] for _ in range(pieces)]
            term = mm_tn(jnp.concatenate(a) if pieces > 1 else a[0], next(refs)[...])
            total = term if total is None else total + term
        size = total.shape[1]
        out_ref[:, 0, :take, at : at + size] = total.astype(BF16).reshape(inner, take, size)
        at += size


def grads_rows(columns, extra=None):
    outer, inner = lax.axis_size("o"), lax.axis_size("i")
    width = columns[0][0][0][0].shape[1]
    block = width // outer
    rows = block // inner
    size = sum(terms[0][1].shape[1] for terms in columns)
    tokens = sum(b.shape[0] for _, b in columns[0])
    added = 0 if extra is None else extra.shape[2]
    if block % 128:
        whole = [
            sum(mm_tn(jnp.concatenate(a), b) for a, b in terms).astype(BF16) for terms in columns
        ]
        whole = jnp.concatenate(whole, axis=1).reshape(outer, inner, rows, size)
        if added:
            whole = jnp.concatenate([whole, extra], axis=2)
        return whole.transpose(1, 0, 2, 3).reshape(inner, -1, size)
    specs, given = [], []
    for terms in columns:
        for a, b in terms:
            for piece in a:
                specs.append(pl.BlockSpec((piece.shape[0], block), lambda k: (0, k)))
                given.append(piece)
            specs.append(pl.BlockSpec(b.shape, lambda k: (0, 0)))
            given.append(b)
    if added:
        specs.append(pl.BlockSpec((1, inner, added, size), lambda k: (k, 0, 0, 0)))
        given.append(extra)
    plan = tuple(tuple(len(a) for a, _ in terms) for terms in columns)
    result = pl.pallas_call(
        functools.partial(grads_kernel, plan, added),
        grid=(outer,),
        in_specs=specs,
        out_specs=pl.BlockSpec((inner, 1, rows + added, size), lambda k: (0, k, 0, 0)),
        out_shape=jax.ShapeDtypeStruct((inner, outer, rows + added, size), BF16),
        cost_estimate=pl.CostEstimate(
            flops=2 * tokens * width * size,
            bytes_accessed=2 * (tokens * (width + size) + width * size),
            transcendentals=0,
        ),
    )(*given)
    return result.reshape(inner, -1, size)


def unpack_kernel(cuts, *refs):
    parts, in_ref, out_ref = refs[:-2], refs[-2], refs[-1]
    outer = parts[0].shape[0]
    hidden = out_ref.shape[1] // outer
    for part, (start, size) in zip(parts, cuts):
        for k in range(outer):
            at = slice(k * hidden + start, k * hidden + start + size)
            in_ref[0, :, at] = part[k, :, :size].astype(F32)
            in_ref[1, :, at] = part[k, :, size : 2 * size].astype(F32)
            out_ref[:, at] = part[k, :, 2 * size :].astype(F32)


def unpack(parts, cuts, hidden):
    rows = parts[0].shape[1]
    return pl.pallas_call(
        functools.partial(unpack_kernel, cuts),
        in_specs=[VMEM] * len(parts),
        out_specs=[VMEM] * 2,
        out_shape=[
            jax.ShapeDtypeStruct((2, rows, hidden), F32),
            jax.ShapeDtypeStruct((rows, hidden), F32),
        ],
        cost_estimate=pl.CostEstimate(
            flops=0, bytes_accessed=18 * rows * hidden, transcendentals=0
        ),
    )(*parts)


def gelu_tanh(values):
    return jax.nn.gelu(values, approximate=True)


def geglu(gate_vals, up_vals):
    return gelu_tanh(gate_vals) * up_vals


def norm_back(values, scaling, delta):
    inverse = lax.rsqrt(jnp.mean(values * values, axis=-1, keepdims=True) + EPS)
    unit = values * inverse
    scaled = delta * (1.0 + scaling)
    moved = inverse * (scaled - unit * jnp.mean(scaled * unit, axis=-1, keepdims=True))
    return moved, jnp.sum(delta * unit, axis=0)


def rms_norm(values, scaling):
    inverse = lax.rsqrt(jnp.mean(values * values, axis=-1, keepdims=True) + EPS)
    return values * inverse * (1.0 + scaling)


def dot(a, b, contract):
    return lax.dot_general(a, b, ((contract[0], contract[1]), ((), ())), preferred_element_type=F32)


def mm(a, b):
    return dot(a, b, ((1,), (0,)))


def mm_nt(a, b):
    return dot(a, b, ((1,), (1,)))


def mm_tn(a, b):
    return dot(a, b, ((0,), (0,)))


def gather_slots(half):
    slots = []
    for k in range(lax.axis_size("o")):
        if k:
            half = ring(half)
        slots.append([half, swap(half)])
    return slots


def both_cores(part):
    rows = part.shape[0] // 2
    return part[:rows] + swap(part[rows:].astype(BF16)).astype(F32)


def ring_sum(parts):
    total = parts[0].astype(F32)
    for part in parts[1:]:
        low = total.astype(BF16)
        moved = ring(low)
        total = part.astype(F32) + moved.astype(F32)
    return total


def ring_order(parts):
    count, at = lax.axis_size("o"), lax.axis_index("o")
    return [
        lax.dynamic_index_in_dim(parts, lax.rem(at - k + count, count), 0, False)
        for k in [*range(1, count), 0]
    ]


def spread(value):
    return lax.all_to_all(value, "o", 0, 0, tiled=True)


def gather_inner(whole):
    return lax.all_gather(whole, "i", axis=1, tiled=True).reshape(-1, whole.shape[-1])


def sum_inner(rows):
    own = lax.psum_scatter(
        rows.reshape(-1, rows.shape[-1]), "i", scatter_dimension=0, tiled=True
    )
    return own.reshape(lax.axis_size("o"), -1, rows.shape[-1])


def cuts_of(size):
    first = size // 2 // 128 * 128 + 128 if size > 512 else size
    return ((0, first), (first, size - first)) if size > first else ((0, size),)


def per_device(
    inputs,
    segment_ids,
    cotangent,
    branch_weight,
    out_weight,
    ffw_in,
    ffw_out,
    norm_scales,
    branch_bias,
    conv_weight,
    conv_bias,
    gate_weights,
    gate_bias,
    decay_param,
    out_bias,
    ffw_bias,
):
    outer, inner = lax.axis_size("o"), lax.axis_size("i")
    count = outer * inner
    core, along = lax.axis_index("tensor"), lax.axis_index("o")
    tok_rows, width = inputs.shape
    part_width = width // count
    hidden_half = ffw_out.shape[0]
    hidden_part = hidden_half // outer
    taps_count = conv_weight.shape[0]
    rim_rows = taps_count - 1
    heads_half, block_size = gate_weights.shape[1], gate_weights.shape[2]
    width_half = heads_half * block_size

    cuts = cuts_of(hidden_part)
    seg_marks = (segment_ids + 1).astype(F32)
    lanes = jnp.broadcast_to(seg_marks[:, None], (tok_rows, 128))
    (branch_x_full, branch_y_full, out_full_t), parts, (normed_ext, before, after) = (
        gather_weights(
            [branch_weight[0], branch_weight[1], out_weight.T],
            ffw_in,
            ffw_out.T,
            inputs,
            1.0 + norm_scales[:1],
            jnp.concatenate([inputs[tok_rows - HALO :].astype(F32), lanes[-HALO:]], axis=1),
            lanes[:HALO],
            cuts,
        )
    )
    ffw_parts = []
    for k, (_, size) in enumerate(cuts):
        whole = gather_inner(parts[k])
        ffw_parts.append((whole[:, : 2 * size], whole[:, 2 * size :]))
    cot_own, branch_x_full = lax.optimization_barrier((half_of(cotangent, core), branch_x_full))
    cot_halves = [cot_own, ring(cot_own)]

    source_half = half_of(inputs, core).astype(F32)
    place = lax.axis_index(DP)
    marks_before = jnp.where(place == 0, 0.0, before[:, width])
    marks_after = jnp.where(place == count - 1, 0.0, after[:rim_rows, 0])
    normed_low = normed_ext[HALO:]
    marks_ext = jnp.concatenate([marks_before, seg_marks])
    same = [
        (marks_ext[HALO - k : HALO - k + tok_rows] == seg_marks).astype(F32)
        for k in range(taps_count)
    ]
    masks = jnp.stack([1.0 - same[1], *same[1:], *[same[0]] * (8 - taps_count)], axis=1)
    branch_ext = mm(normed_ext, branch_x_full) + branch_bias[0]
    branch_y = mm(normed_low, branch_y_full) + branch_bias[1]
    rate = jax.nn.softplus(decay_param)
    row_params = jnp.stack([conv_bias, gate_bias[0], gate_bias[1], rate] + [rate] * 4)
    conv_low, decay_gate, input_gate, cumulative, local_state, ends = mix(
        branch_ext, masks, conv_weight, row_params, gate_weights
    )
    conv_blocks = conv_low.reshape(tok_rows, heads_half, block_size)
    for k in range(2, min(3, outer)):
        cot_halves.append(ring(cot_halves[-1]))
    carry_in = entering(ends, False)
    carry_in, cot_halves[-1] = lax.optimization_barrier((carry_in, cot_halves[-1]))
    for k in range(3, outer):
        cot_halves.append(ring(cot_halves[-1]))
    states = local_state + cumulative * carry_in
    branch_act, gelu_back = jax.vjp(gelu_tanh, branch_y)
    mixed_in = (states * branch_act).astype(BF16)
    mixed_part = mm_nt(mixed_in, out_full_t)
    residual = (
        source_half
        + half_of(mixed_part, core)
        + swap(half_of(mixed_part, 1 - core))
        + out_bias[0]
    )

    normed_slots = gather_slots(rms_norm(residual, norm_scales[1]).astype(BF16))
    cot_slots = [[half, swap(half)] for half in cot_halves[:outer]]
    normed_joined = [jnp.concatenate(slot) for slot in normed_slots]
    cot_joined = [jnp.concatenate(slot) for slot in cot_slots]
    bias_part = lax.dynamic_slice_in_dim(ffw_bias, along * hidden_part, hidden_part, 1)
    slots = range(outer)
    hidden_of, delta_of, inner_sums, bias_sums, rows = [], [], [], [], None
    for p, (start, size) in enumerate(cuts):
        if rows is not None:
            rows, normed_joined, cot_joined = lax.optimization_barrier(
                (rows, normed_joined, cot_joined)
            )
            inner_sums.append(sum_inner(rows))
        in_full, out_full = ffw_parts[p]
        bias_row = bias_part[:, start : start + size].reshape(2 * size)
        hiddens, deltas = [], []
        for k in slots:
            gate_up = mm(normed_joined[k], in_full) + bias_row
            hidden, hidden_back = jax.vjp(geglu, gate_up[:, :size], gate_up[:, size:])
            hiddens.append(hidden.astype(BF16))
            deltas.append(
                jnp.concatenate(hidden_back(mm(cot_joined[k], out_full)), axis=1).astype(BF16)
            )
        if p == len(cuts) - 1:
            delta_parts = [
                sum(mm_nt(d[k], w[0]) for d, w in zip(delta_of + [deltas], ffw_parts))
                for k in slots
            ]
            sums = [both_cores(part) for part in delta_parts[1:] + delta_parts[:1]]
            _, hiddens, deltas = lax.optimization_barrier((sums[0], hiddens, deltas))
        hidden_of.append(hiddens)
        delta_of.append(deltas)
        bias_sums.append(
            sum(jnp.sum(d, axis=0, dtype=F32) for d in deltas).reshape(2, size)
        )
        rows = grads_rows([list(zip(normed_slots, deltas)), list(zip(cot_slots, hiddens))])
    inner_sums.append(sum_inner(rows))
    delta_normed_two = ring_sum(sums)
    result_parts = [
        sum(mm_nt(hidden_of[p][k], ffw_parts[p][1]) for p in range(len(cuts))) for k in slots
    ]
    result_parts = [both_cores(part) for part in result_parts]
    result_parts = result_parts[1:] + result_parts[:1]
    delta_normed_two, result_parts, inner_sums[0] = lax.optimization_barrier(
        (delta_normed_two, result_parts, inner_sums[0])
    )
    grads = [spread(inner_sums[0])]
    grad_ffw_bias = lax.dynamic_update_slice_in_dim(
        jnp.zeros((2, hidden_half), F32),
        jnp.concatenate(bias_sums, axis=1),
        along * hidden_part,
        1,
    )

    cot_half = half_of(cotangent, core).astype(F32)
    delta_res_norm, grad_scale_two = norm_back(residual, norm_scales[1], delta_normed_two)
    delta_residual = cot_half + delta_res_norm
    delta_half = delta_residual.astype(BF16)
    delta_mixed = join_halves(delta_half, swap(delta_half), core)
    delta_mixed_in = mm(delta_mixed, out_full_t)
    delta_states = delta_mixed_in * branch_act
    (delta_branch_y,) = gelu_back(delta_mixed_in * states)
    delta_y_low = delta_branch_y.astype(BF16)
    oy_rows = grads_rows([[([delta_mixed], mixed_in)], [([normed_low], delta_y_low)]])
    grad_oy_inner = sum_inner(oy_rows)
    reset = masks[:, :1]
    log_decay = -8.0 * decay_gate * rate
    decay = jnp.exp(log_decay)
    keep_rate = decay * (1.0 - reset)
    alpha_next = jnp.concatenate([keep_rate[1:], jnp.ones((1, width_half), F32)], axis=0)
    suffix, local_adjoint = local_scan(alpha_next, delta_states, True)
    leaving = entering(
        jnp.stack([keep_rate[0] * suffix[0], keep_rate[0] * local_adjoint[0]]), True
    )
    leaving, inner_sums[1:] = lax.optimization_barrier((leaving, inner_sums[1:]))
    for k in range(1, len(cuts)):
        grads.append(spread(inner_sums[k]))
    adjoint = local_adjoint + suffix * leaving
    states_before = jnp.concatenate([carry_in[None, :], states[: tok_rows - 1]], axis=0)
    conv_float = conv_low.astype(F32)
    room = -jnp.expm1(2.0 * log_decay)
    multiplier = jnp.sqrt(jnp.maximum(room, 0.001)) * (1.0 - reset) + reset
    drawn = adjoint * input_gate
    delta_log = keep_rate * (
        adjoint * states_before
        - jnp.where(room > 0.001, drawn * conv_float * decay / multiplier, 0.0)
    )
    decay_sum = jnp.sum(delta_log * decay_gate, axis=0)
    delta_conv_direct = drawn * multiplier
    delta_gates = jnp.stack(
        [
            delta_log * (-8.0 * rate) * decay_gate * (1.0 - decay_gate),
            delta_conv_direct * conv_float * (1.0 - input_gate),
        ]
    ).astype(BF16)
    grad_decay = -8.0 * decay_sum * jax.nn.sigmoid(decay_param)
    delta_blocks = delta_gates.reshape(2, tok_rows, heads_half, block_size)
    grad_gate_weights = jnp.einsum(
        "thb,gthc->ghbc", conv_blocks, delta_blocks, preferred_element_type=F32
    )
    split = width_half * 4 // 5
    gate_rows = (
        grad_gate_weights.reshape(2, heads_half, count, block_size // count, block_size)
        .transpose(2, 0, 1, 3, 4)
        .reshape(outer, inner, -1, split)
        .astype(BF16)
    )
    grad_gate_bias = jnp.sum(delta_gates, axis=1, dtype=F32)
    delta_conv = delta_conv_direct + jnp.einsum(
        "gthc,ghbc->thb", delta_blocks, gate_weights, preferred_element_type=F32
    ).reshape(tok_rows, width_half)
    rim_delta = from_behind(delta_conv[:rim_rows], -1)
    rim_delta, result_parts = lax.optimization_barrier((rim_delta, result_parts))
    result_sum = ring_sum(result_parts)
    ffw_in_grad, ffw_out_grad = unpack(grads, cuts, hidden_half)
    padded_delta = jnp.concatenate([delta_conv, rim_delta], axis=0)
    next_marks = jnp.concatenate([seg_marks, marks_after], axis=0)
    delta_branch_x = jnp.zeros_like(delta_conv)
    conv_weight_rows = []
    for offset in range(taps_count):
        matches = (next_marks[offset : offset + tok_rows] == seg_marks).astype(F32)[:, None]
        delta_branch_x = (
            delta_branch_x
            + conv_weight[offset] * padded_delta[offset : offset + tok_rows] * matches
        )
        shifted = branch_ext[HALO - offset : HALO - offset + tok_rows] * same[offset][:, None]
        conv_weight_rows.append(jnp.sum(delta_conv * shifted, axis=0))
    grad_conv_bias = jnp.sum(delta_conv, axis=0)
    delta_x_low = delta_branch_x.astype(BF16)
    x_rows = grads_rows([[([normed_low], delta_x_low[:, :split])]], gate_rows)
    grad_x_inner = sum_inner(x_rows)
    x_rows = grads_rows([[([normed_low], delta_x_low[:, split:])]])
    grad_z_inner = sum_inner(x_rows)
    delta_part = mm_nt(delta_x_low, branch_x_full) + mm_nt(delta_y_low, branch_y_full)
    delta_normed = half_of(delta_part, core) + swap(
        half_of(delta_part, 1 - core).astype(BF16)
    ).astype(F32)
    delta_source_norm, grad_scale_one = norm_back(source_half, norm_scales[0], delta_normed)
    grad_half = delta_residual + delta_source_norm
    input_grad = join_halves(grad_half, swap(grad_half), core)

    halves = jnp.stack(
        [
            grad_scale_one,
            grad_scale_two,
            jnp.sum(delta_half, axis=0, dtype=F32),
            jnp.sum(cot_half, axis=0),
        ]
    )
    halves = halves + swap(halves)
    flat = [
        halves.reshape(-1),
        jnp.sum(delta_x_low, axis=0, dtype=F32),
        jnp.sum(delta_y_low, axis=0, dtype=F32),
        *conv_weight_rows,
        grad_conv_bias,
        grad_gate_bias.reshape(-1),
        grad_decay,
        grad_ffw_bias.reshape(-1),
    ]
    grad_oy = ring_sum(ring_order(grad_oy_inner))
    small = sum_over_all(jnp.concatenate(flat).reshape(-1, 128))
    result_half = residual + result_sum + out_bias[1]
    result = join_halves(result_half, swap(result_half), core)
    grad_x_gate = ring_sum(ring_order(grad_x_inner))
    grad_x_rest = ring_sum(ring_order(grad_z_inner))
    grad_branch_x = jnp.concatenate([grad_x_gate[:part_width], grad_x_rest], axis=1)
    gate_grad = grad_x_gate[part_width:].reshape(2, heads_half, block_size // count, block_size)
    small = small.reshape(-1)
    at = 0
    taken = []
    for shape in (
        (2, width),
        (2, width),
        (2, width_half),
        (taps_count, width_half),
        (width_half,),
        (2, width_half),
        (width_half,),
        (2, hidden_half),
    ):
        size = 1
        for n in shape:
            size *= n
        taken.append(small[at : at + size].reshape(shape))
        at += size
    scales, out_bias_grad, branch_bias_grad, taps_grad, conv_bias_grad, gate_bias_grad, decay_grad, ffw_bias_grad = taken
    return (
        result,
        input_grad,
        jnp.stack([grad_branch_x, grad_oy[:, width_half:]]),
        grad_oy[:, :width_half].T,
        ffw_in_grad,
        ffw_out_grad.T,
        scales,
        branch_bias_grad,
        taps_grad,
        conv_bias_grad,
        gate_grad,
        gate_bias_grad,
        decay_grad,
        out_bias_grad,
        ffw_bias_grad,
    )


def solution(mesh):
    count = mesh.shape["dp"]
    grid = Mesh(
        mesh.devices.reshape(count // INNER, INNER, mesh.shape["tensor"]), ("o", "i", "tensor")
    )
    in_specs = (
        P(DP, None),
        P(DP),
        P(DP, None),
        P(None, DP, "tensor"),
        P("tensor", DP),
        P(None, DP, "tensor"),
        P("tensor", DP),
        P(),
        P(None, "tensor"),
        P(None, "tensor"),
        P("tensor"),
        P(None, "tensor", None, None),
        P(None, "tensor"),
        P("tensor"),
        P(),
        P(None, "tensor"),
    )
    out_specs = (
        P(DP, None),
        P(DP, None),
        P(None, DP, "tensor"),
        P("tensor", DP),
        P(None, DP, "tensor"),
        P("tensor", DP),
        P(),
        P(None, "tensor"),
        P(None, "tensor"),
        P("tensor"),
        P(None, "tensor", DP, None),
        P(None, "tensor"),
        P("tensor"),
        P(),
        P(None, "tensor"),
    )

    return jax.shard_map(
        per_device, mesh=grid, in_specs=in_specs, out_specs=out_specs, check_vma=False
    )
```
